32 devices in a mesh: dp: 1 (over z), tph: 4 (over y), tpw: 8 (over x, core).
Axes of the slice: x: 4, y: 4, z: 1, core: 2. Of those that a mesh axis runs over, the one named last changes fastest.
The devices are a block of a 4x4x8 slice.
Arguments:
- x_in: bfloat16 [128, 8192], P('dp', 'tpw')
- ln_attn: float32 [2, 8192], P(None, 'tpw')
- ln_mlp: float32 [2, 8192], P(None, 'tpw')
- w_qkv: bfloat16 [8192, 8, 18, 64], P('tpw', 'tph')
- w_out: bfloat16 [8, 16, 64, 8192], P('tph', None, None, 'tpw')
- w_up: bfloat16 [8192, 32768], P('tpw', 'tph')
- w_down: bfloat16 [32768, 8192], P('tph', 'tpw')
- k_cache: bfloat16 [128, 8, 512, 64], P(('dp', 'tpw'), 'tph')
- v_cache: bfloat16 [128, 8, 512, 64], P(('dp', 'tpw'), 'tph')
- positions: int32 [128], P(('dp', 'tpw'))
Outputs:
- output 1: bfloat16 [128, 8192], P('dp', 'tpw')
- output 2: bfloat16 [128, 8, 64], P(('dp', 'tpw'), 'tph')
- output 3: bfloat16 [128, 8, 64], P(('dp', 'tpw'), 'tph')
All inputs are finite; a program needn't handle non-finite values.
Results may differ from the reference program's by a relative error of at most 0.013997.
Values are sent between devices in bfloat16 or wider.
A program may use at most 768 MiB of HBM per device.

```python
import math
import jax
import jax.numpy as jnp
from jax import lax

MODEL_WIDTH = 8192
FF_WIDTH = 32768
KV_GROUPS = 8
Q_PER_GROUP = 16
HEAD_DIM = 64
BATCH_ROWS = 128
CACHE_LEN = 512
LN_EPS = 1e-5
ROPE_BASE = 10000.0
ATTN_SCALE = HEAD_DIM ** -0.5


def setup_inputs(seed: int = 0, part: int = 0) -> dict:
    shared = jax.random.split(jax.random.key(seed), 6)
    part_keys = jax.random.split(jax.random.fold_in(jax.random.key(seed + 1), part), 8)
    col_pos = jnp.arange(MODEL_WIDTH, dtype=jnp.float32) / MODEL_WIDTH
    wave_params = jax.random.uniform(part_keys[0], (3,), jnp.float32)
    col_scale = jnp.exp((0.6 + 0.4 * wave_params[0]) * jnp.cos(2.0 * math.pi * (col_pos + wave_params[1])))
    col_mean = 0.5 * jnp.sin(2.0 * math.pi * (col_pos + wave_params[2]))
    row_scale = jnp.exp(jax.random.uniform(part_keys[1], (BATCH_ROWS, 1), jnp.float32, -0.4, 0.4))
    row_mean = 0.3 * jax.random.normal(part_keys[2], (BATCH_ROWS, 1), jnp.float32)
    noise_x = jax.random.normal(part_keys[3], (BATCH_ROWS, MODEL_WIDTH), jnp.float32)
    x_in = (row_mean + col_mean + row_scale * col_scale * noise_x).astype(jnp.bfloat16)

    def norm_params(key_norm):
        key_gain, key_bias = jax.random.split(key_norm)
        gain_row = 1.0 + 0.3 * jax.random.normal(key_gain, (MODEL_WIDTH,), jnp.float32)
        bias_row = 0.3 * jax.random.normal(key_bias, (MODEL_WIDTH,), jnp.float32)
        return jnp.stack([gain_row, bias_row])

    def weight(key_w, shape_w, fan_in):
        return (jax.random.normal(key_w, shape_w, jnp.float32) * fan_in ** -0.5).astype(jnp.bfloat16)

    key_scale = math.sqrt(max(math.log(CACHE_LEN / 16.0), 1.0))
    cache_shape = (BATCH_ROWS, KV_GROUPS, CACHE_LEN, HEAD_DIM)
    k_cache = (key_scale * jax.random.normal(part_keys[4], cache_shape, jnp.float32)).astype(jnp.bfloat16)
    v_cache = jax.random.normal(part_keys[5], cache_shape, jnp.float32).astype(jnp.bfloat16)
    pos_keys = jax.random.split(part_keys[6])
    drawn_pos = jax.random.randint(pos_keys[0], (BATCH_ROWS,), 0, CACHE_LEN)
    full_row = jax.random.randint(pos_keys[1], (), 0, BATCH_ROWS)
    positions = jnp.where(jnp.arange(BATCH_ROWS) == full_row, CACHE_LEN - 1, drawn_pos).astype(jnp.int32)
    return {
        "x_in": x_in,
        "ln_attn": norm_params(shared[0]),
        "ln_mlp": norm_params(shared[1]),
        "w_qkv": weight(shared[2], (MODEL_WIDTH, KV_GROUPS, Q_PER_GROUP + 2, HEAD_DIM), MODEL_WIDTH),
        "w_out": weight(shared[3], (KV_GROUPS, Q_PER_GROUP, HEAD_DIM, MODEL_WIDTH), KV_GROUPS * Q_PER_GROUP * HEAD_DIM),
        "w_up": weight(shared[4], (MODEL_WIDTH, FF_WIDTH), MODEL_WIDTH),
        "w_down": weight(shared[5], (FF_WIDTH, MODEL_WIDTH), FF_WIDTH),
        "k_cache": k_cache,
        "v_cache": v_cache,
        "positions": positions,
    }


def layer_norm(x_f32, params):
    row_sum = jnp.sum(x_f32, axis=-1, keepdims=True)
    row_sq = jnp.sum(x_f32 * x_f32, axis=-1, keepdims=True)
    row_mean = row_sum / MODEL_WIDTH
    row_var = row_sq / MODEL_WIDTH - row_mean * row_mean
    return ((x_f32 - row_mean) * lax.rsqrt(row_var + LN_EPS) * params[0] + params[1]).astype(jnp.bfloat16)


def rotary(vectors, cos_t, sin_t):
    half_dim = HEAD_DIM // 2
    lo_half = vectors[..., :half_dim]
    hi_half = vectors[..., half_dim:]
    return jnp.concatenate([lo_half * cos_t - hi_half * sin_t, hi_half * cos_t + lo_half * sin_t], axis=-1)


def attend_row(row_args):
    q_row, k_row, v_row, k_rows, v_rows, pos_row = row_args
    q_f32 = q_row.astype(jnp.float32)
    old_scores = jnp.einsum("gqh,gsh->gqs", q_f32, k_rows.astype(jnp.float32)) * ATTN_SCALE
    old_scores = jnp.where(jnp.arange(CACHE_LEN) < pos_row, old_scores, -jnp.inf)
    new_score = jnp.einsum("gqh,gh->gq", q_f32, k_row.astype(jnp.float32))[..., None] * ATTN_SCALE
    attn_wts = jax.nn.softmax(jnp.concatenate([old_scores, new_score], axis=-1), axis=-1)
    attn_wts = attn_wts.astype(jnp.bfloat16).astype(jnp.float32)
    context = jnp.einsum("gqs,gsh->gqh", attn_wts[..., :CACHE_LEN], v_rows.astype(jnp.float32))
    context = context + attn_wts[..., CACHE_LEN:] * v_row.astype(jnp.float32)[:, None, :]
    return context.astype(jnp.bfloat16)


def reference(x_in, ln_attn, ln_mlp, w_qkv, w_out, w_up, w_down, k_cache, v_cache, positions):
    x_f32 = x_in.astype(jnp.float32)
    h_attn = layer_norm(x_f32, ln_attn)
    h_mlp = layer_norm(x_f32, ln_mlp)
    qkv_rows = jnp.dot(h_attn, w_qkv.reshape(MODEL_WIDTH, -1), preferred_element_type=jnp.float32)
    qkv_rows = qkv_rows.reshape(BATCH_ROWS, KV_GROUPS, Q_PER_GROUP + 2, HEAD_DIM).astype(jnp.bfloat16).astype(jnp.float32)
    half_dim = HEAD_DIM // 2
    inv_freq = ROPE_BASE ** (-jnp.arange(half_dim, dtype=jnp.float32) * (2.0 / HEAD_DIM))
    angles = positions.astype(jnp.float32)[:, None] * inv_freq[None, :]
    cos_t = jnp.cos(angles)[:, None, :]
    sin_t = jnp.sin(angles)[:, None, :]
    q_rot = rotary(qkv_rows[:, :, :Q_PER_GROUP], cos_t[:, :, None, :], sin_t[:, :, None, :]).astype(jnp.bfloat16)
    k_new = rotary(qkv_rows[:, :, Q_PER_GROUP], cos_t, sin_t).astype(jnp.bfloat16)
    v_new = qkv_rows[:, :, Q_PER_GROUP + 1].astype(jnp.bfloat16)
    context = lax.map(attend_row, (q_rot, k_new, v_new, k_cache, v_cache, positions))
    attn_out = jnp.dot(context.reshape(BATCH_ROWS, -1), w_out.reshape(-1, MODEL_WIDTH), preferred_element_type=jnp.float32)
    pre_act = jnp.dot(h_mlp, w_up, preferred_element_type=jnp.float32)
    act_bf = jax.nn.gelu(pre_act, approximate=False).astype(jnp.bfloat16)
    mlp_out = jnp.dot(act_bf, w_down, preferred_element_type=jnp.float32)
    x_out = (x_f32 + attn_out + mlp_out).astype(jnp.bfloat16)
    return (x_out, k_new, v_new)
```

```python
import functools
import math

import jax
import jax.numpy as jnp
from jax import lax
from jax.experimental import pallas as pl
from jax.experimental.pallas import tpu as pltpu
from jax.sharding import PartitionSpec as P

LN_EPS = 1e-5
ROPE_BASE = 10000.0
MESH = pl.DeviceIdType.MESH
F32 = jnp.float32
BF16 = jnp.bfloat16
VMEM_LIMIT = 67043328
GROUPS_OF_ROWS = 2
NN = (((1,), (0,)), ((), ()))
NT = (((1,), (1,)), ((), ()))
PIECES = ((2, 0), (2, 1), (1, 1), (3, 0), (1, 0), (3, 1), (0, 0), (0, 1))
ARRIVALS = ((0, 0), (0, 1), (3, 0), (1, 1), (3, 1), (1, 0), (2, 0), (2, 1))


def dot(a, b, dims=NN):
    return lax.dot_general(a, b, dims, preferred_element_type=F32)


def layer_kernel(
    W, NY,
    pos_ref, x_hbm, lna_hbm, lnm_hbm, wqkv_hbm, wout_hbm, wup_hbm, wdn_hbm, k_hbm, v_hbm,
    xout_ref, knew_ref, vnew_ref,
    x_v, lna_v, lnm_v, wqkv_v, wout_v, wup_v, wdn_v, k_v, v_v,
    stat_send, stat_recv, ha_v, hm_v,
    qpart, qsib, qsend, qrecv, qrot, kvrot, ctxs, ctx_all,
    upart, usib, usend, urecv, act_all, acc, ysend, yrecv,
    lsem, ssem, rsem,
):
    NX = W // 2
    R, D = x_v.shape
    NG = GROUPS_OF_ROWS
    RG = R // NG
    RY = RG // NY
    RB = R // W
    G, HD = kvrot.shape[0], k_v.shape[1]
    L = k_v.shape[2]
    QT = qrot.shape[1] // RB
    HB = wup_v.shape[2] // 2
    model_width = float(D * W)

    w = lax.axis_index("tpw")
    y = lax.axis_index("tph")
    c = lax.rem(w, 2)
    x = lax.div(w, 2)
    sib = w + 1 - 2 * c
    right = lax.rem(w + 2, W)
    left = lax.rem(w + W - 2, W)
    opp = lax.rem(w + W // 2, W)

    def chip(o):
        return lax.rem(x + o, NX)

    loads = {}

    def load(name, src, dst):
        cp = pltpu.make_async_copy(src, dst, lsem.at[len(loads)])
        cp.start()
        loads[name] = cp

    load("x", x_hbm, x_v)
    load("lna", lna_hbm, lna_v)
    load("lnm", lnm_hbm, lnm_v)
    qw = wqkv_v.shape[1]
    for g in range(G):
        load(("qkv", g), wqkv_hbm.at[pl.ds(g * qw, qw), :], wqkv_v.at[g])
    for i, (o, h) in enumerate(PIECES):
        col = pl.multiple_of((chip(o) * 2 + h) * 2 * HB, 2 * HB)
        load(("up", i), wup_hbm.at[:, pl.ds(col, 2 * HB)], wup_v.at[i])
    load("k", k_hbm, k_v)
    load("v", v_hbm, v_v)
    load("out", wout_hbm, wout_v)
    for i, (o, h) in enumerate(ARRIVALS):
        row = pl.multiple_of((chip(o) * 2 + h) * 2 * HB, 2 * HB)
        load(("down", i), wdn_hbm.at[pl.ds(row, 2 * HB), :], wdn_v.at[i])

    barrier = pltpu.get_barrier_semaphore()
    for i in range(1, W):
        pl.semaphore_signal(barrier, inc=1, device_id={"tpw": lax.rem(w + i, W)}, device_id_type=MESH)
    for i in range(1, NY):
        pl.semaphore_signal(barrier, inc=1, device_id={"tph": lax.rem(y + i, NY)}, device_id_type=MESH)

    sent = []
    messages = {}

    def send(name, src, dst, axis, to):
        i = len(sent)
        cp = pltpu.make_async_remote_copy(
            src_ref=src, dst_ref=dst, send_sem=ssem.at[i], recv_sem=rsem.at[i],
            device_id={axis: to}, device_id_type=MESH,
        )
        cp.start()
        sent.append(cp)
        messages[name] = cp

    def arrived(name):
        messages[name].wait_recv()

    loads["x"].wait()
    xf = x_v[...].astype(F32)
    s1 = jnp.sum(xf, axis=1, keepdims=True)
    s2 = jnp.sum(xf * xf, axis=1, keepdims=True)
    lane = lax.broadcasted_iota(jnp.int32, (R, 128), 1)
    stat_send[...] = jnp.where(lane == 0, s1, jnp.where(lane == 1, s2, 0.0)).T[0:8, :]
    pl.semaphore_wait(barrier, W - 1 + NY - 1)
    for i in range(1, W):
        send(("stat", i), stat_send, stat_recv.at[i - 1], "tpw", lax.rem(w + i, W))

    prow = lax.broadcasted_iota(jnp.int32, (RB, 128), 0)
    plane = lax.broadcasted_iota(jnp.int32, (RB, 128), 1)
    pos = jnp.zeros((RB, 128), jnp.int32)
    for b in range(RB):
        pos = jnp.where(prow == b, pos_ref[b], pos)
    half = HD // 2
    freq = jnp.exp(lax.rem(plane, half).astype(F32) * (-math.log(ROPE_BASE) * 2.0 / HD))
    angle = pos.astype(F32) * freq
    cos_t = jnp.cos(angle)
    first = lax.rem(plane, HD) < half
    sin_t = jnp.where(first, -jnp.sin(angle), jnp.sin(angle))

    for i in range(1, W):
        arrived(("stat", i))
    tot = stat_send[...]
    for i in range(1, W):
        tot = tot + stat_recv[i - 1]
    cols = jnp.concatenate([tot, jnp.zeros((R - 8, R), F32)], axis=0).T
    mean = cols[:, 0:1] / model_width
    var = cols[:, 1:2] / model_width - mean * mean
    rstd = lax.rsqrt(var + LN_EPS)
    loads["lna"].wait()
    loads["lnm"].wait()
    cen = (x_v[...].astype(F32) - mean) * rstd
    ha_v[...] = (cen * lna_v[0:1, :] + lna_v[1:2, :]).astype(BF16)
    hm_v[...] = (cen * lnm_v[0:1, :] + lnm_v[1:2, :]).astype(BF16)

    def tree(tag, own, stage, landing):
        def m1():
            stage[0] = own(2, 0).astype(BF16)
            send((tag, 0), stage.at[0], landing.at[0], "tpw", right)
            stage[1] = own(2, 1).astype(BF16)
            send((tag, 1), stage.at[1], landing.at[1], "tpw", left)

        def m2():
            stage[2] = own(1, 1).astype(BF16)
            send((tag, 2), stage.at[2], landing.at[2], "tpw", right)
            stage[3] = own(3, 0).astype(BF16)
            send((tag, 3), stage.at[3], landing.at[3], "tpw", left)

        def m3():
            arrived((tag, 0))
            stage[4] = (own(1, 0) + landing[0].astype(F32)).astype(BF16)
            send((tag, 4), stage.at[4], landing.at[4], "tpw", right)
            arrived((tag, 1))
            stage[5] = (own(3, 1) + landing[1].astype(F32)).astype(BF16)
            send((tag, 5), stage.at[5], landing.at[5], "tpw", left)

        def total(h):
            a, b = ((3, 4), (2, 5))[h]
            arrived((tag, a))
            arrived((tag, b))
            return own(0, h) + landing[a].astype(F32) + landing[b].astype(F32)

        return m1, m2, m3, total

    def qkv_mm(g):
        loads[("qkv", g)].wait()
        part = dot(ha_v[...], wqkv_v[g], NT).astype(BF16)
        qpart[g] = part.reshape(NX, 2, RB, qw)
        send(("qs", g), qpart.at[g, :, 1 - c], qsib.at[g], "tpw", sib)

    def qkv_own(o, g):
        return qpart[g, chip(o), c].astype(F32) + qsib[g, chip(o)].astype(F32)

    q1, q2, q3, q_total = tree("q", qkv_own, qsend, qrecv)

    def up_mm(r, i):
        if r == 0:
            loads[("up", i)].wait()
        hm = hm_v[r * RG:(r + 1) * RG, :]
        for k in range(2):
            upart[r, i, k] = dot(hm, wup_v[i, :, k * HB:(k + 1) * HB]).astype(BF16)
        send(("us", r, i), upart.at[r, i, 1 - c], usib.at[r, i], "tpw", sib)

    def up_tree(r):
        waited = set()

        def own(o, h):
            i = PIECES.index((o, h))
            if i not in waited:
                arrived(("us", r, i))
                waited.add(i)
            return upart[r, i, c].astype(F32) + usib[r, i].astype(F32)

        return tree(("u", r), own, usend.at[r], urecv.at[r])

    trees = [up_tree(r) for r in range(NG)]
    mine = pl.ds(pl.multiple_of(c * HB, HB), HB)

    def act_slot(r, o, h):
        return act_all.at[r, ARRIVALS.index((o, h)), :, mine]

    def act_send(r, name, o, h, axis_to, to_o):
        send(("a", r, name), act_slot(r, o, h), act_slot(r, to_o, h), "tpw", axis_to)

    def act_first(r, h):
        pre = trees[r][3](h)
        act = 0.5 * pre * (1.0 + lax.erf(pre * (2.0 ** -0.5)))
        act_all[r, ARRIVALS.index((0, h)), :, mine] = act.astype(BF16)
        if h == 0:
            act_send(r, "1r", 0, 0, right, 3)
        else:
            act_send(r, "1l", 0, 1, left, 1)
        act_send(r, ("s", 0, h), 0, h, sib, 0)

    def act_second(r):
        act_send(r, "2r", 0, 1, right, 3)
        act_send(r, "2l", 0, 0, left, 1)

    def act_third(r):
        arrived(("a", r, "1r"))
        act_send(r, "3r", 3, 0, right, 2)
        act_send(r, ("s", 3, 0), 3, 0, sib, 3)
        arrived(("a", r, "1l"))
        act_send(r, "3l", 1, 1, left, 2)
        act_send(r, ("s", 1, 1), 1, 1, sib, 1)

    def act_pass(r, name, o, h):
        arrived(("a", r, name))
        act_send(r, ("s", o, h), o, h, sib, o)

    def down_mm(r, i):
        o, h = ARRIVALS[i]
        arrived(("a", r, ("s", o, h)))
        if r == 0:
            loads[("down", i)].wait()
        part = dot(act_all[r, i], wdn_v[i])
        if i == 0:
            acc[r] = part
        else:
            acc[r] += part

    def rotary(t):
        swapped = jnp.where(first, pltpu.roll(t, 128 - half, 1), pltpu.roll(t, half, 1))
        return (t * cos_t + swapped * sin_t).astype(BF16).astype(F32)

    def attention():
        for g in range(G):
            qkv = q_total(g).astype(BF16).astype(F32)
            for t in range(QT):
                qrot[g, t * RB:(t + 1) * RB, :] = rotary(qkv[:, t * 128:(t + 1) * 128])
            last = qkv[:, QT * 128:]
            kv = jnp.where(plane < HD, rotary(last), last)
            kvrot[g] = kv
            knew_ref[:, g * HD:(g + 1) * HD] = kv[:, :HD].astype(BF16)
            vnew_ref[:, g * HD:(g + 1) * HD] = kv[:, HD:].astype(BF16)
        loads["k"].wait()
        loads["v"].wait()
        scale = HD ** -0.5
        when = lax.broadcasted_iota(jnp.int32, (2 * QT, L), 1)

        def row(b):
            for g in range(G):
                q8 = qrot[g, pl.ds(b, QT, stride=RB), :]
                q = jnp.concatenate([q8[:, :HD], q8[:, HD:]], axis=0)
                kv = kvrot[g, pl.ds(b, 1), :]
                s = dot(q.astype(BF16), k_v[b * G + g]) * scale
                s = jnp.where(when < pos_ref[b], s, -jnp.inf)
                sn = jnp.sum(q * kv[:, :HD], axis=1, keepdims=True) * scale
                m = jnp.maximum(jnp.max(s, axis=1, keepdims=True), sn)
                e = jnp.exp(s - m)
                en = jnp.exp(sn - m)
                rz = 1.0 / (jnp.sum(e, axis=1, keepdims=True) + en)
                wn = (en * rz).astype(BF16).astype(F32)
                ctx = dot((e * rz).astype(BF16), v_v[b * G + g], NT) + wn * kv[:, HD:]
                ctxs[g, pl.ds(b, QT, stride=RB), :] = jnp.concatenate([ctx[:QT], ctx[QT:]], axis=1)

        def rows(i, _):
            for j in range(4):
                row(i * 4 + j)
            return 0

        lax.fori_loop(0, RB // 4, rows, 0)
        for g in range(G):
            for t in range(QT):
                ctx_all[w, g, :, t * 128:(t + 1) * 128] = ctxs[g, t * RB:(t + 1) * RB, :].astype(BF16)

    def ctx_send(name, who, g, to):
        send(("c", name), ctx_all.at[who, g], ctx_all.at[who, g], "tpw", to)

    def ctx_first():
        ctx_send("1r", w, 0, right)
        ctx_send("1l", w, 1, left)
        ctx_send("2r", w, 1, right)
        ctx_send("2l", w, 0, left)
        for g in range(G):
            ctx_send(("s", 0, g), w, g, sib)

    def ctx_third():
        arrived(("c", "1r"))
        ctx_send("3r", left, 0, right)
        ctx_send(("s", 3, 0), left, 0, sib)
        arrived(("c", "1l"))
        ctx_send("3l", right, 1, left)
        ctx_send(("s", 1, 1), right, 1, sib)

    def ctx_rest():
        for name, who, o, g in (("2r", left, 3, 1), ("2l", right, 1, 0), ("3r", opp, 2, 0), ("3l", opp, 2, 1)):
            arrived(("c", name))
            ctx_send(("s", o, g), who, g, sib)

    def attn_mm():
        for o in range(NX):
            for g in range(G):
                arrived(("c", ("s", o, g)))
        loads["out"].wait()
        for g in range(G):
            n = QT * 128
            part = dot(ctx_all[:, g].reshape(R, n), wout_v[g * n:(g + 1) * n, :])
            for r in range(NG):
                acc[r] += part[r * RG:(r + 1) * RG]

    def y_scatter(r):
        ysend[r] = acc[r].astype(BF16)
        for i in range(1, NY):
            to = lax.rem(y + i, NY)
            rows = pl.ds(pl.multiple_of(to * RY, RY), RY)
            send(("y", r, i), ysend.at[r, rows], yrecv.at[r, i - 1], "tph", to)

    def y_gather(r):
        start = pl.multiple_of(y * RY, RY)
        tot = acc[r, pl.ds(start, RY), :]
        for i in range(1, NY):
            arrived(("y", r, i))
            tot = tot + yrecv[r, i - 1].astype(F32)
        rows = pl.ds(pl.multiple_of(r * RG + start, RY), RY)
        xout_ref[rows, :] = (x_v[rows, :].astype(F32) + tot).astype(BF16)
        for i in range(1, NY):
            send(("z", r, i), xout_ref.at[rows, :], xout_ref.at[rows, :], "tph", lax.rem(y + i, NY))

    qkv_mm(0)
    qkv_mm(1)
    up_mm(0, 0)
    up_mm(0, 1)
    for g in range(G):
        arrived(("qs", g))
    q1()
    q2()
    up_mm(0, 2)
    up_mm(0, 3)
    trees[0][0]()
    up_mm(0, 4)
    up_mm(0, 5)
    trees[0][1]()
    q3()
    up_mm(0, 6)
    up_mm(0, 7)
    up_mm(1, 0)
    up_mm(1, 1)
    trees[0][2]()
    up_mm(1, 2)
    up_mm(1, 3)
    trees[1][0]()
    up_mm(1, 4)
    up_mm(1, 5)
    trees[1][1]()
    up_mm(1, 6)
    up_mm(1, 7)
    act_first(0, 0)
    act_first(0, 1)
    trees[1][2]()
    act_second(0)
    attention()
    act_third(0)
    ctx_first()
    act_first(1, 0)
    act_first(1, 1)
    act_second(1)
    ctx_third()
    down_mm(0, 0)
    down_mm(0, 1)
    act_pass(0, "2r", 3, 1)
    act_pass(0, "2l", 1, 0)
    act_pass(0, "3r", 2, 0)
    act_pass(0, "3l", 2, 1)
    act_third(1)
    ctx_rest()
    for i in range(2, 8):
        down_mm(0, i)
    down_mm(1, 0)
    down_mm(1, 1)
    attn_mm()
    y_scatter(0)
    act_pass(1, "2r", 3, 1)
    act_pass(1, "2l", 1, 0)
    for i in range(2, 4):
        down_mm(1, i)
    act_pass(1, "3r", 2, 0)
    act_pass(1, "3l", 2, 1)
    y_gather(0)
    for i in range(4, 8):
        down_mm(1, i)
    y_scatter(1)
    y_gather(1)
    for r in range(NG):
        for i in range(1, NY):
            arrived(("z", r, i))
    for cp in sent:
        cp.wait_send()


def solution(mesh):
    W = mesh.shape["tpw"]
    NY = mesh.shape["tph"]
    if W != 8:
        raise ValueError("tpw")

    def local_layer(x_in, ln_attn, ln_mlp, w_qkv, w_out, w_up, w_down, k_cache, v_cache, positions):
        R, D = x_in.shape
        _, G, S, HD = w_qkv.shape
        F = w_up.shape[1]
        L = k_cache.shape[2]
        RB = R // W
        NX = W // 2
        NG = GROUPS_OF_ROWS
        RG = R // NG
        qw = S * HD
        cw = (S - 2) * HD
        QT = cw // 128
        HB = F // W // 2
        wqkv_t = jnp.transpose(w_qkv, (1, 2, 3, 0)).reshape(G * qw, D)
        k_t = jnp.swapaxes(k_cache, 2, 3).reshape(RB * G, HD, L)
        v_t = jnp.swapaxes(v_cache, 2, 3).reshape(RB * G, HD, L)
        n_messages = 7 + 2 + 6 + NG * 8 + NG * 6 + NG * 14 + 14 + NG * 6
        any_spec = pl.BlockSpec(memory_space=pl.ANY)
        vmem_spec = pl.BlockSpec(memory_space=pltpu.VMEM)
        x_out, k_new, v_new = pl.pallas_call(
            functools.partial(layer_kernel, W, NY),
            name="layer",
            out_shape=(
                jax.ShapeDtypeStruct((R, D), BF16),
                jax.ShapeDtypeStruct((RB, G * HD), BF16),
                jax.ShapeDtypeStruct((RB, G * HD), BF16),
            ),
            in_specs=[pl.BlockSpec(memory_space=pltpu.SMEM)] + [any_spec] * 9,
            out_specs=(vmem_spec,) * 3,
            scratch_shapes=[
                pltpu.VMEM((R, D), BF16),
                pltpu.VMEM((2, D), F32),
                pltpu.VMEM((2, D), F32),
                pltpu.VMEM((G, qw, D), BF16),
                pltpu.VMEM((G * cw, D), BF16),
                pltpu.VMEM((8, D, 2 * HB), BF16),
                pltpu.VMEM((8, 2 * HB, D), BF16),
                pltpu.VMEM((RB * G, HD, L), BF16),
                pltpu.VMEM((RB * G, HD, L), BF16),
                pltpu.VMEM((8, 128), F32),
                pltpu.VMEM((W - 1, 8, 128), F32),
                pltpu.VMEM((R, D), BF16),
                pltpu.VMEM((R, D), BF16),
                pltpu.VMEM((G, NX, 2, RB, qw), BF16),
                pltpu.VMEM((G, NX, RB, qw), BF16),
                pltpu.VMEM((6, RB, qw), BF16),
                pltpu.VMEM((6, RB, qw), BF16),
                pltpu.VMEM((G, QT * RB, 128), F32),
                pltpu.VMEM((G, RB, 128), F32),
                pltpu.VMEM((G, QT * RB, 128), F32),
                pltpu.VMEM((W, G, RB, cw), BF16),
                pltpu.VMEM((NG, 8, 2, RG, HB), BF16),
                pltpu.VMEM((NG, 8, RG, HB), BF16),
                pltpu.VMEM((NG, 6, RG, HB), BF16),
                pltpu.VMEM((NG, 6, RG, HB), BF16),
                pltpu.VMEM((NG, 8, RG, 2 * HB), BF16),
                pltpu.VMEM((NG, RG, D), F32),
                pltpu.VMEM((NG, RG, D), BF16),
                pltpu.VMEM((NG, NY - 1, RG // NY, D), BF16),
                pltpu.SemaphoreType.DMA((24,)),
                pltpu.SemaphoreType.DMA((n_messages,)),
                pltpu.SemaphoreType.DMA((n_messages,)),
            ],
            compiler_params=pltpu.CompilerParams(
                collective_id=0, has_side_effects=True, vmem_limit_bytes=VMEM_LIMIT
            ),
        )(
            positions, x_in, ln_attn, ln_mlp, wqkv_t, w_out.reshape(G * cw, D), w_up, w_down, k_t, v_t,
        )
        return x_out, k_new.reshape(RB, G, HD), v_new.reshape(RB, G, HD)

    cache_spec = P(("dp", "tpw"), "tph", None, None)
    new_spec = P(("dp", "tpw"), "tph", None)
    in_specs = (
        P("dp", "tpw"),
        P(None, "tpw"),
        P(None, "tpw"),
        P("tpw", "tph", None, None),
        P("tph", None, None, "tpw"),
        P("tpw", "tph"),
        P("tph", "tpw"),
        cache_spec,
        cache_spec,
        P(("dp", "tpw")),
    )
    out_specs = (P("dp", "tpw"), new_spec, new_spec)
    return jax.shard_map(local_layer, mesh=mesh, in_specs=in_specs, out_specs=out_specs, check_vma=False)
```

```python
import functools
import math

import jax
import jax.numpy as jnp
from jax import lax
from jax.experimental import pallas as pl
from jax.experimental.pallas import tpu as pltpu
from jax.sharding import PartitionSpec as P

LN_EPS = 1e-5
ROPE_BASE = 10000.0
MESH = pl.DeviceIdType.MESH
F32 = jnp.float32
BF16 = jnp.bfloat16
VMEM_LIMIT = 58 << 20
GROUPS_OF_ROWS = 2
NN = (((1,), (0,)), ((), ()))
NT = (((1,), (1,)), ((), ()))
PIECES = ((2, 0), (2, 1), (1, 1), (3, 0), (1, 0), (3, 1), (0, 0), (0, 1))
ARRIVALS = ((0, 0), (0, 1), (3, 0), (1, 1), (3, 1), (1, 0), (2, 0), (2, 1))


def dot(a, b, dims=NN):
    return lax.dot_general(a, b, dims, preferred_element_type=F32)


def layer_kernel(
    W, NY,
    pos_hbm, x_hbm, lna_hbm, lnm_hbm, wqkv_hbm, wout_hbm, wup_hbm, wdn_hbm, k_hbm, v_hbm,
    xout_ref, knew_ref, vnew_ref,
    pos_ref, x_v, lna_v, lnm_v, wqkv_v, wout_v, wup_v, wdn_v, k_v, v_v,
    stat_send, stat_recv, ha_v, hm_v,
    qpart, qsib, qsend, qrecv, qrot, kvrot, ctxs, ctx_all,
    upart, usib, usend, urecv, act_all, acc, ysend, yrecv,
    lsem, ssem, rsem,
):
    NX = W // 2
    R, D = x_v.shape
    NG = GROUPS_OF_ROWS
    RG = R // NG
    RY = RG // NY
    RB = R // W
    G, HD = kvrot.shape[0], k_v.shape[1]
    L = k_v.shape[2]
    QT = qrot.shape[1] // RB
    HB = wup_v.shape[2] // 2
    model_width = float(D * W)

    w = lax.axis_index("tpw")
    y = lax.axis_index("tph")
    c = lax.rem(w, 2)
    x = lax.div(w, 2)
    sib = w + 1 - 2 * c
    right = lax.rem(w + 2, W)
    left = lax.rem(w + W - 2, W)
    opp = lax.rem(w + W // 2, W)

    def chip(o):
        return lax.rem(x + o, NX)

    loads = {}

    def load(name, src, dst):
        cp = pltpu.make_async_copy(src, dst, lsem.at[len(loads)])
        cp.start()
        loads[name] = cp

    load("x", x_hbm, x_v)
    load("pos", pos_hbm, pos_ref)
    load("lna", lna_hbm, lna_v)
    load("lnm", lnm_hbm, lnm_v)
    qw = wqkv_v.shape[1]
    for g in range(G):
        load(("qkv", g), wqkv_hbm.at[pl.ds(g * qw, qw), :], wqkv_v.at[g])
    for i, (o, h) in enumerate(PIECES):
        col = pl.multiple_of((chip(o) * 2 + h) * 2 * HB, 2 * HB)
        load(("up", i), wup_hbm.at[:, pl.ds(col, 2 * HB)], wup_v.at[i])
    load("k", k_hbm, k_v)
    load("v", v_hbm, v_v)
    load("out", wout_hbm, wout_v)
    for i, (o, h) in enumerate(ARRIVALS):
        row = pl.multiple_of((chip(o) * 2 + h) * 2 * HB, 2 * HB)
        load(("down", i), wdn_hbm.at[pl.ds(row, 2 * HB), :], wdn_v.at[i])

    barrier = pltpu.get_barrier_semaphore()
    for i in range(1, W):
        pl.semaphore_signal(barrier, inc=1, device_id={"tpw": lax.rem(w + i, W)}, device_id_type=MESH)
    for i in range(1, NY):
        pl.semaphore_signal(barrier, inc=1, device_id={"tph": lax.rem(y + i, NY)}, device_id_type=MESH)

    sent = []
    messages = {}

    def send(name, src, dst, axis, to):
        i = len(sent)
        cp = pltpu.make_async_remote_copy(
            src_ref=src, dst_ref=dst, send_sem=ssem.at[i], recv_sem=rsem.at[i],
            device_id={axis: to}, device_id_type=MESH,
        )
        cp.start()
        sent.append(cp)
        messages[name] = cp

    def arrived(name):
        messages[name].wait_recv()

    loads["x"].wait()
    xf = x_v[...].astype(F32)
    s1 = jnp.sum(xf, axis=1, keepdims=True)
    s2 = jnp.sum(xf * xf, axis=1, keepdims=True)
    lane = lax.broadcasted_iota(jnp.int32, (R, 128), 1)
    stat_send[...] = jnp.where(lane == 0, s1, jnp.where(lane == 1, s2, 0.0)).T[0:8, :]
    pl.semaphore_wait(barrier, W - 1 + NY - 1)
    for i in range(1, W):
        send(("stat", i), stat_send, stat_recv.at[i - 1], "tpw", lax.rem(w + i, W))

    loads["pos"].wait()
    prow = lax.broadcasted_iota(jnp.int32, (RB, 128), 0)
    plane = lax.broadcasted_iota(jnp.int32, (RB, 128), 1)
    pos = jnp.zeros((RB, 128), jnp.int32)
    for b in range(RB):
        pos = jnp.where(prow == b, pos_ref[b], pos)
    half = HD // 2
    freq = jnp.exp(lax.rem(plane, half).astype(F32) * (-math.log(ROPE_BASE) * 2.0 / HD))
    angle = pos.astype(F32) * freq
    cos_t = jnp.cos(angle)
    first = lax.rem(plane, HD) < half
    sin_t = jnp.where(first, -jnp.sin(angle), jnp.sin(angle))

    for i in range(1, W):
        arrived(("stat", i))
    tot = stat_send[...]
    for i in range(1, W):
        tot = tot + stat_recv[i - 1]
    cols = jnp.concatenate([tot, jnp.zeros((R - 8, R), F32)], axis=0).T
    mean = cols[:, 0:1] / model_width
    var = cols[:, 1:2] / model_width - mean * mean
    rstd = lax.rsqrt(var + LN_EPS)
    loads["lna"].wait()
    loads["lnm"].wait()
    cen = (x_v[...].astype(F32) - mean) * rstd
    ha_v[...] = (cen * lna_v[0:1, :] + lna_v[1:2, :]).astype(BF16)
    hm_v[...] = (cen * lnm_v[0:1, :] + lnm_v[1:2, :]).astype(BF16)

    def tree(tag, own, stage, landing):
        def m1():
            stage[0] = own(2, 0).astype(BF16)
            send((tag, 0), stage.at[0], landing.at[0], "tpw", right)
            stage[1] = own(2, 1).astype(BF16)
            send((tag, 1), stage.at[1], landing.at[1], "tpw", left)

        def m2():
            stage[2] = own(1, 1).astype(BF16)
            send((tag, 2), stage.at[2], landing.at[2], "tpw", right)
            stage[3] = own(3, 0).astype(BF16)
            send((tag, 3), stage.at[3], landing.at[3], "tpw", left)

        def m3():
            arrived((tag, 0))
            stage[4] = (own(1, 0) + landing[0].astype(F32)).astype(BF16)
            send((tag, 4), stage.at[4], landing.at[4], "tpw", right)
            arrived((tag, 1))
            stage[5] = (own(3, 1) + landing[1].astype(F32)).astype(BF16)
            send((tag, 5), stage.at[5], landing.at[5], "tpw", left)

        def total(h):
            a, b = ((3, 4), (2, 5))[h]
            arrived((tag, a))
            arrived((tag, b))
            return own(0, h) + landing[a].astype(F32) + landing[b].astype(F32)

        return m1, m2, m3, total

    def qkv_mm(g):
        loads[("qkv", g)].wait()
        part = dot(ha_v[...], wqkv_v[g], NT).astype(BF16)
        qpart[g] = part.reshape(NX, 2, RB, qw)
        send(("qs", g), qpart.at[g, :, 1 - c], qsib.at[g], "tpw", sib)

    def qkv_own(o, g):
        return qpart[g, chip(o), c].astype(F32) + qsib[g, chip(o)].astype(F32)

    q1, q2, q3, q_total = tree("q", qkv_own, qsend, qrecv)

    def up_mm(r, i):
        if r == 0:
            loads[("up", i)].wait()
        hm = hm_v[r * RG:(r + 1) * RG, :]
        for k in range(2):
            upart[r, i, k] = dot(hm, wup_v[i, :, k * HB:(k + 1) * HB]).astype(BF16)
        send(("us", r, i), upart.at[r, i, 1 - c], usib.at[r, i], "tpw", sib)

    def up_tree(r):
        waited = set()

        def own(o, h):
            i = PIECES.index((o, h))
            if i not in waited:
                arrived(("us", r, i))
                waited.add(i)
            return upart[r, i, c].astype(F32) + usib[r, i].astype(F32)

        return tree(("u", r), own, usend.at[r], urecv.at[r])

    trees = [up_tree(r) for r in range(NG)]
    mine = pl.ds(pl.multiple_of(c * HB, HB), HB)

    def act_slot(r, o, h):
        return act_all.at[r, ARRIVALS.index((o, h)), :, mine]

    def act_send(r, name, o, h, axis_to, to_o):
        send(("a", r, name), act_slot(r, o, h), act_slot(r, to_o, h), "tpw", axis_to)

    def act_first(r, h):
        pre = trees[r][3](h)
        act = 0.5 * pre * (1.0 + lax.erf(pre * (2.0 ** -0.5)))
        act_all[r, ARRIVALS.index((0, h)), :, mine] = act.astype(BF16)
        if h == 0:
            act_send(r, "1r", 0, 0, right, 3)
        else:
            act_send(r, "1l", 0, 1, left, 1)
        act_send(r, ("s", 0, h), 0, h, sib, 0)

    def act_second(r):
        act_send(r, "2r", 0, 1, right, 3)
        act_send(r, "2l", 0, 0, left, 1)

    def act_third(r):
        arrived(("a", r, "1r"))
        act_send(r, "3r", 3, 0, right, 2)
        act_send(r, ("s", 3, 0), 3, 0, sib, 3)
        arrived(("a", r, "1l"))
        act_send(r, "3l", 1, 1, left, 2)
        act_send(r, ("s", 1, 1), 1, 1, sib, 1)

    def act_pass(r, name, o, h):
        arrived(("a", r, name))
        act_send(r, ("s", o, h), o, h, sib, o)

    def down_mm(r, i):
        o, h = ARRIVALS[i]
        arrived(("a", r, ("s", o, h)))
        if r == 0:
            loads[("down", i)].wait()
        part = dot(act_all[r, i], wdn_v[i])
        if i == 0:
            acc[r] = part
        else:
            acc[r] += part

    def rotary(t):
        swapped = jnp.where(first, pltpu.roll(t, 128 - half, 1), pltpu.roll(t, half, 1))
        return (t * cos_t + swapped * sin_t).astype(BF16).astype(F32)

    def attention():
        for g in range(G):
            qkv = q_total(g).astype(BF16).astype(F32)
            for t in range(QT):
                qrot[g, t * RB:(t + 1) * RB, :] = rotary(qkv[:, t * 128:(t + 1) * 128])
            last = qkv[:, QT * 128:]
            kv = jnp.where(plane < HD, rotary(last), last)
            kvrot[g] = kv
            knew_ref[:, g * HD:(g + 1) * HD] = kv[:, :HD].astype(BF16)
            vnew_ref[:, g * HD:(g + 1) * HD] = kv[:, HD:].astype(BF16)
        loads["k"].wait()
        loads["v"].wait()
        scale = HD ** -0.5
        when = lax.broadcasted_iota(jnp.int32, (2 * QT, L), 1)

        def row(b):
            for g in range(G):
                q8 = qrot[g, pl.ds(b, QT, stride=RB), :]
                q = jnp.concatenate([q8[:, :HD], q8[:, HD:]], axis=0)
                kv = kvrot[g, pl.ds(b, 1), :]
                s = dot(q.astype(BF16), k_v[b * G + g]) * scale
                s = jnp.where(when < pos_ref[b], s, -jnp.inf)
                sn = jnp.sum(q * kv[:, :HD], axis=1, keepdims=True) * scale
                m = jnp.maximum(jnp.max(s, axis=1, keepdims=True), sn)
                e = jnp.exp(s - m)
                en = jnp.exp(sn - m)
                rz = 1.0 / (jnp.sum(e, axis=1, keepdims=True) + en)
                wn = (en * rz).astype(BF16).astype(F32)
                ctx = dot((e * rz).astype(BF16), v_v[b * G + g], NT) + wn * kv[:, HD:]
                ctxs[g, pl.ds(b, QT, stride=RB), :] = jnp.concatenate([ctx[:QT], ctx[QT:]], axis=1)

        def rows(i, _):
            for j in range(4):
                row(i * 4 + j)
            return 0

        lax.fori_loop(0, RB // 4, rows, 0)
        for g in range(G):
            for t in range(QT):
                ctx_all[w, g, :, t * 128:(t + 1) * 128] = ctxs[g, t * RB:(t + 1) * RB, :].astype(BF16)

    def ctx_send(name, who, g, to):
        send(("c", name), ctx_all.at[who, g], ctx_all.at[who, g], "tpw", to)

    def ctx_first():
        ctx_send("1r", w, 0, right)
        ctx_send("1l", w, 1, left)
        ctx_send("2r", w, 1, right)
        ctx_send("2l", w, 0, left)
        for g in range(G):
            ctx_send(("s", 0, g), w, g, sib)

    def ctx_third():
        arrived(("c", "1r"))
        ctx_send("3r", left, 0, right)
        ctx_send(("s", 3, 0), left, 0, sib)
        arrived(("c", "1l"))
        ctx_send("3l", right, 1, left)
        ctx_send(("s", 1, 1), right, 1, sib)

    def ctx_rest():
        for name, who, o, g in (("2r", left, 3, 1), ("2l", right, 1, 0), ("3r", opp, 2, 0), ("3l", opp, 2, 1)):
            arrived(("c", name))
            ctx_send(("s", o, g), who, g, sib)

    def attn_mm():
        for o in range(NX):
            for g in range(G):
                arrived(("c", ("s", o, g)))
        loads["out"].wait()
        for g in range(G):
            n = QT * 128
            part = dot(ctx_all[:, g].reshape(R, n), wout_v[g * n:(g + 1) * n, :])
            for r in range(NG):
                acc[r] += part[r * RG:(r + 1) * RG]

    def y_scatter(r):
        ysend[r] = acc[r].astype(BF16)
        for i in range(1, NY):
            to = lax.rem(y + i, NY)
            rows = pl.ds(pl.multiple_of(to * RY, RY), RY)
            send(("y", r, i), ysend.at[r, rows], yrecv.at[r, i - 1], "tph", to)

    def y_gather(r):
        start = pl.multiple_of(y * RY, RY)
        tot = acc[r, pl.ds(start, RY), :]
        for i in range(1, NY):
            arrived(("y", r, i))
            tot = tot + yrecv[r, i - 1].astype(F32)
        rows = pl.ds(pl.multiple_of(r * RG + start, RY), RY)
        xout_ref[rows, :] = (x_v[rows, :].astype(F32) + tot).astype(BF16)
        for i in range(1, NY):
            send(("z", r, i), xout_ref.at[rows, :], xout_ref.at[rows, :], "tph", lax.rem(y + i, NY))

    qkv_mm(0)
    qkv_mm(1)
    up_mm(0, 0)
    up_mm(0, 1)
    for g in range(G):
        arrived(("qs", g))
    q1()
    q2()
    up_mm(0, 2)
    up_mm(0, 3)
    trees[0][0]()
    up_mm(0, 4)
    up_mm(0, 5)
    trees[0][1]()
    q3()
    up_mm(0, 6)
    up_mm(0, 7)
    up_mm(1, 0)
    up_mm(1, 1)
    trees[0][2]()
    up_mm(1, 2)
    up_mm(1, 3)
    trees[1][0]()
    up_mm(1, 4)
    up_mm(1, 5)
    trees[1][1]()
    up_mm(1, 6)
    up_mm(1, 7)
    act_first(0, 0)
    act_first(0, 1)
    trees[1][2]()
    act_second(0)
    attention()
    act_third(0)
    ctx_first()
    act_first(1, 0)
    act_first(1, 1)
    act_second(1)
    ctx_third()
    down_mm(0, 0)
    down_mm(0, 1)
    act_pass(0, "2r", 3, 1)
    act_pass(0, "2l", 1, 0)
    act_pass(0, "3r", 2, 0)
    act_pass(0, "3l", 2, 1)
    act_third(1)
    ctx_rest()
    for i in range(2, 8):
        down_mm(0, i)
    down_mm(1, 0)
    down_mm(1, 1)
    attn_mm()
    y_scatter(0)
    act_pass(1, "2r", 3, 1)
    act_pass(1, "2l", 1, 0)
    for i in range(2, 4):
        down_mm(1, i)
    act_pass(1, "3r", 2, 0)
    act_pass(1, "3l", 2, 1)
    for i in range(4, 8):
        down_mm(1, i)
    y_scatter(1)
    y_gather(0)
    y_gather(1)
    for r in range(NG):
        for i in range(1, NY):
            arrived(("z", r, i))
    for cp in sent:
        cp.wait_send()


def finish_kernel(x_ref, k_ref, v_ref, xout_ref, knew_ref, vnew_ref):
    xout_ref[...] = x_ref[...]
    hd = knew_ref.shape[2]
    for g in range(knew_ref.shape[1]):
        knew_ref[:, g, :] = k_ref[:, g * hd:(g + 1) * hd]
        vnew_ref[:, g, :] = v_ref[:, g * hd:(g + 1) * hd]


def solution(mesh):
    W = mesh.shape["tpw"]
    NY = mesh.shape["tph"]
    if W != 8:
        raise ValueError("tpw")

    def local_layer(x_in, ln_attn, ln_mlp, w_qkv, w_out, w_up, w_down, k_cache, v_cache, positions):
        R, D = x_in.shape
        _, G, S, HD = w_qkv.shape
        F = w_up.shape[1]
        L = k_cache.shape[2]
        RB = R // W
        NX = W // 2
        NG = GROUPS_OF_ROWS
        RG = R // NG
        qw = S * HD
        cw = (S - 2) * HD
        QT = cw // 128
        HB = F // W // 2
        wqkv_t = jnp.transpose(w_qkv, (1, 2, 3, 0)).reshape(G * qw, D)
        k_t = jnp.swapaxes(k_cache, 2, 3).reshape(RB * G, HD, L)
        v_t = jnp.swapaxes(v_cache, 2, 3).reshape(RB * G, HD, L)
        n_messages = 7 + 2 + 6 + NG * 8 + NG * 6 + NG * 14 + 14 + NG * 6
        any_spec = pl.BlockSpec(memory_space=pl.ANY)
        vmem_spec = pl.BlockSpec(memory_space=pltpu.VMEM)
        x_out, k_new, v_new = pl.pallas_call(
            functools.partial(layer_kernel, W, NY),
            name="layer",
            out_shape=(
                pltpu.VMEM((R, D), BF16),
                pltpu.VMEM((RB, G * HD), BF16),
                pltpu.VMEM((RB, G * HD), BF16),
            ),
            in_specs=[any_spec] * 10,
            out_specs=(vmem_spec,) * 3,
            scratch_shapes=[
                pltpu.SMEM((RB,), jnp.int32),
                pltpu.VMEM((R, D), BF16),
                pltpu.VMEM((2, D), F32),
                pltpu.VMEM((2, D), F32),
                pltpu.VMEM((G, qw, D), BF16),
                pltpu.VMEM((G * cw, D), BF16),
                pltpu.VMEM((8, D, 2 * HB), BF16),
                pltpu.VMEM((8, 2 * HB, D), BF16),
                pltpu.VMEM((RB * G, HD, L), BF16),
                pltpu.VMEM((RB * G, HD, L), BF16),
                pltpu.VMEM((8, 128), F32),
                pltpu.VMEM((W - 1, 8, 128), F32),
                pltpu.VMEM((R, D), BF16),
                pltpu.VMEM((R, D), BF16),
                pltpu.VMEM((G, NX, 2, RB, qw), BF16),
                pltpu.VMEM((G, NX, RB, qw), BF16),
                pltpu.VMEM((6, RB, qw), BF16),
                pltpu.VMEM((6, RB, qw), BF16),
                pltpu.VMEM((G, QT * RB, 128), F32),
                pltpu.VMEM((G, RB, 128), F32),
                pltpu.VMEM((G, QT * RB, 128), F32),
                pltpu.VMEM((W, G, RB, cw), BF16),
                pltpu.VMEM((NG, 8, 2, RG, HB), BF16),
                pltpu.VMEM((NG, 8, RG, HB), BF16),
                pltpu.VMEM((NG, 6, RG, HB), BF16),
                pltpu.VMEM((NG, 6, RG, HB), BF16),
                pltpu.VMEM((NG, 8, RG, 2 * HB), BF16),
                pltpu.VMEM((NG, RG, D), F32),
                pltpu.VMEM((NG, RG, D), BF16),
                pltpu.VMEM((NG, NY - 1, RG // NY, D), BF16),
                pltpu.SemaphoreType.DMA((32,)),
                pltpu.SemaphoreType.DMA((n_messages,)),
                pltpu.SemaphoreType.DMA((n_messages,)),
            ],
            compiler_params=pltpu.CompilerParams(
                collective_id=0, has_side_effects=True, vmem_limit_bytes=VMEM_LIMIT
            ),
        )(
            positions, x_in, ln_attn, ln_mlp, wqkv_t, w_out.reshape(G * cw, D), w_up, w_down, k_t, v_t,
        )
        return pl.pallas_call(
            finish_kernel,
            name="finish",
            out_shape=(
                jax.ShapeDtypeStruct((R, D), BF16),
                jax.ShapeDtypeStruct((RB, G, HD), BF16),
                jax.ShapeDtypeStruct((RB, G, HD), BF16),
            ),
            in_specs=[vmem_spec] * 3,
            out_specs=(vmem_spec,) * 3,
        )(*(pltpu.with_memory_space_constraint(a, pltpu.VMEM) for a in (x_out, k_new, v_new)))

    cache_spec = P(("dp", "tpw"), "tph", None, None)
    new_spec = P(("dp", "tpw"), "tph", None)
    in_specs = (
        P("dp", "tpw"),
        P(None, "tpw"),
        P(None, "tpw"),
        P("tpw", "tph", None, None),
        P("tph", None, None, "tpw"),
        P("tpw", "tph"),
        P("tph", "tpw"),
        cache_spec,
        cache_spec,
        P(("dp", "tpw")),
    )
    out_specs = (P("dp", "tpw"), new_spec, new_spec)
    return jax.shard_map(local_layer, mesh=mesh, in_specs=in_specs, out_specs=out_specs, check_vma=False)
```

```python
import functools
import math

import jax
import jax.numpy as jnp
from jax import lax
from jax.experimental import pallas as pl
from jax.experimental.pallas import tpu as pltpu
from jax.sharding import PartitionSpec as P

LN_EPS = 1e-5
ROPE_BASE = 10000.0
MESH = pl.DeviceIdType.MESH
F32 = jnp.float32
BF16 = jnp.bfloat16
VMEM_LIMIT = 58 << 20
GROUPS_OF_ROWS = 2
NN = (((1,), (0,)), ((), ()))
NT = (((1,), (1,)), ((), ()))
PIECES = ((2, 0), (2, 1), (1, 1), (3, 0), (1, 0), (3, 1), (0, 0), (0, 1))
ARRIVALS = ((0, 0), (0, 1), (3, 0), (1, 1), (3, 1), (1, 0), (2, 0), (2, 1))

ORDER = (
    ("qmm", 1), ("qmm", 0), ("umm", 0, 1), ("umm", 0, 2), ("qm", "2r"), ("qm", "1l"),
    ("umm", 0, 0), ("umm", 0, 5), ("um", 0, "1l"), ("qm", "1r"), ("umm", 1, 1), ("um", 0, "2r"),
    ("umm", 1, 3), ("um", 0, "1r"), ("umm", 1, 4), ("umm", 1, 5), ("umm", 0, 4), ("um", 1, "2l"),
    ("umm", 1, 0), ("um", 1, "1l"), ("umm", 0, 6), ("umm", 0, 7), ("umm", 1, 6), ("qm", "3l"),
    ("um", 1, "1r"), ("qm", "2l"), ("umm", 1, 2), ("umm", 0, 3), ("qm", "3r"), ("umm", 1, 7),
    ("um", 0, "3l"), ("um", 1, "2r"), ("um", 0, "2l"), ("um", 0, "3r"), ("um", 1, "3l"), ("um", 1, "3r"),
    ("qt", 1), ("att", 1), ("c", "1l"), ("qt", 0), ("c", "2r"), ("att", 0),
    ("c", "2l"), ("c", "1r"), ("a", 0, "1"), ("a", 0, "2r"), ("dmm", 0, 1), ("a", 0, "0"),
    ("a", 0, "2l"), ("a", 1, "0"), ("a", 1, "1"), ("a", 1, "2r"), ("a", 1, "2l"), ("dmm", 0, 0),
    ("pc", "2r"), ("c", "3l"), ("dmm", 1, 0), ("c", "3r"), ("dmm", 1, 1), ("pc", "2l"),
    ("ap", 0, "2r"), ("a", 0, "3l"), ("dmm", 0, 4), ("a", 0, "3r"), ("dmm", 0, 3), ("ap", 0, "2l"),
    ("dmm", 0, 2), ("a", 1, "3r"), ("dmm", 0, 5), ("a", 1, "3l"), ("dmm", 1, 2), ("ap", 1, "2r"),
    ("dmm", 1, 3), ("ap", 1, "2l"), ("pc", "3r"), ("dmm", 1, 4), ("dmm", 1, 5), ("pc", "3l"),
    ("ap", 0, "3r"), ("ap", 0, "3l"), ("amm",), ("dmm", 0, 6), ("ap", 1, "3r"), ("dmm", 0, 7),
    ("ysc", 0), ("ap", 1, "3l"), ("dmm", 1, 6), ("dmm", 1, 7), ("ysc", 1), ("yga", 0),
    ("yga", 1),
)


def dot(a, b, dims=NN):
    return lax.dot_general(a, b, dims, preferred_element_type=F32)


def layer_kernel(
    W, NY,
    pos_hbm, x_hbm, lna_hbm, lnm_hbm, wqkv_hbm, wout_hbm, wup_hbm, wdn_hbm, k_hbm, v_hbm,
    xout_ref, knew_ref, vnew_ref,
    pos_ref, x_v, lna_v, lnm_v, wqkv_v, wout_v, wup_v, wdn_v, k_v, v_v,
    stat_send, stat_recv, ha_v, hm_v,
    qpart, qsib, qsend, qrecv, qrot, kvrot, ctxs, ctx_all,
    upart, usib, usend, urecv, act_all, acc, ysend, yrecv,
    lsem, ssem, rsem,
):
    NX = W // 2
    R, D = x_v.shape
    NG = GROUPS_OF_ROWS
    RG = R // NG
    RY = RG // NY
    RB = R // W
    G, HD = kvrot.shape[0], k_v.shape[1]
    L = k_v.shape[2]
    QT = qrot.shape[1] // RB
    HB = wup_v.shape[2] // 2
    model_width = float(D * W)

    w = lax.axis_index("tpw")
    y = lax.axis_index("tph")
    c = lax.rem(w, 2)
    x = lax.div(w, 2)
    sib = w + 1 - 2 * c
    right = lax.rem(w + 2, W)
    left = lax.rem(w + W - 2, W)
    opp = lax.rem(w + W // 2, W)

    def chip(o):
        return lax.rem(x + o, NX)

    barrier = pltpu.get_barrier_semaphore()
    for i in range(1, W):
        pl.semaphore_signal(barrier, inc=1, device_id={"tpw": lax.rem(w + i, W)}, device_id_type=MESH)
    for i in range(1, NY):
        pl.semaphore_signal(barrier, inc=1, device_id={"tph": lax.rem(y + i, NY)}, device_id_type=MESH)

    loads = {}

    def load(name, src, dst):
        cp = pltpu.make_async_copy(src, dst, lsem.at[len(loads)])
        cp.start()
        loads[name] = cp

    load("x", x_hbm, x_v)
    load("pos", pos_hbm, pos_ref)
    load("lna", lna_hbm, lna_v)
    load("lnm", lnm_hbm, lnm_v)
    qw = wqkv_v.shape[1]
    for g in range(G):
        load(("qkv", g), wqkv_hbm.at[pl.ds(g * qw, qw), :], wqkv_v.at[g])
    for i, (o, h) in enumerate(PIECES):
        col = pl.multiple_of((chip(o) * 2 + h) * 2 * HB, 2 * HB)
        load(("up", i), wup_hbm.at[:, pl.ds(col, 2 * HB)], wup_v.at[i])
    load("k", k_hbm, k_v)
    load("v", v_hbm, v_v)
    load("out", wout_hbm, wout_v)
    for i, (o, h) in enumerate(ARRIVALS):
        row = pl.multiple_of((chip(o) * 2 + h) * 2 * HB, 2 * HB)
        load(("down", i), wdn_hbm.at[pl.ds(row, 2 * HB), :], wdn_v.at[i])

    sent = []
    messages = {}

    def send(name, src, dst, axis, to):
        i = len(sent)
        cp = pltpu.make_async_remote_copy(
            src_ref=src, dst_ref=dst, send_sem=ssem.at[i], recv_sem=rsem.at[i],
            device_id={axis: to}, device_id_type=MESH,
        )
        cp.start()
        sent.append(cp)
        messages[name] = cp

    seen = set()

    def arrived(name):
        if name not in seen:
            seen.add(name)
            messages[name].wait_recv()

    def need(name):
        if name not in seen:
            seen.add(name)
            loads[name].wait()

    loads["x"].wait()
    xf = x_v[...].astype(F32)
    s1 = jnp.sum(xf, axis=1, keepdims=True)
    s2 = jnp.sum(xf * xf, axis=1, keepdims=True)
    lane = lax.broadcasted_iota(jnp.int32, (R, 128), 1)
    stat_send[...] = jnp.where(lane == 0, s1, jnp.where(lane == 1, s2, 0.0)).T[0:8, :]
    pl.semaphore_wait(barrier, W - 1 + NY - 1)
    for i in range(1, W):
        send(("stat", i), stat_send, stat_recv.at[i - 1], "tpw", lax.rem(w + i, W))

    loads["pos"].wait()
    prow = lax.broadcasted_iota(jnp.int32, (RB, 128), 0)
    plane = lax.broadcasted_iota(jnp.int32, (RB, 128), 1)
    pos = jnp.zeros((RB, 128), jnp.int32)
    for b in range(RB):
        pos = jnp.where(prow == b, pos_ref[b], pos)
    half = HD // 2
    freq = jnp.exp(lax.rem(plane, half).astype(F32) * (-math.log(ROPE_BASE) * 2.0 / HD))
    angle = pos.astype(F32) * freq
    cos_t = jnp.cos(angle)
    first = lax.rem(plane, HD) < half
    sin_t = jnp.where(first, -jnp.sin(angle), jnp.sin(angle))

    for i in range(1, W):
        arrived(("stat", i))
    tot = stat_send[...]
    for i in range(1, W):
        tot = tot + stat_recv[i - 1]
    cols = jnp.concatenate([tot, jnp.zeros((R - 8, R), F32)], axis=0).T
    mean = cols[:, 0:1] / model_width
    var = cols[:, 1:2] / model_width - mean * mean
    rstd = lax.rsqrt(var + LN_EPS)
    loads["lna"].wait()
    loads["lnm"].wait()
    cen = (x_v[...].astype(F32) - mean) * rstd
    ha_v[...] = (cen * lna_v[0:1, :] + lna_v[1:2, :]).astype(BF16)
    hm_v[...] = (cen * lnm_v[0:1, :] + lnm_v[1:2, :]).astype(BF16)

    legs = {
        "1r": (0, 2, 0, None, right), "1l": (1, 2, 1, None, left),
        "2r": (2, 1, 1, None, right), "2l": (3, 3, 0, None, left),
        "3r": (4, 1, 0, 0, right), "3l": (5, 3, 1, 1, left),
    }

    def leg(tag, key, own, stage, landing):
        i, o, h, add, to = legs[key]
        val = own(o, h)
        if add is not None:
            arrived((tag, add))
            val = val + landing[add].astype(F32)
        stage[i] = val.astype(BF16)
        send((tag, i), stage.at[i], landing.at[i], "tpw", to)

    def total(tag, h, own, landing):
        val = own(0, h)
        for i in ((3, 4), (2, 5))[h]:
            arrived((tag, i))
            val = val + landing[i].astype(F32)
        return val

    def qmm(g):
        need(("qkv", g))
        part = dot(ha_v[...], wqkv_v[g], NT).astype(BF16)
        qpart[g] = part.reshape(NX, 2, RB, qw)
        send(("qs", g), qpart.at[g, :, 1 - c], qsib.at[g], "tpw", sib)

    def qkv_own(o, g):
        arrived(("qs", g))
        return qpart[g, chip(o), c].astype(F32) + qsib[g, chip(o)].astype(F32)

    def qm(key):
        leg("q", key, qkv_own, qsend, qrecv)

    def umm(r, i):
        need(("up", i))
        hm = hm_v[r * RG:(r + 1) * RG, :]
        for k in range(2):
            upart[r, i, k] = dot(hm, wup_v[i, :, k * HB:(k + 1) * HB]).astype(BF16)
        send(("us", r, i), upart.at[r, i, 1 - c], usib.at[r, i], "tpw", sib)

    def up_own(r):
        def own(o, h):
            i = PIECES.index((o, h))
            arrived(("us", r, i))
            return upart[r, i, c].astype(F32) + usib[r, i].astype(F32)

        return own

    def um(r, key):
        leg(("u", r), key, up_own(r), usend.at[r], urecv.at[r])

    mine = pl.ds(pl.multiple_of(c * HB, HB), HB)

    def act_send(r, name, o, h, to, to_o):
        src = act_all.at[r, ARRIVALS.index((o, h)), :, mine]
        dst = act_all.at[r, ARRIVALS.index((to_o, h)), :, mine]
        send(("a", r, name), src, dst, "tpw", to)

    def act(r, key):
        if key in ("0", "1"):
            h = int(key)
            pre = total(("u", r), h, up_own(r), urecv.at[r])
            val = 0.5 * pre * (1.0 + lax.erf(pre * (2.0 ** -0.5)))
            act_all[r, ARRIVALS.index((0, h)), :, mine] = val.astype(BF16)
            if h == 0:
                act_send(r, "1r", 0, 0, right, 3)
            else:
                act_send(r, "1l", 0, 1, left, 1)
            act_send(r, ("s", 0, h), 0, h, sib, 0)
        elif key == "2r":
            act_send(r, "2r", 0, 1, right, 3)
        elif key == "2l":
            act_send(r, "2l", 0, 0, left, 1)
        elif key == "3r":
            arrived(("a", r, "1r"))
            act_send(r, "3r", 3, 0, right, 2)
            act_send(r, ("s", 3, 0), 3, 0, sib, 3)
        else:
            arrived(("a", r, "1l"))
            act_send(r, "3l", 1, 1, left, 2)
            act_send(r, ("s", 1, 1), 1, 1, sib, 1)

    def ap(r, key):
        o, h = {"2r": (3, 1), "2l": (1, 0), "3r": (2, 0), "3l": (2, 1)}[key]
        arrived(("a", r, key))
        act_send(r, ("s", o, h), o, h, sib, o)

    begun = set()

    def accumulate(r, part):
        if r in begun:
            acc[r] += part
        else:
            acc[r] = part
            begun.add(r)

    def dmm(r, i):
        o, h = ARRIVALS[i]
        arrived(("a", r, ("s", o, h)))
        need(("down", i))
        accumulate(r, dot(act_all[r, i], wdn_v[i]))

    scale = HD ** -0.5
    when = lax.broadcasted_iota(jnp.int32, (2 * QT, L), 1)

    def rotary(t):
        swapped = jnp.where(first, pltpu.roll(t, 128 - half, 1), pltpu.roll(t, half, 1))
        return (t * cos_t + swapped * sin_t).astype(BF16).astype(F32)

    def qt(g):
        qkv = total("q", g, qkv_own, qrecv).astype(BF16).astype(F32)
        for t in range(QT):
            qrot[g, t * RB:(t + 1) * RB, :] = rotary(qkv[:, t * 128:(t + 1) * 128])
        last = qkv[:, QT * 128:]
        kv = jnp.where(plane < HD, rotary(last), last)
        kvrot[g] = kv
        knew_ref[:, g * HD:(g + 1) * HD] = kv[:, :HD].astype(BF16)
        vnew_ref[:, g * HD:(g + 1) * HD] = kv[:, HD:].astype(BF16)

    def att(g):
        need("k")
        need("v")

        def row(b):
            q8 = qrot[g, pl.ds(b, QT, stride=RB), :]
            q = jnp.concatenate([q8[:, :HD], q8[:, HD:]], axis=0)
            kv = kvrot[g, pl.ds(b, 1), :]
            s = dot(q.astype(BF16), k_v[b * G + g]) * scale
            s = jnp.where(when < pos_ref[b], s, -jnp.inf)
            sn = jnp.sum(q * kv[:, :HD], axis=1, keepdims=True) * scale
            m = jnp.maximum(jnp.max(s, axis=1, keepdims=True), sn)
            e = jnp.exp(s - m)
            en = jnp.exp(sn - m)
            rz = 1.0 / (jnp.sum(e, axis=1, keepdims=True) + en)
            wn = (en * rz).astype(BF16).astype(F32)
            ctx = dot((e * rz).astype(BF16), v_v[b * G + g], NT) + wn * kv[:, HD:]
            ctxs[g, pl.ds(b, QT, stride=RB), :] = jnp.concatenate([ctx[:QT], ctx[QT:]], axis=1)

        def rows(i, _):
            for j in range(8):
                row(i * 8 + j)
            return 0

        lax.fori_loop(0, RB // 8, rows, 0)
        for t in range(QT):
            ctx_all[w, g, :, t * 128:(t + 1) * 128] = ctxs[g, t * RB:(t + 1) * RB, :].astype(BF16)
        send(("c", ("s", 0, g)), ctx_all.at[w, g], ctx_all.at[w, g], "tpw", sib)

    def ctx_send(name, who, g, to):
        send(("c", name), ctx_all.at[who, g], ctx_all.at[who, g], "tpw", to)

    def ctx(key):
        if key == "1r":
            ctx_send("1r", w, 0, right)
        elif key == "1l":
            ctx_send("1l", w, 1, left)
        elif key == "2r":
            ctx_send("2r", w, 1, right)
        elif key == "2l":
            ctx_send("2l", w, 0, left)
        elif key == "3r":
            arrived(("c", "1r"))
            ctx_send("3r", left, 0, right)
            ctx_send(("s", 3, 0), left, 0, sib)
        else:
            arrived(("c", "1l"))
            ctx_send("3l", right, 1, left)
            ctx_send(("s", 1, 1), right, 1, sib)

    def pc(key):
        who, o, g = {"2r": (left, 3, 1), "2l": (right, 1, 0), "3r": (opp, 2, 0), "3l": (opp, 2, 1)}[key]
        arrived(("c", key))
        ctx_send(("s", o, g), who, g, sib)

    def amm():
        for o in range(NX):
            for g in range(G):
                arrived(("c", ("s", o, g)))
        need("out")
        n = QT * 128
        for g in range(G):
            part = dot(ctx_all[:, g].reshape(R, n), wout_v[g * n:(g + 1) * n, :])
            for r in range(NG):
                accumulate(r, part[r * RG:(r + 1) * RG])

    def ysc(r):
        ysend[r] = acc[r].astype(BF16)
        for i in (2, 1, 3):
            to = lax.rem(y + i, NY)
            rows = pl.ds(pl.multiple_of(to * RY, RY), RY)
            send(("y", r, i), ysend.at[r, rows], yrecv.at[r, i - 1], "tph", to)

    def yga(r):
        start = pl.multiple_of(y * RY, RY)
        tot = acc[r, pl.ds(start, RY), :]
        for i in range(1, NY):
            arrived(("y", r, i))
            tot = tot + yrecv[r, i - 1].astype(F32)
        rows = pl.ds(pl.multiple_of(r * RG + start, RY), RY)
        xout_ref[rows, :] = (x_v[rows, :].astype(F32) + tot).astype(BF16)
        for i in (2, 1, 3):
            send(("z", r, i), xout_ref.at[rows, :], xout_ref.at[rows, :], "tph", lax.rem(y + i, NY))

    steps = {
        "qmm": qmm, "qm": qm, "umm": umm, "um": um, "a": act, "ap": ap, "dmm": dmm, "qt": qt, "att": att,
        "c": ctx, "pc": pc, "amm": amm, "ysc": ysc, "yga": yga,
    }
    for step in ORDER:
        steps[step[0]](*step[1:])
    for name in messages:
        arrived(name)
    for cp in sent:
        cp.wait_send()


def finish_kernel(x_ref, k_ref, v_ref, xout_ref, knew_ref, vnew_ref):
    xout_ref[...] = x_ref[...]
    hd = knew_ref.shape[2]
    for g in range(knew_ref.shape[1]):
        knew_ref[:, g, :] = k_ref[:, g * hd:(g + 1) * hd]
        vnew_ref[:, g, :] = v_ref[:, g * hd:(g + 1) * hd]


def solution(mesh):
    W = mesh.shape["tpw"]
    NY = mesh.shape["tph"]
    if W != 8:
        raise ValueError("tpw")

    def local_layer(x_in, ln_attn, ln_mlp, w_qkv, w_out, w_up, w_down, k_cache, v_cache, positions):
        R, D = x_in.shape
        _, G, S, HD = w_qkv.shape
        F = w_up.shape[1]
        L = k_cache.shape[2]
        RB = R // W
        NX = W // 2
        NG = GROUPS_OF_ROWS
        RG = R // NG
        qw = S * HD
        cw = (S - 2) * HD
        QT = cw // 128
        HB = F // W // 2
        wqkv_t = jnp.transpose(w_qkv, (1, 2, 3, 0)).reshape(G * qw, D)
        k_t = jnp.swapaxes(k_cache, 2, 3).reshape(RB * G, HD, L)
        v_t = jnp.swapaxes(v_cache, 2, 3).reshape(RB * G, HD, L)
        n_messages = 7 + 2 + 6 + NG * 8 + NG * 6 + NG * 14 + 14 + NG * 6
        any_spec = pl.BlockSpec(memory_space=pl.ANY)
        vmem_spec = pl.BlockSpec(memory_space=pltpu.VMEM)
        x_out, k_new, v_new = pl.pallas_call(
            functools.partial(layer_kernel, W, NY),
            name="layer",
            out_shape=(
                pltpu.VMEM((R, D), BF16),
                pltpu.VMEM((RB, G * HD), BF16),
                pltpu.VMEM((RB, G * HD), BF16),
            ),
            in_specs=[any_spec] * 10,
            out_specs=(vmem_spec,) * 3,
            scratch_shapes=[
                pltpu.SMEM((RB,), jnp.int32),
                pltpu.VMEM((R, D), BF16),
                pltpu.VMEM((2, D), F32),
                pltpu.VMEM((2, D), F32),
                pltpu.VMEM((G, qw, D), BF16),
                pltpu.VMEM((G * cw, D), BF16),
                pltpu.VMEM((8, D, 2 * HB), BF16),
                pltpu.VMEM((8, 2 * HB, D), BF16),
                pltpu.VMEM((RB * G, HD, L), BF16),
                pltpu.VMEM((RB * G, HD, L), BF16),
                pltpu.VMEM((8, 128), F32),
                pltpu.VMEM((W - 1, 8, 128), F32),
                pltpu.VMEM((R, D), BF16),
                pltpu.VMEM((R, D), BF16),
                pltpu.VMEM((G, NX, 2, RB, qw), BF16),
                pltpu.VMEM((G, NX, RB, qw), BF16),
                pltpu.VMEM((6, RB, qw), BF16),
                pltpu.VMEM((6, RB, qw), BF16),
                pltpu.VMEM((G, QT * RB, 128), F32),
                pltpu.VMEM((G, RB, 128), F32),
                pltpu.VMEM((G, QT * RB, 128), F32),
                pltpu.VMEM((W, G, RB, cw), BF16),
                pltpu.VMEM((NG, 8, 2, RG, HB), BF16),
                pltpu.VMEM((NG, 8, RG, HB), BF16),
                pltpu.VMEM((NG, 6, RG, HB), BF16),
                pltpu.VMEM((NG, 6, RG, HB), BF16),
                pltpu.VMEM((NG, 8, RG, 2 * HB), BF16),
                pltpu.VMEM((NG, RG, D), F32),
                pltpu.VMEM((NG, RG, D), BF16),
                pltpu.VMEM((NG, NY - 1, RG // NY, D), BF16),
                pltpu.SemaphoreType.DMA((32,)),
                pltpu.SemaphoreType.DMA((n_messages,)),
                pltpu.SemaphoreType.DMA((n_messages,)),
            ],
            compiler_params=pltpu.CompilerParams(
                collective_id=0, has_side_effects=True, vmem_limit_bytes=VMEM_LIMIT
            ),
        )(
            positions, x_in, ln_attn, ln_mlp, wqkv_t, w_out.reshape(G * cw, D), w_up, w_down, k_t, v_t,
        )
        return pl.pallas_call(
            finish_kernel,
            name="finish",
            out_shape=(
                jax.ShapeDtypeStruct((R, D), BF16),
                jax.ShapeDtypeStruct((RB, G, HD), BF16),
                jax.ShapeDtypeStruct((RB, G, HD), BF16),
            ),
            in_specs=[vmem_spec] * 3,
            out_specs=(vmem_spec,) * 3,
        )(*(pltpu.with_memory_space_constraint(a, pltpu.VMEM) for a in (x_out, k_new, v_new)))

    cache_spec = P(("dp", "tpw"), "tph", None, None)
    new_spec = P(("dp", "tpw"), "tph", None)
    in_specs = (
        P("dp", "tpw"),
        P(None, "tpw"),
        P(None, "tpw"),
        P("tpw", "tph", None, None),
        P("tph", None, None, "tpw"),
        P("tpw", "tph"),
        P("tph", "tpw"),
        cache_spec,
        cache_spec,
        P(("dp", "tpw")),
    )
    out_specs = (P("dp", "tpw"), new_spec, new_spec)
    return jax.shard_map(local_layer, mesh=mesh, in_specs=in_specs, out_specs=out_specs, check_vma=False)
```

```python
import functools
import math

import jax
import jax.numpy as jnp
from jax import lax
from jax.experimental import pallas as pl
from jax.experimental.pallas import tpu as pltpu
from jax.sharding import PartitionSpec as P

LN_EPS = 1e-5
ROPE_BASE = 10000.0
MESH = pl.DeviceIdType.MESH
F32 = jnp.float32
BF16 = jnp.bfloat16
VMEM_LIMIT = 58 << 20
GROUPS_OF_ROWS = 2
NN = (((1,), (0,)), ((), ()))
NT = (((1,), (1,)), ((), ()))
PIECES = ((2, 0), (2, 1), (1, 1), (3, 0), (1, 0), (3, 1), (0, 0), (0, 1))
ARRIVALS = ((0, 0), (0, 1), (3, 0), (1, 1), (3, 1), (1, 0), (2, 0), (2, 1))

LOADS = (
    (("up", 1), ("up", 2),),
    (("up", 0), ("up", 5), ("up", 3),),
    (("up", 4), ("up", 6), ("up", 7),),
    (("kv",), ("down", 1), ("down", 0), ("out",), ("down", 4), ("down", 3), ("down", 2), ("down", 5), ("down", 6), ("down", 7),),
)
ORDER = (
    ("qmm", 1), ("qmm", 0), ("umm", 0, 1), ("umm", 0, 2), ("qm", "2r"), ("qm", "1l"),
    ("umm", 0, 0), ("umm", 0, 5), ("um", 0, "1l"), ("qm", "1r"), ("umm", 1, 1), ("um", 0, "2r"),
    ("umm", 1, 3), ("um", 0, "1r"), ("umm", 1, 4), ("umm", 1, 5), ("umm", 0, 4), ("um", 1, "2l"),
    ("umm", 1, 0), ("um", 1, "1l"), ("umm", 0, 6), ("umm", 0, 7), ("umm", 1, 6), ("qm", "3l"),
    ("um", 1, "1r"), ("qm", "2l"), ("umm", 1, 2), ("umm", 0, 3), ("qm", "3r"), ("umm", 1, 7),
    ("um", 0, "3l"), ("um", 1, "2r"), ("um", 0, "2l"), ("um", 0, "3r"), ("um", 1, "3l"), ("um", 1, "3r"),
    ("qt", 1), ("att", 1), ("c", "1l"), ("qt", 0), ("c", "2r"), ("att", 0),
    ("c", "2l"), ("c", "1r"), ("a", 0, "1"), ("a", 0, "2r"), ("dmm", 0, 1), ("a", 0, "0"),
    ("a", 0, "2l"), ("a", 1, "0"), ("a", 1, "1"), ("a", 1, "2r"), ("a", 1, "2l"), ("dmm", 0, 0),
    ("pc", "2r"), ("c", "3l"), ("dmm", 1, 0), ("c", "3r"), ("dmm", 1, 1), ("pc", "2l"),
    ("ap", 0, "2r"), ("a", 0, "3l"), ("dmm", 0, 4), ("a", 0, "3r"), ("dmm", 0, 3), ("ap", 0, "2l"),
    ("dmm", 0, 2), ("a", 1, "3r"), ("dmm", 0, 5), ("a", 1, "3l"), ("dmm", 1, 2), ("ap", 1, "2r"),
    ("dmm", 1, 3), ("ap", 1, "2l"), ("pc", "3r"), ("dmm", 1, 4), ("dmm", 1, 5), ("pc", "3l"),
    ("ap", 0, "3r"), ("ap", 0, "3l"), ("amm",), ("dmm", 0, 6), ("ap", 1, "3r"), ("dmm", 0, 7),
    ("ysc", 0), ("ap", 1, "3l"), ("dmm", 1, 6), ("dmm", 1, 7), ("ysc", 1), ("yga", 0),
    ("yga", 1),
)


def dot(a, b, dims=NN):
    return lax.dot_general(a, b, dims, preferred_element_type=F32)


def layer_kernel(
    W, NY,
    pos_hbm, x_hbm, lna_hbm, lnm_hbm, wqkv_hbm, wout_hbm, wup_hbm, wdn_hbm, k_hbm, v_hbm,
    xout_ref, knew_ref, vnew_ref,
    pos_ref, x_v, lna_v, lnm_v, wqkv_v, wout_v, wup_v, wdn_v, k_v, v_v,
    stat_send, stat_recv, ha_v, hm_v,
    qpart, qsib, qsend, qrecv, qrot, kvrot, ctxs, ctx_all,
    upart, usib, usend, urecv, act_all, acc, ysend, yrecv,
    lsem, ssem, rsem,
):
    NX = W // 2
    R, D = x_v.shape
    NG = GROUPS_OF_ROWS
    RG = R // NG
    RY = RG // NY
    RB = R // W
    G, HD = kvrot.shape[0], k_v.shape[1]
    L = k_v.shape[2]
    QT = qrot.shape[1] // RB
    HB = wup_v.shape[2] // 2
    model_width = float(D * W)

    w = lax.axis_index("tpw")
    y = lax.axis_index("tph")
    c = lax.rem(w, 2)
    x = lax.div(w, 2)
    sib = w + 1 - 2 * c
    right = lax.rem(w + 2, W)
    left = lax.rem(w + W - 2, W)
    opp = lax.rem(w + W // 2, W)

    def chip(o):
        return lax.rem(x + o, NX)

    barrier = pltpu.get_barrier_semaphore()
    for i in range(1, W):
        pl.semaphore_signal(barrier, inc=1, device_id={"tpw": lax.rem(w + i, W)}, device_id_type=MESH)
    for i in range(1, NY):
        pl.semaphore_signal(barrier, inc=1, device_id={"tph": lax.rem(y + i, NY)}, device_id_type=MESH)

    loads = {}

    def load(name, src, dst):
        cp = pltpu.make_async_copy(src, dst, lsem.at[len(loads)])
        cp.start()
        loads[name] = cp

    qw = wqkv_v.shape[1]

    def load_up(i):
        o, h = PIECES[i]
        col = pl.multiple_of((chip(o) * 2 + h) * 2 * HB, 2 * HB)
        load(("up", i), wup_hbm.at[:, pl.ds(col, 2 * HB)], wup_v.at[i])

    def load_down(i):
        o, h = ARRIVALS[i]
        row = pl.multiple_of((chip(o) * 2 + h) * 2 * HB, 2 * HB)
        load(("down", i), wdn_hbm.at[pl.ds(row, 2 * HB), :], wdn_v.at[i])

    def ld(key, *index):
        if key == "up":
            load_up(*index)
        elif key == "down":
            load_down(*index)
        elif key == "kv":
            load("k", k_hbm, k_v)
            load("v", v_hbm, v_v)
        else:
            load("out", wout_hbm, wout_v)

    load("x", x_hbm, x_v)
    load("pos", pos_hbm, pos_ref)
    load("lna", lna_hbm, lna_v)
    load("lnm", lnm_hbm, lnm_v)
    for g in range(G):
        load(("qkv", g), wqkv_hbm.at[pl.ds(g * qw, qw), :], wqkv_v.at[g])
    for step in LOADS[0]:
        ld(*step)

    sent = []
    messages = {}

    def send(name, src, dst, axis, to):
        i = len(sent)
        cp = pltpu.make_async_remote_copy(
            src_ref=src, dst_ref=dst, send_sem=ssem.at[i], recv_sem=rsem.at[i],
            device_id={axis: to}, device_id_type=MESH,
        )
        cp.start()
        sent.append(cp)
        messages[name] = cp

    seen = set()

    def arrived(name):
        if name not in seen:
            seen.add(name)
            messages[name].wait_recv()

    def need(name):
        if name not in seen:
            seen.add(name)
            loads[name].wait()

    loads["x"].wait()
    xf = x_v[...].astype(F32)
    s1 = jnp.sum(xf, axis=1, keepdims=True)
    s2 = jnp.sum(xf * xf, axis=1, keepdims=True)
    lane = lax.broadcasted_iota(jnp.int32, (R, 128), 1)
    stat_send[...] = jnp.where(lane == 0, s1, jnp.where(lane == 1, s2, 0.0)).T[0:8, :]
    pl.semaphore_wait(barrier, W - 1 + NY - 1)
    for i in range(1, W):
        send(("stat", i), stat_send, stat_recv.at[i - 1], "tpw", lax.rem(w + i, W))

    for step in LOADS[1]:
        ld(*step)

    loads["pos"].wait()
    prow = lax.broadcasted_iota(jnp.int32, (RB, 128), 0)
    plane = lax.broadcasted_iota(jnp.int32, (RB, 128), 1)
    pos = jnp.zeros((RB, 128), jnp.int32)
    for b in range(RB):
        pos = jnp.where(prow == b, pos_ref[b], pos)
    half = HD // 2
    freq = jnp.exp(lax.rem(plane, half).astype(F32) * (-math.log(ROPE_BASE) * 2.0 / HD))
    angle = pos.astype(F32) * freq
    cos_t = jnp.cos(angle)
    first = lax.rem(plane, HD) < half
    sin_t = jnp.where(first, -jnp.sin(angle), jnp.sin(angle))

    for i in range(1, W):
        arrived(("stat", i))
    tot = stat_send[...]
    for i in range(1, W):
        tot = tot + stat_recv[i - 1]
    cols = jnp.concatenate([tot, jnp.zeros((R - 8, R), F32)], axis=0).T
    mean = cols[:, 0:1] / model_width
    var = cols[:, 1:2] / model_width - mean * mean
    rstd = lax.rsqrt(var + LN_EPS)
    loads["lna"].wait()
    loads["lnm"].wait()
    cen = (x_v[...].astype(F32) - mean) * rstd
    ha_v[...] = (cen * lna_v[0:1, :] + lna_v[1:2, :]).astype(BF16)
    hm_v[...] = (cen * lnm_v[0:1, :] + lnm_v[1:2, :]).astype(BF16)

    for step in LOADS[2]:
        ld(*step)

    legs = {
        "1r": (0, 2, 0, None, right), "1l": (1, 2, 1, None, left),
        "2r": (2, 1, 1, None, right), "2l": (3, 3, 0, None, left),
        "3r": (4, 1, 0, 0, right), "3l": (5, 3, 1, 1, left),
    }

    def leg(tag, key, own, stage, landing):
        i, o, h, add, to = legs[key]
        val = own(o, h)
        if add is not None:
            arrived((tag, add))
            val = val + landing[add].astype(F32)
        stage[i] = val.astype(BF16)
        send((tag, i), stage.at[i], landing.at[i], "tpw", to)

    def total(tag, h, own, landing):
        val = own(0, h)
        for i in ((3, 4), (2, 5))[h]:
            arrived((tag, i))
            val = val + landing[i].astype(F32)
        return val

    def qmm(g):
        need(("qkv", g))
        part = dot(ha_v[...], wqkv_v[g], NT).astype(BF16)
        qpart[g] = part.reshape(NX, 2, RB, qw)
        send(("qs", g), qpart.at[g, :, 1 - c], qsib.at[g], "tpw", sib)

    def qkv_own(o, g):
        arrived(("qs", g))
        return qpart[g, chip(o), c].astype(F32) + qsib[g, chip(o)].astype(F32)

    def qm(key):
        leg("q", key, qkv_own, qsend, qrecv)

    def umm(r, i):
        need(("up", i))
        hm = hm_v[r * RG:(r + 1) * RG, :]
        for k in range(2):
            upart[r, i, k] = dot(hm, wup_v[i, :, k * HB:(k + 1) * HB]).astype(BF16)
        send(("us", r, i), upart.at[r, i, 1 - c], usib.at[r, i], "tpw", sib)

    def up_own(r):
        def own(o, h):
            i = PIECES.index((o, h))
            arrived(("us", r, i))
            return upart[r, i, c].astype(F32) + usib[r, i].astype(F32)

        return own

    def um(r, key):
        leg(("u", r), key, up_own(r), usend.at[r], urecv.at[r])

    mine = pl.ds(pl.multiple_of(c * HB, HB), HB)

    def act_send(r, name, o, h, to, to_o):
        src = act_all.at[r, ARRIVALS.index((o, h)), :, mine]
        dst = act_all.at[r, ARRIVALS.index((to_o, h)), :, mine]
        send(("a", r, name), src, dst, "tpw", to)

    def act(r, key):
        if key in ("0", "1"):
            h = int(key)
            pre = total(("u", r), h, up_own(r), urecv.at[r])
            val = 0.5 * pre * (1.0 + lax.erf(pre * (2.0 ** -0.5)))
            act_all[r, ARRIVALS.index((0, h)), :, mine] = val.astype(BF16)
            if h == 0:
                act_send(r, "1r", 0, 0, right, 3)
            else:
                act_send(r, "1l", 0, 1, left, 1)
            act_send(r, ("s", 0, h), 0, h, sib, 0)
        elif key == "2r":
            act_send(r, "2r", 0, 1, right, 3)
        elif key == "2l":
            act_send(r, "2l", 0, 0, left, 1)
        elif key == "3r":
            arrived(("a", r, "1r"))
            act_send(r, "3r", 3, 0, right, 2)
            act_send(r, ("s", 3, 0), 3, 0, sib, 3)
        else:
            arrived(("a", r, "1l"))
            act_send(r, "3l", 1, 1, left, 2)
            act_send(r, ("s", 1, 1), 1, 1, sib, 1)

    def ap(r, key):
        o, h = {"2r": (3, 1), "2l": (1, 0), "3r": (2, 0), "3l": (2, 1)}[key]
        arrived(("a", r, key))
        act_send(r, ("s", o, h), o, h, sib, o)

    begun = set()

    def accumulate(r, part):
        if r in begun:
            acc[r] += part
        else:
            acc[r] = part
            begun.add(r)

    def dmm(r, i):
        o, h = ARRIVALS[i]
        arrived(("a", r, ("s", o, h)))
        need(("down", i))
        accumulate(r, dot(act_all[r, i], wdn_v[i]))

    scale = HD ** -0.5
    when = lax.broadcasted_iota(jnp.int32, (2 * QT, L), 1)

    def rotary(t):
        swapped = jnp.where(first, pltpu.roll(t, 128 - half, 1), pltpu.roll(t, half, 1))
        return (t * cos_t + swapped * sin_t).astype(BF16).astype(F32)

    def qt(g):
        qkv = total("q", g, qkv_own, qrecv).astype(BF16).astype(F32)
        for t in range(QT):
            qrot[g, t * RB:(t + 1) * RB, :] = rotary(qkv[:, t * 128:(t + 1) * 128])
        last = qkv[:, QT * 128:]
        kv = jnp.where(plane < HD, rotary(last), last)
        kvrot[g] = kv
        knew_ref[:, g * HD:(g + 1) * HD] = kv[:, :HD].astype(BF16)
        vnew_ref[:, g * HD:(g + 1) * HD] = kv[:, HD:].astype(BF16)

    def att(g):
        need("k")
        need("v")

        def row(b):
            q8 = qrot[g, pl.ds(b, QT, stride=RB), :]
            q = jnp.concatenate([q8[:, :HD], q8[:, HD:]], axis=0)
            kv = kvrot[g, pl.ds(b, 1), :]
            s = dot(q.astype(BF16), k_v[b * G + g]) * scale
            s = jnp.where(when < pos_ref[b], s, -jnp.inf)
            sn = jnp.sum(q * kv[:, :HD], axis=1, keepdims=True) * scale
            m = jnp.maximum(jnp.max(s, axis=1, keepdims=True), sn)
            e = jnp.exp(s - m)
            en = jnp.exp(sn - m)
            rz = 1.0 / (jnp.sum(e, axis=1, keepdims=True) + en)
            wn = (en * rz).astype(BF16).astype(F32)
            ctx = dot((e * rz).astype(BF16), v_v[b * G + g], NT) + wn * kv[:, HD:]
            ctxs[g, pl.ds(b, QT, stride=RB), :] = jnp.concatenate([ctx[:QT], ctx[QT:]], axis=1)

        def rows(i, _):
            for j in range(8):
                row(i * 8 + j)
            return 0

        lax.fori_loop(0, RB // 8, rows, 0)
        for t in range(QT):
            ctx_all[w, g, :, t * 128:(t + 1) * 128] = ctxs[g, t * RB:(t + 1) * RB, :].astype(BF16)
        send(("c", ("s", 0, g)), ctx_all.at[w, g], ctx_all.at[w, g], "tpw", sib)

    def ctx_send(name, who, g, to):
        send(("c", name), ctx_all.at[who, g], ctx_all.at[who, g], "tpw", to)

    def ctx(key):
        if key == "1r":
            ctx_send("1r", w, 0, right)
        elif key == "1l":
            ctx_send("1l", w, 1, left)
        elif key == "2r":
            ctx_send("2r", w, 1, right)
        elif key == "2l":
            ctx_send("2l", w, 0, left)
        elif key == "3r":
            arrived(("c", "1r"))
            ctx_send("3r", left, 0, right)
            ctx_send(("s", 3, 0), left, 0, sib)
        else:
            arrived(("c", "1l"))
            ctx_send("3l", right, 1, left)
            ctx_send(("s", 1, 1), right, 1, sib)

    def pc(key):
        who, o, g = {"2r": (left, 3, 1), "2l": (right, 1, 0), "3r": (opp, 2, 0), "3l": (opp, 2, 1)}[key]
        arrived(("c", key))
        ctx_send(("s", o, g), who, g, sib)

    def amm():
        for o in range(NX):
            for g in range(G):
                arrived(("c", ("s", o, g)))
        need("out")
        n = QT * 128
        for g in range(G):
            part = dot(ctx_all[:, g].reshape(R, n), wout_v[g * n:(g + 1) * n, :])
            for r in range(NG):
                accumulate(r, part[r * RG:(r + 1) * RG])

    def ysc(r):
        ysend[r] = acc[r].astype(BF16)
        for i in (2, 1, 3):
            to = lax.rem(y + i, NY)
            rows = pl.ds(pl.multiple_of(to * RY, RY), RY)
            send(("y", r, i), ysend.at[r, rows], yrecv.at[r, i - 1], "tph", to)

    def yga(r):
        start = pl.multiple_of(y * RY, RY)
        tot = acc[r, pl.ds(start, RY), :]
        for i in range(1, NY):
            arrived(("y", r, i))
            tot = tot + yrecv[r, i - 1].astype(F32)
        rows = pl.ds(pl.multiple_of(r * RG + start, RY), RY)
        xout_ref[rows, :] = (x_v[rows, :].astype(F32) + tot).astype(BF16)
        for i in (2, 1, 3):
            send(("z", r, i), xout_ref.at[rows, :], xout_ref.at[rows, :], "tph", lax.rem(y + i, NY))

    steps = {
        "qmm": qmm, "qm": qm, "umm": umm, "um": um, "a": act, "ap": ap, "dmm": dmm, "qt": qt, "att": att,
        "c": ctx, "pc": pc, "amm": amm, "ysc": ysc, "yga": yga,
    }
    later = list(LOADS[3])
    for step in ORDER:
        steps[step[0]](*step[1:])
        if later and step[0] == "umm":
            ld(*later.pop(0))
    for name in messages:
        arrived(name)
    for cp in sent:
        cp.wait_send()


def finish_kernel(x_ref, k_ref, v_ref, xout_ref, knew_ref, vnew_ref):
    xout_ref[...] = x_ref[...]
    hd = knew_ref.shape[2]
    for g in range(knew_ref.shape[1]):
        knew_ref[:, g, :] = k_ref[:, g * hd:(g + 1) * hd]
        vnew_ref[:, g, :] = v_ref[:, g * hd:(g + 1) * hd]


def solution(mesh):
    W = mesh.shape["tpw"]
    NY = mesh.shape["tph"]
    if W != 8:
        raise ValueError("tpw")

    def local_layer(x_in, ln_attn, ln_mlp, w_qkv, w_out, w_up, w_down, k_cache, v_cache, positions):
        R, D = x_in.shape
        _, G, S, HD = w_qkv.shape
        F = w_up.shape[1]
        L = k_cache.shape[2]
        RB = R // W
        NX = W // 2
        NG = GROUPS_OF_ROWS
        RG = R // NG
        qw = S * HD
        cw = (S - 2) * HD
        QT = cw // 128
        HB = F // W // 2
        wqkv_t = jnp.transpose(w_qkv, (1, 2, 3, 0)).reshape(G * qw, D)
        k_t = jnp.swapaxes(k_cache, 2, 3).reshape(RB * G, HD, L)
        v_t = jnp.swapaxes(v_cache, 2, 3).reshape(RB * G, HD, L)
        n_messages = 7 + 2 + 6 + NG * 8 + NG * 6 + NG * 14 + 14 + NG * 6
        any_spec = pl.BlockSpec(memory_space=pl.ANY)
        vmem_spec = pl.BlockSpec(memory_space=pltpu.VMEM)
        x_out, k_new, v_new = pl.pallas_call(
            functools.partial(layer_kernel, W, NY),
            name="layer",
            out_shape=(
                pltpu.VMEM((R, D), BF16),
                pltpu.VMEM((RB, G * HD), BF16),
                pltpu.VMEM((RB, G * HD), BF16),
            ),
            in_specs=[any_spec] * 10,
            out_specs=(vmem_spec,) * 3,
            scratch_shapes=[
                pltpu.SMEM((RB,), jnp.int32),
                pltpu.VMEM((R, D), BF16),
                pltpu.VMEM((2, D), F32),
                pltpu.VMEM((2, D), F32),
                pltpu.VMEM((G, qw, D), BF16),
                pltpu.VMEM((G * cw, D), BF16),
                pltpu.VMEM((8, D, 2 * HB), BF16),
                pltpu.VMEM((8, 2 * HB, D), BF16),
                pltpu.VMEM((RB * G, HD, L), BF16),
                pltpu.VMEM((RB * G, HD, L), BF16),
                pltpu.VMEM((8, 128), F32),
                pltpu.VMEM((W - 1, 8, 128), F32),
                pltpu.VMEM((R, D), BF16),
                pltpu.VMEM((R, D), BF16),
                pltpu.VMEM((G, NX, 2, RB, qw), BF16),
                pltpu.VMEM((G, NX, RB, qw), BF16),
                pltpu.VMEM((6, RB, qw), BF16),
                pltpu.VMEM((6, RB, qw), BF16),
                pltpu.VMEM((G, QT * RB, 128), F32),
                pltpu.VMEM((G, RB, 128), F32),
                pltpu.VMEM((G, QT * RB, 128), F32),
                pltpu.VMEM((W, G, RB, cw), BF16),
                pltpu.VMEM((NG, 8, 2, RG, HB), BF16),
                pltpu.VMEM((NG, 8, RG, HB), BF16),
                pltpu.VMEM((NG, 6, RG, HB), BF16),
                pltpu.VMEM((NG, 6, RG, HB), BF16),
                pltpu.VMEM((NG, 8, RG, 2 * HB), BF16),
                pltpu.VMEM((NG, RG, D), F32),
                pltpu.VMEM((NG, RG, D), BF16),
                pltpu.VMEM((NG, NY - 1, RG // NY, D), BF16),
                pltpu.SemaphoreType.DMA((32,)),
                pltpu.SemaphoreType.DMA((n_messages,)),
                pltpu.SemaphoreType.DMA((n_messages,)),
            ],
            compiler_params=pltpu.CompilerParams(
                collective_id=0, has_side_effects=True, vmem_limit_bytes=VMEM_LIMIT
            ),
        )(
            positions, x_in, ln_attn, ln_mlp, wqkv_t, w_out.reshape(G * cw, D), w_up, w_down, k_t, v_t,
        )
        return pl.pallas_call(
            finish_kernel,
            name="finish",
            out_shape=(
                jax.ShapeDtypeStruct((R, D), BF16),
                jax.ShapeDtypeStruct((RB, G, HD), BF16),
                jax.ShapeDtypeStruct((RB, G, HD), BF16),
            ),
            in_specs=[vmem_spec] * 3,
            out_specs=(vmem_spec,) * 3,
        )(*(pltpu.with_memory_space_constraint(a, pltpu.VMEM) for a in (x_out, k_new, v_new)))

    cache_spec = P(("dp", "tpw"), "tph", None, None)
    new_spec = P(("dp", "tpw"), "tph", None)
    in_specs = (
        P("dp", "tpw"),
        P(None, "tpw"),
        P(None, "tpw"),
        P("tpw", "tph", None, None),
        P("tph", None, None, "tpw"),
        P("tpw", "tph"),
        P("tph", "tpw"),
        cache_spec,
        cache_spec,
        P(("dp", "tpw")),
    )
    out_specs = (P("dp", "tpw"), new_spec, new_spec)
    return jax.shard_map(local_layer, mesh=mesh, in_specs=in_specs, out_specs=out_specs, check_vma=False)
```

```python
import functools
import math

import jax
import jax.numpy as jnp
from jax import lax
from jax.experimental import pallas as pl
from jax.experimental.pallas import tpu as pltpu
from jax.sharding import PartitionSpec as P

LN_EPS = 1e-5
ROPE_BASE = 10000.0
MESH = pl.DeviceIdType.MESH
F32 = jnp.float32
BF16 = jnp.bfloat16
VMEM_LIMIT = 58 << 20
GROUPS_OF_ROWS = 1
NN = (((1,), (0,)), ((), ()))
NT = (((1,), (1,)), ((), ()))
PIECES = ((2, 0), (2, 1), (1, 1), (3, 0), (1, 0), (3, 1), (0, 0), (0, 1))
ARRIVALS = ((0, 0), (0, 1), (3, 0), (1, 1), (3, 1), (1, 0), (2, 0), (2, 1))

ORDER = (
    ("qmm", 1), ("qmm", 0), ("umm", 0, 0), ("qm", "2r"), ("qm", "1l"), ("umm", 0, 1),
    ("umm", 0, 2), ("qm", "1r"), ("um", 0, "1r"), ("qm", "2l"), ("umm", 0, 7), ("um", 0, "1l"),
    ("umm", 0, 5), ("um", 0, "2r"), ("umm", 0, 4), ("umm", 0, 6), ("qm", "3l"), ("umm", 0, 3),
    ("qm", "3r"), ("um", 0, "2l"), ("um", 0, "3r"), ("um", 0, "3l"), ("qt", 1), ("att", 1),
    ("c", "1l"), ("c", "2r"), ("qt", 0), ("att", 0), ("c", "1r"), ("c", "2l"),
    ("a", 0, "0"), ("a", 0, "1"), ("a", 0, "2r"), ("a", 0, "2l"), ("pc", "2r"), ("c", "3l"),
    ("c", "3r"), ("dmm", 0, 1), ("pc", "2l"), ("dmm", 0, 0), ("a", 0, "3r"), ("a", 0, "3l"),
    ("dmm", 0, 2), ("dmm", 0, 3), ("ap", 0, "2r"), ("ap", 0, "2l"), ("pc", "3r"), ("pc", "3l"),
    ("dmm", 0, 4), ("dmm", 0, 5), ("amm",), ("ap", 0, "3r"), ("ap", 0, "3l"), ("dmm", 0, 6),
    ("dmm", 0, 7), ("ysc", 0), ("yga", 0),
)


def dot(a, b, dims=NN):
    return lax.dot_general(a, b, dims, preferred_element_type=F32)


def layer_kernel(
    W, NY,
    pos_hbm, x_hbm, lna_hbm, lnm_hbm, wqkv_hbm, wout_hbm, wup_hbm, wdn_hbm, k_hbm, v_hbm,
    xout_ref, knew_ref, vnew_ref,
    pos_ref, x_v, lna_v, lnm_v, wqkv_v, wout_v, wup_v, wdn_v, k_v, v_v,
    stat_send, stat_recv, ha_v, hm_v,
    qpart, qsib, qsend, qrecv, qrot, kvrot, ctxs, ctx_all,
    upart, usib, usend, urecv, act_all, acc, ysend, yrecv,
    lsem, ssem, rsem,
):
    NX = W // 2
    R, D = x_v.shape
    NG = GROUPS_OF_ROWS
    RG = R // NG
    RY = RG // NY
    RB = R // W
    G, HD = kvrot.shape[0], k_v.shape[1]
    L = k_v.shape[2]
    QT = qrot.shape[1] // RB
    HB = wup_v.shape[2] // 2
    model_width = float(D * W)

    w = lax.axis_index("tpw")
    y = lax.axis_index("tph")
    c = lax.rem(w, 2)
    x = lax.div(w, 2)
    sib = w + 1 - 2 * c
    right = lax.rem(w + 2, W)
    left = lax.rem(w + W - 2, W)
    opp = lax.rem(w + W // 2, W)

    def chip(o):
        return lax.rem(x + o, NX)

    barrier = pltpu.get_barrier_semaphore()
    for i in range(1, W):
        pl.semaphore_signal(barrier, inc=1, device_id={"tpw": lax.rem(w + i, W)}, device_id_type=MESH)
    for i in range(1, NY):
        pl.semaphore_signal(barrier, inc=1, device_id={"tph": lax.rem(y + i, NY)}, device_id_type=MESH)

    loads = {}

    def load(name, src, dst):
        cp = pltpu.make_async_copy(src, dst, lsem.at[len(loads)])
        cp.start()
        loads[name] = cp

    load("x", x_hbm, x_v)
    load("pos", pos_hbm, pos_ref)
    load("lna", lna_hbm, lna_v)
    load("lnm", lnm_hbm, lnm_v)
    qw = wqkv_v.shape[1]
    for g in range(G):
        load(("qkv", g), wqkv_hbm.at[pl.ds(g * qw, qw), :], wqkv_v.at[g])
    for i, (o, h) in enumerate(PIECES):
        col = pl.multiple_of((chip(o) * 2 + h) * 2 * HB, 2 * HB)
        load(("up", i), wup_hbm.at[:, pl.ds(col, 2 * HB)], wup_v.at[i])
    load("k", k_hbm, k_v)
    load("v", v_hbm, v_v)
    load("out", wout_hbm, wout_v)
    for i, (o, h) in enumerate(ARRIVALS):
        row = pl.multiple_of((chip(o) * 2 + h) * 2 * HB, 2 * HB)
        load(("down", i), wdn_hbm.at[pl.ds(row, 2 * HB), :], wdn_v.at[i])

    sent = []
    messages = {}

    def send(name, src, dst, axis, to):
        i = len(sent)
        cp = pltpu.make_async_remote_copy(
            src_ref=src, dst_ref=dst, send_sem=ssem.at[i], recv_sem=rsem.at[i],
            device_id={axis: to}, device_id_type=MESH,
        )
        cp.start()
        sent.append(cp)
        messages[name] = cp

    seen = set()

    def arrived(name):
        if name not in seen:
            seen.add(name)
            messages[name].wait_recv()

    def need(name):
        if name not in seen:
            seen.add(name)
            loads[name].wait()

    loads["x"].wait()
    xf = x_v[...].astype(F32)
    s1 = jnp.sum(xf, axis=1, keepdims=True)
    s2 = jnp.sum(xf * xf, axis=1, keepdims=True)
    lane = lax.broadcasted_iota(jnp.int32, (R, 128), 1)
    stat_send[...] = jnp.where(lane == 0, s1, jnp.where(lane == 1, s2, 0.0)).T[0:8, :]
    pl.semaphore_wait(barrier, W - 1 + NY - 1)
    for i in range(1, W):
        send(("stat", i), stat_send, stat_recv.at[i - 1], "tpw", lax.rem(w + i, W))

    loads["pos"].wait()
    prow = lax.broadcasted_iota(jnp.int32, (RB, 128), 0)
    plane = lax.broadcasted_iota(jnp.int32, (RB, 128), 1)
    pos = jnp.zeros((RB, 128), jnp.int32)
    for b in range(RB):
        pos = jnp.where(prow == b, pos_ref[b], pos)
    half = HD // 2
    freq = jnp.exp(lax.rem(plane, half).astype(F32) * (-math.log(ROPE_BASE) * 2.0 / HD))
    angle = pos.astype(F32) * freq
    cos_t = jnp.cos(angle)
    first = lax.rem(plane, HD) < half
    sin_t = jnp.where(first, -jnp.sin(angle), jnp.sin(angle))

    for i in range(1, W):
        arrived(("stat", i))
    tot = stat_send[...]
    for i in range(1, W):
        tot = tot + stat_recv[i - 1]
    cols = jnp.concatenate([tot, jnp.zeros((R - 8, R), F32)], axis=0).T
    mean = cols[:, 0:1] / model_width
    var = cols[:, 1:2] / model_width - mean * mean
    rstd = lax.rsqrt(var + LN_EPS)
    loads["lna"].wait()
    loads["lnm"].wait()
    cen = (x_v[...].astype(F32) - mean) * rstd
    ha_v[...] = (cen * lna_v[0:1, :] + lna_v[1:2, :]).astype(BF16)
    hm_v[...] = (cen * lnm_v[0:1, :] + lnm_v[1:2, :]).astype(BF16)

    legs = {
        "1r": (0, 2, 0, None, right), "1l": (1, 2, 1, None, left),
        "2r": (2, 1, 1, None, right), "2l": (3, 3, 0, None, left),
        "3r": (4, 1, 0, 0, right), "3l": (5, 3, 1, 1, left),
    }

    def leg(tag, key, own, stage, landing):
        i, o, h, add, to = legs[key]
        val = own(o, h)
        if add is not None:
            arrived((tag, add))
            val = val + landing[add].astype(F32)
        stage[i] = val.astype(BF16)
        send((tag, i), stage.at[i], landing.at[i], "tpw", to)

    def total(tag, h, own, landing):
        val = own(0, h)
        for i in ((3, 4), (2, 5))[h]:
            arrived((tag, i))
            val = val + landing[i].astype(F32)
        return val

    def qmm(g):
        need(("qkv", g))
        part = dot(ha_v[...], wqkv_v[g], NT).astype(BF16)
        qpart[g] = part.reshape(NX, 2, RB, qw)
        send(("qs", g), qpart.at[g, :, 1 - c], qsib.at[g], "tpw", sib)

    def qkv_own(o, g):
        arrived(("qs", g))
        return qpart[g, chip(o), c].astype(F32) + qsib[g, chip(o)].astype(F32)

    def qm(key):
        leg("q", key, qkv_own, qsend, qrecv)

    def umm(r, i):
        need(("up", i))
        hm = hm_v[r * RG:(r + 1) * RG, :]
        for k in range(2):
            upart[r, i, k] = dot(hm, wup_v[i, :, k * HB:(k + 1) * HB]).astype(BF16)
        send(("us", r, i), upart.at[r, i, 1 - c], usib.at[r, i], "tpw", sib)

    def up_own(r):
        def own(o, h):
            i = PIECES.index((o, h))
            arrived(("us", r, i))
            return upart[r, i, c].astype(F32) + usib[r, i].astype(F32)

        return own

    def um(r, key):
        leg(("u", r), key, up_own(r), usend.at[r], urecv.at[r])

    mine = pl.ds(pl.multiple_of(c * HB, HB), HB)

    def act_send(r, name, o, h, to, to_o):
        src = act_all.at[r, ARRIVALS.index((o, h)), :, mine]
        dst = act_all.at[r, ARRIVALS.index((to_o, h)), :, mine]
        send(("a", r, name), src, dst, "tpw", to)

    def act(r, key):
        if key in ("0", "1"):
            h = int(key)
            pre = total(("u", r), h, up_own(r), urecv.at[r])
            val = 0.5 * pre * (1.0 + lax.erf(pre * (2.0 ** -0.5)))
            act_all[r, ARRIVALS.index((0, h)), :, mine] = val.astype(BF16)
            if h == 0:
                act_send(r, "1r", 0, 0, right, 3)
            else:
                act_send(r, "1l", 0, 1, left, 1)
            act_send(r, ("s", 0, h), 0, h, sib, 0)
        elif key == "2r":
            act_send(r, "2r", 0, 1, right, 3)
        elif key == "2l":
            act_send(r, "2l", 0, 0, left, 1)
        elif key == "3r":
            arrived(("a", r, "1r"))
            act_send(r, "3r", 3, 0, right, 2)
            act_send(r, ("s", 3, 0), 3, 0, sib, 3)
        else:
            arrived(("a", r, "1l"))
            act_send(r, "3l", 1, 1, left, 2)
            act_send(r, ("s", 1, 1), 1, 1, sib, 1)

    def ap(r, key):
        o, h = {"2r": (3, 1), "2l": (1, 0), "3r": (2, 0), "3l": (2, 1)}[key]
        arrived(("a", r, key))
        act_send(r, ("s", o, h), o, h, sib, o)

    begun = set()

    def accumulate(r, part):
        if r in begun:
            acc[r] += part
        else:
            acc[r] = part
            begun.add(r)

    def dmm(r, i):
        o, h = ARRIVALS[i]
        arrived(("a", r, ("s", o, h)))
        need(("down", i))
        accumulate(r, dot(act_all[r, i], wdn_v[i]))

    scale = HD ** -0.5
    when = lax.broadcasted_iota(jnp.int32, (2 * QT, L), 1)

    def rotary(t):
        swapped = jnp.where(first, pltpu.roll(t, 128 - half, 1), pltpu.roll(t, half, 1))
        return (t * cos_t + swapped * sin_t).astype(BF16).astype(F32)

    def qt(g):
        qkv = total("q", g, qkv_own, qrecv).astype(BF16).astype(F32)
        for t in range(QT):
            qrot[g, t * RB:(t + 1) * RB, :] = rotary(qkv[:, t * 128:(t + 1) * 128])
        last = qkv[:, QT * 128:]
        kv = jnp.where(plane < HD, rotary(last), last)
        kvrot[g] = kv
        knew_ref[:, g * HD:(g + 1) * HD] = kv[:, :HD].astype(BF16)
        vnew_ref[:, g * HD:(g + 1) * HD] = kv[:, HD:].astype(BF16)

    def att(g):
        need("k")
        need("v")

        def row(b):
            q8 = qrot[g, pl.ds(b, QT, stride=RB), :]
            q = jnp.concatenate([q8[:, :HD], q8[:, HD:]], axis=0)
            kv = kvrot[g, pl.ds(b, 1), :]
            s = dot(q.astype(BF16), k_v[b * G + g]) * scale
            s = jnp.where(when < pos_ref[b], s, -jnp.inf)
            sn = jnp.sum(q * kv[:, :HD], axis=1, keepdims=True) * scale
            m = jnp.maximum(jnp.max(s, axis=1, keepdims=True), sn)
            e = jnp.exp(s - m)
            en = jnp.exp(sn - m)
            rz = 1.0 / (jnp.sum(e, axis=1, keepdims=True) + en)
            wn = (en * rz).astype(BF16).astype(F32)
            ctx = dot((e * rz).astype(BF16), v_v[b * G + g], NT) + wn * kv[:, HD:]
            ctxs[g, pl.ds(b, QT, stride=RB), :] = jnp.concatenate([ctx[:QT], ctx[QT:]], axis=1)

        def rows(i, _):
            for j in range(8):
                row(i * 8 + j)
            return 0

        lax.fori_loop(0, RB // 8, rows, 0)
        for t in range(QT):
            ctx_all[w, g, :, t * 128:(t + 1) * 128] = ctxs[g, t * RB:(t + 1) * RB, :].astype(BF16)
        send(("c", ("s", 0, g)), ctx_all.at[w, g], ctx_all.at[w, g], "tpw", sib)

    def ctx_send(name, who, g, to):
        send(("c", name), ctx_all.at[who, g], ctx_all.at[who, g], "tpw", to)

    def ctx(key):
        if key == "1r":
            ctx_send("1r", w, 0, right)
        elif key == "1l":
            ctx_send("1l", w, 1, left)
        elif key == "2r":
            ctx_send("2r", w, 1, right)
        elif key == "2l":
            ctx_send("2l", w, 0, left)
        elif key == "3r":
            arrived(("c", "1r"))
            ctx_send("3r", left, 0, right)
            ctx_send(("s", 3, 0), left, 0, sib)
        else:
            arrived(("c", "1l"))
            ctx_send("3l", right, 1, left)
            ctx_send(("s", 1, 1), right, 1, sib)

    def pc(key):
        who, o, g = {"2r": (left, 3, 1), "2l": (right, 1, 0), "3r": (opp, 2, 0), "3l": (opp, 2, 1)}[key]
        arrived(("c", key))
        ctx_send(("s", o, g), who, g, sib)

    def amm():
        for o in range(NX):
            for g in range(G):
                arrived(("c", ("s", o, g)))
        need("out")
        n = QT * 128
        for g in range(G):
            part = dot(ctx_all[:, g].reshape(R, n), wout_v[g * n:(g + 1) * n, :])
            for r in range(NG):
                accumulate(r, part[r * RG:(r + 1) * RG])

    def ysc(r):
        ysend[r] = acc[r].astype(BF16)
        for i in (2, 1, 3):
            to = lax.rem(y + i, NY)
            rows = pl.ds(pl.multiple_of(to * RY, RY), RY)
            send(("y", r, i), ysend.at[r, rows], yrecv.at[r, i - 1], "tph", to)

    def yga(r):
        start = pl.multiple_of(y * RY, RY)
        tot = acc[r, pl.ds(start, RY), :]
        for i in range(1, NY):
            arrived(("y", r, i))
            tot = tot + yrecv[r, i - 1].astype(F32)
        rows = pl.ds(pl.multiple_of(r * RG + start, RY), RY)
        xout_ref[rows, :] = (x_v[rows, :].astype(F32) + tot).astype(BF16)
        for i in (2, 1, 3):
            send(("z", r, i), xout_ref.at[rows, :], xout_ref.at[rows, :], "tph", lax.rem(y + i, NY))

    steps = {
        "qmm": qmm, "qm": qm, "umm": umm, "um": um, "a": act, "ap": ap, "dmm": dmm, "qt": qt, "att": att,
        "c": ctx, "pc": pc, "amm": amm, "ysc": ysc, "yga": yga,
    }
    for step in ORDER:
        steps[step[0]](*step[1:])
    for name in messages:
        arrived(name)
    for cp in sent:
        cp.wait_send()


def finish_kernel(x_ref, k_ref, v_ref, xout_ref, knew_ref, vnew_ref):
    xout_ref[...] = x_ref[...]
    hd = knew_ref.shape[2]
    for g in range(knew_ref.shape[1]):
        knew_ref[:, g, :] = k_ref[:, g * hd:(g + 1) * hd]
        vnew_ref[:, g, :] = v_ref[:, g * hd:(g + 1) * hd]


def solution(mesh):
    W = mesh.shape["tpw"]
    NY = mesh.shape["tph"]
    if W != 8:
        raise ValueError("tpw")

    def local_layer(x_in, ln_attn, ln_mlp, w_qkv, w_out, w_up, w_down, k_cache, v_cache, positions):
        R, D = x_in.shape
        _, G, S, HD = w_qkv.shape
        F = w_up.shape[1]
        L = k_cache.shape[2]
        RB = R // W
        NX = W // 2
        NG = GROUPS_OF_ROWS
        RG = R // NG
        qw = S * HD
        cw = (S - 2) * HD
        QT = cw // 128
        HB = F // W // 2
        wqkv_t = jnp.transpose(w_qkv, (1, 2, 3, 0)).reshape(G * qw, D)
        k_t = jnp.swapaxes(k_cache, 2, 3).reshape(RB * G, HD, L)
        v_t = jnp.swapaxes(v_cache, 2, 3).reshape(RB * G, HD, L)
        n_messages = 7 + 2 + 6 + NG * 8 + NG * 6 + NG * 14 + 14 + NG * 6
        any_spec = pl.BlockSpec(memory_space=pl.ANY)
        vmem_spec = pl.BlockSpec(memory_space=pltpu.VMEM)
        x_out, k_new, v_new = pl.pallas_call(
            functools.partial(layer_kernel, W, NY),
            name="layer",
            out_shape=(
                pltpu.VMEM((R, D), BF16),
                pltpu.VMEM((RB, G * HD), BF16),
                pltpu.VMEM((RB, G * HD), BF16),
            ),
            in_specs=[any_spec] * 10,
            out_specs=(vmem_spec,) * 3,
            scratch_shapes=[
                pltpu.SMEM((RB,), jnp.int32),
                pltpu.VMEM((R, D), BF16),
                pltpu.VMEM((2, D), F32),
                pltpu.VMEM((2, D), F32),
                pltpu.VMEM((G, qw, D), BF16),
                pltpu.VMEM((G * cw, D), BF16),
                pltpu.VMEM((8, D, 2 * HB), BF16),
                pltpu.VMEM((8, 2 * HB, D), BF16),
                pltpu.VMEM((RB * G, HD, L), BF16),
                pltpu.VMEM((RB * G, HD, L), BF16),
                pltpu.VMEM((8, 128), F32),
                pltpu.VMEM((W - 1, 8, 128), F32),
                pltpu.VMEM((R, D), BF16),
                pltpu.VMEM((R, D), BF16),
                pltpu.VMEM((G, NX, 2, RB, qw), BF16),
                pltpu.VMEM((G, NX, RB, qw), BF16),
                pltpu.VMEM((6, RB, qw), BF16),
                pltpu.VMEM((6, RB, qw), BF16),
                pltpu.VMEM((G, QT * RB, 128), F32),
                pltpu.VMEM((G, RB, 128), F32),
                pltpu.VMEM((G, QT * RB, 128), F32),
                pltpu.VMEM((W, G, RB, cw), BF16),
                pltpu.VMEM((NG, 8, 2, RG, HB), BF16),
                pltpu.VMEM((NG, 8, RG, HB), BF16),
                pltpu.VMEM((NG, 6, RG, HB), BF16),
                pltpu.VMEM((NG, 6, RG, HB), BF16),
                pltpu.VMEM((NG, 8, RG, 2 * HB), BF16),
                pltpu.VMEM((NG, RG, D), F32),
                pltpu.VMEM((NG, RG, D), BF16),
                pltpu.VMEM((NG, NY - 1, RG // NY, D), BF16),
                pltpu.SemaphoreType.DMA((32,)),
                pltpu.SemaphoreType.DMA((n_messages,)),
                pltpu.SemaphoreType.DMA((n_messages,)),
            ],
            compiler_params=pltpu.CompilerParams(
                collective_id=0, has_side_effects=True, vmem_limit_bytes=VMEM_LIMIT
            ),
        )(
            positions, x_in, ln_attn, ln_mlp, wqkv_t, w_out.reshape(G * cw, D), w_up, w_down, k_t, v_t,
        )
        return pl.pallas_call(
            finish_kernel,
            name="finish",
            out_shape=(
                jax.ShapeDtypeStruct((R, D), BF16),
                jax.ShapeDtypeStruct((RB, G, HD), BF16),
                jax.ShapeDtypeStruct((RB, G, HD), BF16),
            ),
            in_specs=[vmem_spec] * 3,
            out_specs=(vmem_spec,) * 3,
        )(*(pltpu.with_memory_space_constraint(a, pltpu.VMEM) for a in (x_out, k_new, v_new)))

    cache_spec = P(("dp", "tpw"), "tph", None, None)
    new_spec = P(("dp", "tpw"), "tph", None)
    in_specs = (
        P("dp", "tpw"),
        P(None, "tpw"),
        P(None, "tpw"),
        P("tpw", "tph", None, None),
        P("tph", None, None, "tpw"),
        P("tpw", "tph"),
        P("tph", "tpw"),
        cache_spec,
        cache_spec,
        P(("dp", "tpw")),
    )
    out_specs = (P("dp", "tpw"), new_spec, new_spec)
    return jax.shard_map(local_layer, mesh=mesh, in_specs=in_specs, out_specs=out_specs, check_vma=False)
```

```python
import functools
import math

import jax
import jax.numpy as jnp
from jax import lax
from jax.experimental import pallas as pl
from jax.experimental.pallas import tpu as pltpu
from jax.sharding import PartitionSpec as P

LN_EPS = 1e-5
ROPE_BASE = 10000.0
MESH = pl.DeviceIdType.MESH
F32 = jnp.float32
BF16 = jnp.bfloat16
VMEM_LIMIT = 58 << 20
GROUPS_OF_ROWS = 2
GROUPS_OF_COLUMNS = 2
NN = (((1,), (0,)), ((), ()))
NT = (((1,), (1,)), ((), ()))
PIECES = ((2, 0), (2, 1), (1, 1), (3, 0), (1, 0), (3, 1), (0, 0), (0, 1))
ARRIVALS = ((0, 0), (0, 1), (3, 0), (1, 1), (3, 1), (1, 0), (2, 0), (2, 1))

ORDER = (
    ("qmm", 0), ("qmm", 1), ("umm", 1), ("qm", "1r"), ("qm", "2l"), ("umm", 0),
    ("umm", 6), ("qm", "1l"), ("qm", "2r"), ("um", 1, "1l"), ("um", 0, "1l"), ("umm", 4),
    ("um", 1, "1r"), ("umm", 7), ("um", 0, "1r"), ("umm", 3), ("umm", 2), ("qm", "3r"),
    ("umm", 5), ("um", 0, "2l"), ("qm", "3l"), ("um", 1, "2l"), ("um", 1, "2r"), ("um", 0, "2r"),
    ("um", 1, "3l"), ("um", 1, "3r"), ("um", 0, "3l"), ("um", 0, "3r"), ("qt", 0), ("att", 0),
    ("c", "2l"), ("qt", 1), ("att", 1), ("c", "1r"), ("c", "2r"), ("c", "1l"),
    ("a", 1, "0"), ("a", 1, "2l"), ("a", 1, "1"), ("a", 1, "2r"), ("a", 0, "1"), ("a", 0, "0"),
    ("a", 0, "2l"), ("a", 0, "2r"), ("pc", "2l"), ("c", "3r"), ("dmm", 1), ("c", "3l"),
    ("pc", "2r"), ("dmm", 0), ("a", 1, "3r"), ("ap", 1, "2l"), ("ap", 1, "2r"), ("a", 1, "3l"),
    ("a", 0, "3l"), ("a", 0, "3r"), ("dmm", 3), ("ap", 0, "2r"), ("ap", 0, "2l"), ("dmm", 2),
    ("pc", "3l"), ("pc", "3r"), ("dmm", 4), ("dmm", 5), ("ap", 1, "3l"), ("ap", 1, "3r"),
    ("amm",), ("ap", 0, "3l"), ("ap", 0, "3r"), ("dmm", 7, 1), ("dmm", 6, 1), ("ysc", 1),
    ("dmm", 6, 0), ("dmm", 7, 0), ("ysc", 0), ("yga", 1), ("yga", 0),
)


def dot(a, b, dims=NN):
    return lax.dot_general(a, b, dims, preferred_element_type=F32)


def layer_kernel(
    W, NY,
    pos_hbm, x_hbm, lna_hbm, lnm_hbm, wqkv_hbm, wout_hbm, wup_hbm, wdn_hbm, k_hbm, v_hbm,
    xout_ref, knew_ref, vnew_ref,
    pos_ref, x_v, lna_v, lnm_v, wqkv_v, wout_v, wup_v, wdn_v, k_v, v_v,
    stat_send, stat_recv, ha_v, hm_v,
    qpart, qsib, qsend, qrecv, qrot, kvrot, ctxs, ctx_all,
    upart, usib, usend, urecv, act_all, acc, ysend, yrecv,
    lsem, ssem, rsem,
):
    NX = W // 2
    R, D = x_v.shape
    NG = GROUPS_OF_ROWS
    RG = R // NG
    RY = R // NY
    NC = GROUPS_OF_COLUMNS
    DC = D // NC
    RB = R // W
    G, HD = kvrot.shape[0], k_v.shape[1]
    L = k_v.shape[2]
    QT = qrot.shape[1] // RB
    HB = wup_v.shape[2] // 2
    model_width = float(D * W)

    w = lax.axis_index("tpw")
    y = lax.axis_index("tph")
    c = lax.rem(w, 2)
    x = lax.div(w, 2)
    sib = w + 1 - 2 * c
    right = lax.rem(w + 2, W)
    left = lax.rem(w + W - 2, W)
    opp = lax.rem(w + W // 2, W)

    def chip(o):
        return lax.rem(x + o, NX)

    barrier = pltpu.get_barrier_semaphore()
    for i in range(1, W):
        pl.semaphore_signal(barrier, inc=1, device_id={"tpw": lax.rem(w + i, W)}, device_id_type=MESH)
    for i in range(1, NY):
        pl.semaphore_signal(barrier, inc=1, device_id={"tph": lax.rem(y + i, NY)}, device_id_type=MESH)

    loads = {}

    def load(name, src, dst):
        cp = pltpu.make_async_copy(src, dst, lsem.at[len(loads)])
        cp.start()
        loads[name] = cp

    load("x", x_hbm, x_v)
    load("pos", pos_hbm, pos_ref)
    load("lna", lna_hbm, lna_v)
    load("lnm", lnm_hbm, lnm_v)
    qw = wqkv_v.shape[1]
    for g in range(G):
        load(("qkv", g), wqkv_hbm.at[pl.ds(g * qw, qw), :], wqkv_v.at[g])
    for i, (o, h) in enumerate(PIECES):
        col = pl.multiple_of((chip(o) * 2 + h) * 2 * HB, 2 * HB)
        load(("up", i), wup_hbm.at[:, pl.ds(col, 2 * HB)], wup_v.at[i])
    load("k", k_hbm, k_v)
    load("v", v_hbm, v_v)
    load("out", wout_hbm, wout_v)
    for i, (o, h) in enumerate(ARRIVALS):
        row = pl.multiple_of((chip(o) * 2 + h) * 2 * HB, 2 * HB)
        load(("down", i), wdn_hbm.at[pl.ds(row, 2 * HB), :], wdn_v.at[i])

    sent = []
    messages = {}

    def send(name, src, dst, axis, to):
        i = len(sent)
        cp = pltpu.make_async_remote_copy(
            src_ref=src, dst_ref=dst, send_sem=ssem.at[i], recv_sem=rsem.at[i],
            device_id={axis: to}, device_id_type=MESH,
        )
        cp.start()
        sent.append(cp)
        messages[name] = cp

    seen = set()

    def arrived(name):
        if name not in seen:
            seen.add(name)
            messages[name].wait_recv()

    def need(name):
        if name not in seen:
            seen.add(name)
            loads[name].wait()

    loads["x"].wait()
    xf = x_v[...].astype(F32)
    s1 = jnp.sum(xf, axis=1, keepdims=True)
    s2 = jnp.sum(xf * xf, axis=1, keepdims=True)
    lane = lax.broadcasted_iota(jnp.int32, (R, 128), 1)
    stat_send[...] = jnp.where(lane == 0, s1, jnp.where(lane == 1, s2, 0.0)).T[0:8, :]
    pl.semaphore_wait(barrier, W - 1 + NY - 1)
    for i in range(1, W):
        send(("stat", i), stat_send, stat_recv.at[i - 1], "tpw", lax.rem(w + i, W))

    loads["pos"].wait()
    prow = lax.broadcasted_iota(jnp.int32, (RB, 128), 0)
    plane = lax.broadcasted_iota(jnp.int32, (RB, 128), 1)
    pos = jnp.zeros((RB, 128), jnp.int32)
    for b in range(RB):
        pos = jnp.where(prow == b, pos_ref[b], pos)
    half = HD // 2
    freq = jnp.exp(lax.rem(plane, half).astype(F32) * (-math.log(ROPE_BASE) * 2.0 / HD))
    angle = pos.astype(F32) * freq
    cos_t = jnp.cos(angle)
    first = lax.rem(plane, HD) < half
    sin_t = jnp.where(first, -jnp.sin(angle), jnp.sin(angle))

    for i in range(1, W):
        arrived(("stat", i))
    tot = stat_send[...]
    for i in range(1, W):
        tot = tot + stat_recv[i - 1]
    cols = jnp.concatenate([tot, jnp.zeros((R - 8, R), F32)], axis=0).T
    mean = cols[:, 0:1] / model_width
    var = cols[:, 1:2] / model_width - mean * mean
    rstd = lax.rsqrt(var + LN_EPS)
    loads["lna"].wait()
    loads["lnm"].wait()
    cen = (x_v[...].astype(F32) - mean) * rstd
    ha_v[...] = (cen * lna_v[0:1, :] + lna_v[1:2, :]).astype(BF16)
    hm_v[...] = (cen * lnm_v[0:1, :] + lnm_v[1:2, :]).astype(BF16)

    legs = {
        "1r": (0, 2, 0, None, right), "1l": (1, 2, 1, None, left),
        "2r": (2, 1, 1, None, right), "2l": (3, 3, 0, None, left),
        "3r": (4, 1, 0, 0, right), "3l": (5, 3, 1, 1, left),
    }

    def leg(tag, key, own, stage, landing):
        i, o, h, add, to = legs[key]
        val = own(o, h)
        if add is not None:
            arrived((tag, add))
            val = val + landing[add].astype(F32)
        stage[i] = val.astype(BF16)
        send((tag, i), stage.at[i], landing.at[i], "tpw", to)

    def total(tag, h, own, landing):
        val = own(0, h)
        for i in ((3, 4), (2, 5))[h]:
            arrived((tag, i))
            val = val + landing[i].astype(F32)
        return val

    def qmm(g):
        need(("qkv", g))
        part = dot(ha_v[...], wqkv_v[g], NT).astype(BF16)
        qpart[g] = part.reshape(NX, 2, RB, qw)
        send(("qs", g), qpart.at[g, :, 1 - c], qsib.at[g], "tpw", sib)

    def qkv_own(o, g):
        arrived(("qs", g))
        return qpart[g, chip(o), c].astype(F32) + qsib[g, chip(o)].astype(F32)

    def qm(key):
        leg("q", key, qkv_own, qsend, qrecv)

    def umm(i):
        need(("up", i))
        for k in range(2):
            upart[i, k] = dot(hm_v[...], wup_v[i, :, k * HB:(k + 1) * HB]).astype(BF16)
        send(("us", i), upart.at[i, 1 - c], usib.at[i], "tpw", sib)

    def up_own(r):
        def own(o, h):
            i = PIECES.index((o, h))
            arrived(("us", i))
            rows = slice(r * RG, (r + 1) * RG)
            return upart[i, c, rows].astype(F32) + usib[i, rows].astype(F32)

        return own

    def um(r, key):
        leg(("u", r), key, up_own(r), usend.at[r], urecv.at[r])

    mine = pl.ds(pl.multiple_of(c * HB, HB), HB)

    def act_send(r, name, o, h, to, to_o):
        src = act_all.at[ARRIVALS.index((o, h)), pl.ds(r * RG, RG), mine]
        dst = act_all.at[ARRIVALS.index((to_o, h)), pl.ds(r * RG, RG), mine]
        send(("a", r, name), src, dst, "tpw", to)

    def act(r, key):
        if key in ("0", "1"):
            h = int(key)
            pre = total(("u", r), h, up_own(r), urecv.at[r])
            val = 0.5 * pre * (1.0 + lax.erf(pre * (2.0 ** -0.5)))
            act_all[ARRIVALS.index((0, h)), r * RG:(r + 1) * RG, mine] = val.astype(BF16)
            if h == 0:
                act_send(r, "1r", 0, 0, right, 3)
            else:
                act_send(r, "1l", 0, 1, left, 1)
            act_send(r, ("s", 0, h), 0, h, sib, 0)
        elif key == "2r":
            act_send(r, "2r", 0, 1, right, 3)
        elif key == "2l":
            act_send(r, "2l", 0, 0, left, 1)
        elif key == "3r":
            arrived(("a", r, "1r"))
            act_send(r, "3r", 3, 0, right, 2)
            act_send(r, ("s", 3, 0), 3, 0, sib, 3)
        else:
            arrived(("a", r, "1l"))
            act_send(r, "3l", 1, 1, left, 2)
            act_send(r, ("s", 1, 1), 1, 1, sib, 1)

    def ap(r, key):
        o, h = {"2r": (3, 1), "2l": (1, 0), "3r": (2, 0), "3l": (2, 1)}[key]
        arrived(("a", r, key))
        act_send(r, ("s", o, h), o, h, sib, o)

    begun = set()

    def accumulate(part, *j):
        cols = slice(j[0] * DC, (j[0] + 1) * DC) if j else slice(0, D)
        if begun:
            acc[:, cols] += part
        else:
            acc[...] = part
            begun.add(0)

    def dmm(i, *j):
        o, h = ARRIVALS[i]
        for r in range(NG):
            arrived(("a", r, ("s", o, h)))
        need(("down", i))
        if j:
            accumulate(dot(act_all[i], wdn_v[i, :, j[0] * DC:(j[0] + 1) * DC]), *j)
        else:
            accumulate(dot(act_all[i], wdn_v[i]))

    scale = HD ** -0.5
    when = lax.broadcasted_iota(jnp.int32, (2 * QT, L), 1)

    def rotary(t):
        swapped = jnp.where(first, pltpu.roll(t, 128 - half, 1), pltpu.roll(t, half, 1))
        return (t * cos_t + swapped * sin_t).astype(BF16).astype(F32)

    def qt(g):
        qkv = total("q", g, qkv_own, qrecv).astype(BF16).astype(F32)
        for t in range(QT):
            qrot[g, t * RB:(t + 1) * RB, :] = rotary(qkv[:, t * 128:(t + 1) * 128])
        last = qkv[:, QT * 128:]
        kv = jnp.where(plane < HD, rotary(last), last)
        kvrot[g] = kv
        knew_ref[:, g * HD:(g + 1) * HD] = kv[:, :HD].astype(BF16)
        vnew_ref[:, g * HD:(g + 1) * HD] = kv[:, HD:].astype(BF16)

    def att(g):
        need("k")
        need("v")

        def row(b):
            q8 = qrot[g, pl.ds(b, QT, stride=RB), :]
            q = jnp.concatenate([q8[:, :HD], q8[:, HD:]], axis=0)
            kv = kvrot[g, pl.ds(b, 1), :]
            s = dot(q.astype(BF16), k_v[b * G + g]) * scale
            s = jnp.where(when < pos_ref[b], s, -jnp.inf)
            sn = jnp.sum(q * kv[:, :HD], axis=1, keepdims=True) * scale
            m = jnp.maximum(jnp.max(s, axis=1, keepdims=True), sn)
            e = jnp.exp(s - m)
            en = jnp.exp(sn - m)
            rz = 1.0 / (jnp.sum(e, axis=1, keepdims=True) + en)
            wn = (en * rz).astype(BF16).astype(F32)
            ctx = dot((e * rz).astype(BF16), v_v[b * G + g], NT) + wn * kv[:, HD:]
            ctxs[g, pl.ds(b, QT, stride=RB), :] = jnp.concatenate([ctx[:QT], ctx[QT:]], axis=1)

        def rows(i, _):
            for j in range(8):
                row(i * 8 + j)
            return 0

        lax.fori_loop(0, RB // 8, rows, 0)
        for t in range(QT):
            ctx_all[w, g, :, t * 128:(t + 1) * 128] = ctxs[g, t * RB:(t + 1) * RB, :].astype(BF16)
        send(("c", ("s", 0, g)), ctx_all.at[w, g], ctx_all.at[w, g], "tpw", sib)

    def ctx_send(name, who, g, to):
        send(("c", name), ctx_all.at[who, g], ctx_all.at[who, g], "tpw", to)

    def ctx(key):
        if key == "1r":
            ctx_send("1r", w, 0, right)
        elif key == "1l":
            ctx_send("1l", w, 1, left)
        elif key == "2r":
            ctx_send("2r", w, 1, right)
        elif key == "2l":
            ctx_send("2l", w, 0, left)
        elif key == "3r":
            arrived(("c", "1r"))
            ctx_send("3r", left, 0, right)
            ctx_send(("s", 3, 0), left, 0, sib)
        else:
            arrived(("c", "1l"))
            ctx_send("3l", right, 1, left)
            ctx_send(("s", 1, 1), right, 1, sib)

    def pc(key):
        who, o, g = {"2r": (left, 3, 1), "2l": (right, 1, 0), "3r": (opp, 2, 0), "3l": (opp, 2, 1)}[key]
        arrived(("c", key))
        ctx_send(("s", o, g), who, g, sib)

    def amm():
        for o in range(NX):
            for g in range(G):
                arrived(("c", ("s", o, g)))
        need("out")
        n = QT * 128
        for g in range(G):
            accumulate(dot(ctx_all[:, g].reshape(R, n), wout_v[g * n:(g + 1) * n, :]))

    def ysc(j):
        ysend[j] = acc[:, j * DC:(j + 1) * DC].astype(BF16)
        for i in (2, 1, 3):
            to = lax.rem(y + i, NY)
            rows = pl.ds(pl.multiple_of(to * RY, RY), RY)
            send(("y", j, i), ysend.at[j, rows], yrecv.at[j, i - 1], "tph", to)

    def yga(j):
        rows = pl.ds(pl.multiple_of(y * RY, RY), RY)
        cols = slice(j * DC, (j + 1) * DC)
        tot = acc[rows, cols]
        for i in range(1, NY):
            arrived(("y", j, i))
            tot = tot + yrecv[j, i - 1].astype(F32)
        xout_ref[rows, cols] = (x_v[rows, cols].astype(F32) + tot).astype(BF16)
        block = xout_ref.at[rows, pl.ds(j * DC, DC)]
        for i in (2, 1, 3):
            send(("z", j, i), block, block, "tph", lax.rem(y + i, NY))

    steps = {
        "qmm": qmm, "qm": qm, "umm": umm, "um": um, "a": act, "ap": ap, "dmm": dmm, "qt": qt, "att": att,
        "c": ctx, "pc": pc, "amm": amm, "ysc": ysc, "yga": yga,
    }
    for step in ORDER:
        steps[step[0]](*step[1:])
    for name in messages:
        arrived(name)
    for cp in sent:
        cp.wait_send()


def finish_kernel(x_ref, k_ref, v_ref, xout_ref, knew_ref, vnew_ref):
    xout_ref[...] = x_ref[...]
    hd = knew_ref.shape[2]
    for g in range(knew_ref.shape[1]):
        knew_ref[:, g, :] = k_ref[:, g * hd:(g + 1) * hd]
        vnew_ref[:, g, :] = v_ref[:, g * hd:(g + 1) * hd]


def solution(mesh):
    W = mesh.shape["tpw"]
    NY = mesh.shape["tph"]
    if W != 8:
        raise ValueError("tpw")

    def local_layer(x_in, ln_attn, ln_mlp, w_qkv, w_out, w_up, w_down, k_cache, v_cache, positions):
        R, D = x_in.shape
        _, G, S, HD = w_qkv.shape
        F = w_up.shape[1]
        L = k_cache.shape[2]
        RB = R // W
        NX = W // 2
        NG = GROUPS_OF_ROWS
        RG = R // NG
        qw = S * HD
        cw = (S - 2) * HD
        QT = cw // 128
        HB = F // W // 2
        wqkv_t = jnp.transpose(w_qkv, (1, 2, 3, 0)).reshape(G * qw, D)
        k_t = jnp.swapaxes(k_cache, 2, 3).reshape(RB * G, HD, L)
        v_t = jnp.swapaxes(v_cache, 2, 3).reshape(RB * G, HD, L)
        NC = GROUPS_OF_COLUMNS
        n_messages = W - 1 + 2 + 6 + 8 + NG * 6 + NG * 14 + 14 + NC * 6
        any_spec = pl.BlockSpec(memory_space=pl.ANY)
        vmem_spec = pl.BlockSpec(memory_space=pltpu.VMEM)
        x_out, k_new, v_new = pl.pallas_call(
            functools.partial(layer_kernel, W, NY),
            name="layer",
            out_shape=(
                pltpu.VMEM((R, D), BF16),
                pltpu.VMEM((RB, G * HD), BF16),
                pltpu.VMEM((RB, G * HD), BF16),
            ),
            in_specs=[any_spec] * 10,
            out_specs=(vmem_spec,) * 3,
            scratch_shapes=[
                pltpu.SMEM((RB,), jnp.int32),
                pltpu.VMEM((R, D), BF16),
                pltpu.VMEM((2, D), F32),
                pltpu.VMEM((2, D), F32),
                pltpu.VMEM((G, qw, D), BF16),
                pltpu.VMEM((G * cw, D), BF16),
                pltpu.VMEM((8, D, 2 * HB), BF16),
                pltpu.VMEM((8, 2 * HB, D), BF16),
                pltpu.VMEM((RB * G, HD, L), BF16),
                pltpu.VMEM((RB * G, HD, L), BF16),
                pltpu.VMEM((8, 128), F32),
                pltpu.VMEM((W - 1, 8, 128), F32),
                pltpu.VMEM((R, D), BF16),
                pltpu.VMEM((R, D), BF16),
                pltpu.VMEM((G, NX, 2, RB, qw), BF16),
                pltpu.VMEM((G, NX, RB, qw), BF16),
                pltpu.VMEM((6, RB, qw), BF16),
                pltpu.VMEM((6, RB, qw), BF16),
                pltpu.VMEM((G, QT * RB, 128), F32),
                pltpu.VMEM((G, RB, 128), F32),
                pltpu.VMEM((G, QT * RB, 128), F32),
                pltpu.VMEM((W, G, RB, cw), BF16),
                pltpu.VMEM((8, 2, R, HB), BF16),
                pltpu.VMEM((8, R, HB), BF16),
                pltpu.VMEM((NG, 6, RG, HB), BF16),
                pltpu.VMEM((NG, 6, RG, HB), BF16),
                pltpu.VMEM((8, R, 2 * HB), BF16),
                pltpu.VMEM((R, D), F32),
                pltpu.VMEM((NC, R, D // NC), BF16),
                pltpu.VMEM((NC, NY - 1, R // NY, D // NC), BF16),
                pltpu.SemaphoreType.DMA((32,)),
                pltpu.SemaphoreType.DMA((n_messages,)),
                pltpu.SemaphoreType.DMA((n_messages,)),
            ],
            compiler_params=pltpu.CompilerParams(
                collective_id=0, has_side_effects=True, vmem_limit_bytes=VMEM_LIMIT
            ),
        )(
            positions, x_in, ln_attn, ln_mlp, wqkv_t, w_out.reshape(G * cw, D), w_up, w_down, k_t, v_t,
        )
        return pl.pallas_call(
            finish_kernel,
            name="finish",
            out_shape=(
                jax.ShapeDtypeStruct((R, D), BF16),
                jax.ShapeDtypeStruct((RB, G, HD), BF16),
                jax.ShapeDtypeStruct((RB, G, HD), BF16),
            ),
            in_specs=[vmem_spec] * 3,
            out_specs=(vmem_spec,) * 3,
        )(*(pltpu.with_memory_space_constraint(a, pltpu.VMEM) for a in (x_out, k_new, v_new)))

    cache_spec = P(("dp", "tpw"), "tph", None, None)
    new_spec = P(("dp", "tpw"), "tph", None)
    in_specs = (
        P("dp", "tpw"),
        P(None, "tpw"),
        P(None, "tpw"),
        P("tpw", "tph", None, None),
        P("tph", None, None, "tpw"),
        P("tpw", "tph"),
        P("tph", "tpw"),
        cache_spec,
        cache_spec,
        P(("dp", "tpw")),
    )
    out_specs = (P("dp", "tpw"), new_spec, new_spec)
    return jax.shard_map(local_layer, mesh=mesh, in_specs=in_specs, out_specs=out_specs, check_vma=False)
```

```python
import functools
import math

import jax
import jax.numpy as jnp
from jax import lax
from jax.experimental import pallas as pl
from jax.experimental.pallas import tpu as pltpu
from jax.sharding import PartitionSpec as P

LN_EPS = 1e-5
ROPE_BASE = 10000.0
MESH = pl.DeviceIdType.MESH
F32 = jnp.float32
BF16 = jnp.bfloat16
VMEM_LIMIT = 58 << 20
GROUPS_OF_ROWS = 1
LAST_GROUPS = 2
NN = (((1,), (0,)), ((), ()))
NT = (((1,), (1,)), ((), ()))
PIECES = ((2, 0), (2, 1), (1, 1), (3, 0), (1, 0), (3, 1), (0, 0), (0, 1))
ARRIVALS = ((0, 0), (0, 1), (3, 0), (1, 1), (3, 1), (1, 0), (2, 0), (2, 1))

ORDER = (
    ("qmm", 0), ("qmm", 1), ("umm", 1), ("umm", 0), ("qm", "2l"), ("qm", "1r"),
    ("umm", 5), ("qm", "2r"), ("qm", "1l"), ("umm", 6), ("um", 0, "1l"), ("umm", 7),
    ("um", 0, "1r"), ("umm", 2), ("umm", 3), ("umm", 4), ("qm", "3r"), ("um", 0, "2r"),
    ("um", 0, "2l"), ("qm", "3l"), ("um", 0, "3l"), ("um", 0, "3r"), ("qt", 0), ("att", 0),
    ("c", "1r"), ("c", "2l"), ("qt", 1), ("att", 1), ("c", "1l"), ("c", "2r"),
    ("a", 0, "1"), ("a", 0, "0"), ("a", 0, "2r"), ("a", 0, "2l"), ("pc", "2l"), ("c", "3r"),
    ("dmm", 1), ("pc", "2r"), ("c", "3l"), ("dmm", 0), ("a", 0, "3r"), ("a", 0, "3l"),
    ("dmm", 2), ("dmm", 3), ("ap", 0, "2l"), ("ap", 0, "2r"), ("pc", "3l"), ("pc", "3r"),
    ("dmm", 5), ("dmm", 4), ("at", "3l", 0), ("at", "3r", 0), ("amm",), ("at", "3l", 1),
    ("dmm", 6, 0), ("at", "3r", 1), ("dmm", 7, 0), ("ysc", 0), ("dmm", 7, 1), ("dmm", 6, 1),
    ("ysc", 1), ("yga", 0), ("yga", 1),
)


def dot(a, b, dims=NN):
    return lax.dot_general(a, b, dims, preferred_element_type=F32)


def layer_kernel(
    W, NY,
    pos_hbm, x_hbm, lna_hbm, lnm_hbm, wqkv_hbm, wout_hbm, wup_hbm, wdn_hbm, k_hbm, v_hbm,
    xout_ref, knew_ref, vnew_ref,
    pos_ref, x_v, lna_v, lnm_v, wqkv_v, wout_v, wup_v, wdn_v, k_v, v_v,
    stat_send, stat_recv, ha_v, hm_v,
    qpart, qsib, qsend, qrecv, qrot, kvrot, ctxs, ctx_all,
    upart, usib, usend, urecv, act_all, acc, ysend, yrecv,
    lsem, ssem, rsem,
):
    NX = W // 2
    R, D = x_v.shape
    NG = GROUPS_OF_ROWS
    RG = R // NG
    RL = R // LAST_GROUPS
    RY = RL // NY
    RB = R // W
    G, HD = kvrot.shape[0], k_v.shape[1]
    L = k_v.shape[2]
    QT = qrot.shape[1] // RB
    HB = wup_v.shape[2] // 2
    model_width = float(D * W)

    w = lax.axis_index("tpw")
    y = lax.axis_index("tph")
    c = lax.rem(w, 2)
    x = lax.div(w, 2)
    sib = w + 1 - 2 * c
    right = lax.rem(w + 2, W)
    left = lax.rem(w + W - 2, W)
    opp = lax.rem(w + W // 2, W)

    def chip(o):
        return lax.rem(x + o, NX)

    barrier = pltpu.get_barrier_semaphore()
    for i in range(1, W):
        pl.semaphore_signal(barrier, inc=1, device_id={"tpw": lax.rem(w + i, W)}, device_id_type=MESH)
    for i in range(1, NY):
        pl.semaphore_signal(barrier, inc=1, device_id={"tph": lax.rem(y + i, NY)}, device_id_type=MESH)

    loads = {}

    def load(name, src, dst):
        cp = pltpu.make_async_copy(src, dst, lsem.at[len(loads)])
        cp.start()
        loads[name] = cp

    load("x", x_hbm, x_v)
    load("pos", pos_hbm, pos_ref)
    load("lna", lna_hbm, lna_v)
    load("lnm", lnm_hbm, lnm_v)
    qw = wqkv_v.shape[1]
    for g in range(G):
        load(("qkv", g), wqkv_hbm.at[pl.ds(g * qw, qw), :], wqkv_v.at[g])
    for i, (o, h) in enumerate(PIECES):
        col = pl.multiple_of((chip(o) * 2 + h) * 2 * HB, 2 * HB)
        load(("up", i), wup_hbm.at[:, pl.ds(col, 2 * HB)], wup_v.at[i])
    load("k", k_hbm, k_v)
    load("v", v_hbm, v_v)
    load("out", wout_hbm, wout_v)
    for i, (o, h) in enumerate(ARRIVALS):
        row = pl.multiple_of((chip(o) * 2 + h) * 2 * HB, 2 * HB)
        load(("down", i), wdn_hbm.at[pl.ds(row, 2 * HB), :], wdn_v.at[i])

    sent = []
    messages = {}

    def send(name, src, dst, axis, to):
        i = len(sent)
        cp = pltpu.make_async_remote_copy(
            src_ref=src, dst_ref=dst, send_sem=ssem.at[i], recv_sem=rsem.at[i],
            device_id={axis: to}, device_id_type=MESH,
        )
        cp.start()
        sent.append(cp)
        messages[name] = cp

    seen = set()

    def arrived(name):
        if name not in seen:
            seen.add(name)
            messages[name].wait_recv()

    def need(name):
        if name not in seen:
            seen.add(name)
            loads[name].wait()

    loads["x"].wait()
    xf = x_v[...].astype(F32)
    s1 = jnp.sum(xf, axis=1, keepdims=True)
    s2 = jnp.sum(xf * xf, axis=1, keepdims=True)
    lane = lax.broadcasted_iota(jnp.int32, (R, 128), 1)
    stat_send[...] = jnp.where(lane == 0, s1, jnp.where(lane == 1, s2, 0.0)).T[0:8, :]
    pl.semaphore_wait(barrier, W - 1 + NY - 1)
    for i in range(1, W):
        send(("stat", i), stat_send, stat_recv.at[i - 1], "tpw", lax.rem(w + i, W))

    loads["pos"].wait()
    prow = lax.broadcasted_iota(jnp.int32, (RB, 128), 0)
    plane = lax.broadcasted_iota(jnp.int32, (RB, 128), 1)
    pos = jnp.zeros((RB, 128), jnp.int32)
    for b in range(RB):
        pos = jnp.where(prow == b, pos_ref[b], pos)
    half = HD // 2
    freq = jnp.exp(lax.rem(plane, half).astype(F32) * (-math.log(ROPE_BASE) * 2.0 / HD))
    angle = pos.astype(F32) * freq
    cos_t = jnp.cos(angle)
    first = lax.rem(plane, HD) < half
    sin_t = jnp.where(first, -jnp.sin(angle), jnp.sin(angle))

    for i in range(1, W):
        arrived(("stat", i))
    tot = stat_send[...]
    for i in range(1, W):
        tot = tot + stat_recv[i - 1]
    cols = jnp.concatenate([tot, jnp.zeros((R - 8, R), F32)], axis=0).T
    mean = cols[:, 0:1] / model_width
    var = cols[:, 1:2] / model_width - mean * mean
    rstd = lax.rsqrt(var + LN_EPS)
    loads["lna"].wait()
    loads["lnm"].wait()
    cen = (x_v[...].astype(F32) - mean) * rstd
    ha_v[...] = (cen * lna_v[0:1, :] + lna_v[1:2, :]).astype(BF16)
    hm_v[...] = (cen * lnm_v[0:1, :] + lnm_v[1:2, :]).astype(BF16)

    legs = {
        "1r": (0, 2, 0, None, right), "1l": (1, 2, 1, None, left),
        "2r": (2, 1, 1, None, right), "2l": (3, 3, 0, None, left),
        "3r": (4, 1, 0, 0, right), "3l": (5, 3, 1, 1, left),
    }

    def leg(tag, key, own, stage, landing):
        i, o, h, add, to = legs[key]
        val = own(o, h)
        if add is not None:
            arrived((tag, add))
            val = val + landing[add].astype(F32)
        stage[i] = val.astype(BF16)
        send((tag, i), stage.at[i], landing.at[i], "tpw", to)

    def total(tag, h, own, landing):
        val = own(0, h)
        for i in ((3, 4), (2, 5))[h]:
            arrived((tag, i))
            val = val + landing[i].astype(F32)
        return val

    def qmm(g):
        need(("qkv", g))
        part = dot(ha_v[...], wqkv_v[g], NT).astype(BF16)
        qpart[g] = part.reshape(NX, 2, RB, qw)
        send(("qs", g), qpart.at[g, :, 1 - c], qsib.at[g], "tpw", sib)

    def qkv_own(o, g):
        arrived(("qs", g))
        return qpart[g, chip(o), c].astype(F32) + qsib[g, chip(o)].astype(F32)

    def qm(key):
        leg("q", key, qkv_own, qsend, qrecv)

    def umm(i):
        need(("up", i))
        for k in range(2):
            upart[i, k] = dot(hm_v[...], wup_v[i, :, k * HB:(k + 1) * HB]).astype(BF16)
        send(("us", i), upart.at[i, 1 - c], usib.at[i], "tpw", sib)

    def up_own(r):
        def own(o, h):
            i = PIECES.index((o, h))
            arrived(("us", i))
            rows = slice(r * RG, (r + 1) * RG)
            return upart[i, c, rows].astype(F32) + usib[i, rows].astype(F32)

        return own

    def um(r, key):
        leg(("u", r), key, up_own(r), usend.at[r], urecv.at[r])

    mine = pl.ds(pl.multiple_of(c * HB, HB), HB)

    def act_send(r, name, o, h, to, to_o, *part):
        rows = pl.ds(part[0] * RL, RL) if part else pl.ds(r * RG, RG)
        src = act_all.at[ARRIVALS.index((o, h)), rows, mine]
        dst = act_all.at[ARRIVALS.index((to_o, h)), rows, mine]
        send(("a", r, name), src, dst, "tpw", to)

    def act(r, key):
        if key in ("0", "1"):
            h = int(key)
            pre = total(("u", r), h, up_own(r), urecv.at[r])
            val = 0.5 * pre * (1.0 + lax.erf(pre * (2.0 ** -0.5)))
            act_all[ARRIVALS.index((0, h)), r * RG:(r + 1) * RG, mine] = val.astype(BF16)
            if h == 0:
                act_send(r, "1r", 0, 0, right, 3)
            else:
                act_send(r, "1l", 0, 1, left, 1)
            act_send(r, ("s", 0, h), 0, h, sib, 0)
        elif key == "2r":
            act_send(r, "2r", 0, 1, right, 3)
        elif key == "2l":
            act_send(r, "2l", 0, 0, left, 1)
        elif key == "3r":
            arrived(("a", r, "1r"))
            for j in range(LAST_GROUPS):
                act_send(r, ("3r", j), 3, 0, right, 2, j)
            act_send(r, ("s", 3, 0), 3, 0, sib, 3)
        else:
            arrived(("a", r, "1l"))
            for j in range(LAST_GROUPS):
                act_send(r, ("3l", j), 1, 1, left, 2, j)
            act_send(r, ("s", 1, 1), 1, 1, sib, 1)

    def ap(r, key):
        o, h = {"2r": (3, 1), "2l": (1, 0)}[key]
        arrived(("a", r, key))
        act_send(r, ("s", o, h), o, h, sib, o)

    def at(key, j):
        h = {"3r": 0, "3l": 1}[key]
        arrived(("a", 0, (key, j)))
        act_send(0, ("s", 2, h, j), 2, h, sib, 2, j)

    begun = set()

    def accumulate(part, *j):
        rows = slice(j[0] * RL, (j[0] + 1) * RL) if j else slice(0, R)
        if begun:
            acc[rows, :] += part
        else:
            acc[...] = part
            begun.add(0)

    def dmm(i, *j):
        o, h = ARRIVALS[i]
        arrived(("a", 0, ("s", o, h) + j))
        need(("down", i))
        if j:
            accumulate(dot(act_all[i, j[0] * RL:(j[0] + 1) * RL, :], wdn_v[i]), *j)
        else:
            accumulate(dot(act_all[i], wdn_v[i]))

    scale = HD ** -0.5
    when = lax.broadcasted_iota(jnp.int32, (2 * QT, L), 1)

    def rotary(t):
        swapped = jnp.where(first, pltpu.roll(t, 128 - half, 1), pltpu.roll(t, half, 1))
        return (t * cos_t + swapped * sin_t).astype(BF16).astype(F32)

    def qt(g):
        qkv = total("q", g, qkv_own, qrecv).astype(BF16).astype(F32)
        for t in range(QT):
            qrot[g, t * RB:(t + 1) * RB, :] = rotary(qkv[:, t * 128:(t + 1) * 128])
        last = qkv[:, QT * 128:]
        kv = jnp.where(plane < HD, rotary(last), last)
        kvrot[g] = kv
        knew_ref[:, g * HD:(g + 1) * HD] = kv[:, :HD].astype(BF16)
        vnew_ref[:, g * HD:(g + 1) * HD] = kv[:, HD:].astype(BF16)

    def att(g):
        need("k")
        need("v")

        def row(b):
            q8 = qrot[g, pl.ds(b, QT, stride=RB), :]
            q = jnp.concatenate([q8[:, :HD], q8[:, HD:]], axis=0)
            kv = kvrot[g, pl.ds(b, 1), :]
            s = dot(q.astype(BF16), k_v[b * G + g]) * scale
            s = jnp.where(when < pos_ref[b], s, -jnp.inf)
            sn = jnp.sum(q * kv[:, :HD], axis=1, keepdims=True) * scale
            m = jnp.maximum(jnp.max(s, axis=1, keepdims=True), sn)
            e = jnp.exp(s - m)
            en = jnp.exp(sn - m)
            rz = 1.0 / (jnp.sum(e, axis=1, keepdims=True) + en)
            wn = (en * rz).astype(BF16).astype(F32)
            ctx = dot((e * rz).astype(BF16), v_v[b * G + g], NT) + wn * kv[:, HD:]
            ctxs[g, pl.ds(b, QT, stride=RB), :] = jnp.concatenate([ctx[:QT], ctx[QT:]], axis=1)

        def rows(i, _):
            for j in range(8):
                row(i * 8 + j)
            return 0

        lax.fori_loop(0, RB // 8, rows, 0)
        for t in range(QT):
            ctx_all[w, g, :, t * 128:(t + 1) * 128] = ctxs[g, t * RB:(t + 1) * RB, :].astype(BF16)
        send(("c", ("s", 0, g)), ctx_all.at[w, g], ctx_all.at[w, g], "tpw", sib)

    def ctx_send(name, who, g, to):
        send(("c", name), ctx_all.at[who, g], ctx_all.at[who, g], "tpw", to)

    def ctx(key):
        if key == "1r":
            ctx_send("1r", w, 0, right)
        elif key == "1l":
            ctx_send("1l", w, 1, left)
        elif key == "2r":
            ctx_send("2r", w, 1, right)
        elif key == "2l":
            ctx_send("2l", w, 0, left)
        elif key == "3r":
            arrived(("c", "1r"))
            ctx_send("3r", left, 0, right)
            ctx_send(("s", 3, 0), left, 0, sib)
        else:
            arrived(("c", "1l"))
            ctx_send("3l", right, 1, left)
            ctx_send(("s", 1, 1), right, 1, sib)

    def pc(key):
        who, o, g = {"2r": (left, 3, 1), "2l": (right, 1, 0), "3r": (opp, 2, 0), "3l": (opp, 2, 1)}[key]
        arrived(("c", key))
        ctx_send(("s", o, g), who, g, sib)

    def amm():
        for o in range(NX):
            for g in range(G):
                arrived(("c", ("s", o, g)))
        need("out")
        n = QT * 128
        for g in range(G):
            accumulate(dot(ctx_all[:, g].reshape(R, n), wout_v[g * n:(g + 1) * n, :]))

    def ysc(j):
        ysend[j] = acc[j * RL:(j + 1) * RL, :].astype(BF16)
        for i in (2, 1, 3):
            to = lax.rem(y + i, NY)
            rows = pl.ds(pl.multiple_of(to * RY, RY), RY)
            send(("y", j, i), ysend.at[j, rows], yrecv.at[j, i - 1], "tph", to)

    def yga(j):
        rows = pl.ds(pl.multiple_of(j * RL + y * RY, RY), RY)
        tot = acc[rows, :]
        for i in range(1, NY):
            arrived(("y", j, i))
            tot = tot + yrecv[j, i - 1].astype(F32)
        xout_ref[rows, :] = (x_v[rows, :].astype(F32) + tot).astype(BF16)
        for i in (2, 1, 3):
            send(("z", j, i), xout_ref.at[rows, :], xout_ref.at[rows, :], "tph", lax.rem(y + i, NY))

    steps = {
        "qmm": qmm, "qm": qm, "umm": umm, "um": um, "a": act, "ap": ap, "at": at, "dmm": dmm, "qt": qt, "att": att,
        "c": ctx, "pc": pc, "amm": amm, "ysc": ysc, "yga": yga,
    }
    for step in ORDER:
        steps[step[0]](*step[1:])
    for name in messages:
        arrived(name)
    for cp in sent:
        cp.wait_send()


def finish_kernel(x_ref, k_ref, v_ref, xout_ref, knew_ref, vnew_ref):
    xout_ref[...] = x_ref[...]
    hd = knew_ref.shape[2]
    for g in range(knew_ref.shape[1]):
        knew_ref[:, g, :] = k_ref[:, g * hd:(g + 1) * hd]
        vnew_ref[:, g, :] = v_ref[:, g * hd:(g + 1) * hd]


def solution(mesh):
    W = mesh.shape["tpw"]
    NY = mesh.shape["tph"]
    if W != 8:
        raise ValueError("tpw")

    def local_layer(x_in, ln_attn, ln_mlp, w_qkv, w_out, w_up, w_down, k_cache, v_cache, positions):
        R, D = x_in.shape
        _, G, S, HD = w_qkv.shape
        F = w_up.shape[1]
        L = k_cache.shape[2]
        RB = R // W
        NX = W // 2
        NG = GROUPS_OF_ROWS
        RG = R // NG
        qw = S * HD
        cw = (S - 2) * HD
        QT = cw // 128
        HB = F // W // 2
        wqkv_t = jnp.transpose(w_qkv, (1, 2, 3, 0)).reshape(G * qw, D)
        k_t = jnp.swapaxes(k_cache, 2, 3).reshape(RB * G, HD, L)
        v_t = jnp.swapaxes(v_cache, 2, 3).reshape(RB * G, HD, L)
        NL = LAST_GROUPS
        n_messages = W - 1 + 2 + 6 + 8 + NG * 6 + NG * 10 + 4 * NL + 14 + NL * 6
        any_spec = pl.BlockSpec(memory_space=pl.ANY)
        vmem_spec = pl.BlockSpec(memory_space=pltpu.VMEM)
        x_out, k_new, v_new = pl.pallas_call(
            functools.partial(layer_kernel, W, NY),
            name="layer",
            out_shape=(
                pltpu.VMEM((R, D), BF16),
                pltpu.VMEM((RB, G * HD), BF16),
                pltpu.VMEM((RB, G * HD), BF16),
            ),
            in_specs=[any_spec] * 10,
            out_specs=(vmem_spec,) * 3,
            scratch_shapes=[
                pltpu.SMEM((RB,), jnp.int32),
                pltpu.VMEM((R, D), BF16),
                pltpu.VMEM((2, D), F32),
                pltpu.VMEM((2, D), F32),
                pltpu.VMEM((G, qw, D), BF16),
                pltpu.VMEM((G * cw, D), BF16),
                pltpu.VMEM((8, D, 2 * HB), BF16),
                pltpu.VMEM((8, 2 * HB, D), BF16),
                pltpu.VMEM((RB * G, HD, L), BF16),
                pltpu.VMEM((RB * G, HD, L), BF16),
                pltpu.VMEM((8, 128), F32),
                pltpu.VMEM((W - 1, 8, 128), F32),
                pltpu.VMEM((R, D), BF16),
                pltpu.VMEM((R, D), BF16),
                pltpu.VMEM((G, NX, 2, RB, qw), BF16),
                pltpu.VMEM((G, NX, RB, qw), BF16),
                pltpu.VMEM((6, RB, qw), BF16),
                pltpu.VMEM((6, RB, qw), BF16),
                pltpu.VMEM((G, QT * RB, 128), F32),
                pltpu.VMEM((G, RB, 128), F32),
                pltpu.VMEM((G, QT * RB, 128), F32),
                pltpu.VMEM((W, G, RB, cw), BF16),
                pltpu.VMEM((8, 2, R, HB), BF16),
                pltpu.VMEM((8, R, HB), BF16),
                pltpu.VMEM((NG, 6, RG, HB), BF16),
                pltpu.VMEM((NG, 6, RG, HB), BF16),
                pltpu.VMEM((8, R, 2 * HB), BF16),
                pltpu.VMEM((R, D), F32),
                pltpu.VMEM((NL, R // NL, D), BF16),
                pltpu.VMEM((NL, NY - 1, R // NL // NY, D), BF16),
                pltpu.SemaphoreType.DMA((32,)),
                pltpu.SemaphoreType.DMA((n_messages,)),
                pltpu.SemaphoreType.DMA((n_messages,)),
            ],
            compiler_params=pltpu.CompilerParams(
                collective_id=0, has_side_effects=True, vmem_limit_bytes=VMEM_LIMIT
            ),
        )(
            positions, x_in, ln_attn, ln_mlp, wqkv_t, w_out.reshape(G * cw, D), w_up, w_down, k_t, v_t,
        )
        return pl.pallas_call(
            finish_kernel,
            name="finish",
            out_shape=(
                jax.ShapeDtypeStruct((R, D), BF16),
                jax.ShapeDtypeStruct((RB, G, HD), BF16),
                jax.ShapeDtypeStruct((RB, G, HD), BF16),
            ),
            in_specs=[vmem_spec] * 3,
            out_specs=(vmem_spec,) * 3,
        )(*(pltpu.with_memory_space_constraint(a, pltpu.VMEM) for a in (x_out, k_new, v_new)))

    cache_spec = P(("dp", "tpw"), "tph", None, None)
    new_spec = P(("dp", "tpw"), "tph", None)
    in_specs = (
        P("dp", "tpw"),
        P(None, "tpw"),
        P(None, "tpw"),
        P("tpw", "tph", None, None),
        P("tph", None, None, "tpw"),
        P("tpw", "tph"),
        P("tph", "tpw"),
        cache_spec,
        cache_spec,
        P(("dp", "tpw")),
    )
    out_specs = (P("dp", "tpw"), new_spec, new_spec)
    return jax.shard_map(local_layer, mesh=mesh, in_specs=in_specs, out_specs=out_specs, check_vma=False)
```

```python
import functools
import math

import jax
import jax.numpy as jnp
from jax import lax
from jax.experimental import pallas as pl
from jax.experimental.pallas import tpu as pltpu
from jax.sharding import PartitionSpec as P

LN_EPS = 1e-5
ROPE_BASE = 10000.0
MESH = pl.DeviceIdType.MESH
F32 = jnp.float32
BF16 = jnp.bfloat16
VMEM_LIMIT = 58 << 20
GROUPS_OF_ROWS = 2
GROUPS_OF_COLUMNS = 2
NN = (((1,), (0,)), ((), ()))
NT = (((1,), (1,)), ((), ()))
PIECES = ((2, 0), (2, 1), (1, 1), (3, 0), (1, 0), (3, 1), (0, 0), (0, 1))
ARRIVALS = ((0, 0), (0, 1), (3, 0), (1, 1), (3, 1), (1, 0), (2, 0), (2, 1))

ORDER = (
    ("qmm", 0), ("qmm", 1), ("umm", 1), ("qm", "1r"), ("qm", "2l"), ("umm", 0),
    ("umm", 6), ("qm", "1l"), ("qm", "2r"), ("um", 1, "1l"), ("um", 0, "1l"), ("umm", 4),
    ("um", 1, "1r"), ("umm", 7), ("um", 0, "1r"), ("umm", 3), ("umm", 2), ("qm", "3r"),
    ("umm", 5), ("um", 0, "2l"), ("qm", "3l"), ("um", 1, "2l"), ("um", 1, "2r"), ("um", 0, "2r"),
    ("um", 1, "3l"), ("um", 1, "3r"), ("um", 0, "3l"), ("um", 0, "3r"), ("qt", 0), ("att", 0),
    ("c", "2l"), ("qt", 1), ("att", 1), ("c", "1r"), ("c", "2r"), ("c", "1l"),
    ("a", 1, "0"), ("a", 1, "2l"), ("a", 1, "1"), ("a", 1, "2r"), ("a", 0, "1"), ("a", 0, "0"),
    ("a", 0, "2l"), ("a", 0, "2r"), ("pc", "2l"), ("c", "3r"), ("dmm", 1), ("c", "3l"),
    ("pc", "2r"), ("dmm", 0), ("a", 1, "3r"), ("ap", 1, "2l"), ("ap", 1, "2r"), ("a", 1, "3l"),
    ("a", 0, "3l"), ("a", 0, "3r"), ("dmm", 3), ("ap", 0, "2r"), ("ap", 0, "2l"), ("dmm", 2),
    ("pc", "3l"), ("pc", "3r"), ("dmm", 4), ("dmm", 5), ("ap", 1, "3l"), ("ap", 1, "3r"),
    ("amm",), ("ap", 0, "3l"), ("ap", 0, "3r"), ("dmm", 7, 1), ("dmm", 6, 1), ("ysc", 1),
    ("dmm", 6, 0), ("dmm", 7, 0), ("ysc", 0), ("yga", 1), ("yga", 0),
)


def dot(a, b, dims=NN):
    return lax.dot_general(a, b, dims, preferred_element_type=F32)


def layer_kernel(
    W, NY,
    pos_hbm, x_hbm, lna_hbm, lnm_hbm, wqkv_hbm, wout_hbm, wup_hbm, wdn_hbm, k_hbm, v_hbm,
    xout_ref, knew_ref, vnew_ref,
    pos_ref, x_v, lna_v, lnm_v, wqkv_v, wout_v, wup_v, wdn_v, k_v, v_v,
    stat_send, stat_recv, ha_v, hm_v,
    qpart, qsib, qsend, qrecv, qrot, kvrot, ctxs, ctx_all,
    upart, usib, usend, urecv, act_all, acc, ysend, yrecv,
    lsem, ssem, rsem,
):
    NX = W // 2
    R, D = x_v.shape
    NG = GROUPS_OF_ROWS
    RG = R // NG
    RY = R // NY
    NC = GROUPS_OF_COLUMNS
    DC = D // NC
    RB = R // W
    G, HD = kvrot.shape[0], k_v.shape[1]
    L = k_v.shape[2]
    QT = qrot.shape[1] // RB
    HB = wup_v.shape[2] // 2
    model_width = float(D * W)

    w = lax.axis_index("tpw")
    y = lax.axis_index("tph")
    c = lax.rem(w, 2)
    x = lax.div(w, 2)
    sib = w + 1 - 2 * c
    right = lax.rem(w + 2, W)
    left = lax.rem(w + W - 2, W)
    opp = lax.rem(w + W // 2, W)

    def chip(o):
        return lax.rem(x + o, NX)

    barrier = pltpu.get_barrier_semaphore()
    for i in range(1, W):
        pl.semaphore_signal(barrier, inc=1, device_id={"tpw": lax.rem(w + i, W)}, device_id_type=MESH)
    for i in range(1, NY):
        pl.semaphore_signal(barrier, inc=1, device_id={"tph": lax.rem(y + i, NY)}, device_id_type=MESH)

    loads = {}

    def load(name, src, dst):
        cp = pltpu.make_async_copy(src, dst, lsem.at[len(loads)])
        cp.start()
        loads[name] = cp

    load("x", x_hbm, x_v)
    load("pos", pos_hbm, pos_ref)
    load("lna", lna_hbm, lna_v)
    load("lnm", lnm_hbm, lnm_v)
    qw = wqkv_v.shape[1]
    for g in range(G):
        load(("qkv", g), wqkv_hbm.at[pl.ds(g * qw, qw), :], wqkv_v.at[g])
    for i, (o, h) in enumerate(PIECES):
        col = pl.multiple_of((chip(o) * 2 + h) * 2 * HB, 2 * HB)
        load(("up", i), wup_hbm.at[:, pl.ds(col, 2 * HB)], wup_v.at[i])
    sent = []
    messages = {}

    def send(name, src, dst, axis, to):
        i = len(sent)
        cp = pltpu.make_async_remote_copy(
            src_ref=src, dst_ref=dst, send_sem=ssem.at[i], recv_sem=rsem.at[i],
            device_id={axis: to}, device_id_type=MESH,
        )
        cp.start()
        sent.append(cp)
        messages[name] = cp

    seen = set()

    def arrived(name):
        if name not in seen:
            seen.add(name)
            messages[name].wait_recv()

    def need(name):
        if name not in seen:
            seen.add(name)
            loads[name].wait()

    loads["x"].wait()
    xf = x_v[...].astype(F32)
    s1 = jnp.sum(xf, axis=1, keepdims=True)
    s2 = jnp.sum(xf * xf, axis=1, keepdims=True)
    lane = lax.broadcasted_iota(jnp.int32, (R, 128), 1)
    stat_send[...] = jnp.where(lane == 0, s1, jnp.where(lane == 1, s2, 0.0)).T[0:8, :]
    pl.semaphore_wait(barrier, W - 1 + NY - 1)
    for i in range(1, W):
        send(("stat", i), stat_send, stat_recv.at[i - 1], "tpw", lax.rem(w + i, W))

    loads["pos"].wait()
    prow = lax.broadcasted_iota(jnp.int32, (RB, 128), 0)
    plane = lax.broadcasted_iota(jnp.int32, (RB, 128), 1)
    pos = jnp.zeros((RB, 128), jnp.int32)
    for b in range(RB):
        pos = jnp.where(prow == b, pos_ref[b], pos)
    half = HD // 2
    freq = jnp.exp(lax.rem(plane, half).astype(F32) * (-math.log(ROPE_BASE) * 2.0 / HD))
    angle = pos.astype(F32) * freq
    cos_t = jnp.cos(angle)
    first = lax.rem(plane, HD) < half
    sin_t = jnp.where(first, -jnp.sin(angle), jnp.sin(angle))

    for i in range(1, W):
        arrived(("stat", i))
    tot = stat_send[...]
    for i in range(1, W):
        tot = tot + stat_recv[i - 1]
    cols = jnp.concatenate([tot, jnp.zeros((R - 8, R), F32)], axis=0).T
    mean = cols[:, 0:1] / model_width
    var = cols[:, 1:2] / model_width - mean * mean
    rstd = lax.rsqrt(var + LN_EPS)
    loads["lna"].wait()
    loads["lnm"].wait()
    cen = (x_v[...].astype(F32) - mean) * rstd
    ha_v[...] = (cen * lna_v[0:1, :] + lna_v[1:2, :]).astype(BF16)
    hm_v[...] = (cen * lnm_v[0:1, :] + lnm_v[1:2, :]).astype(BF16)

    def load_late():
        load("k", k_hbm, k_v)
        load("v", v_hbm, v_v)
        load("out", wout_hbm, wout_v)
        for i, (o, h) in enumerate(ARRIVALS):
            row = pl.multiple_of((chip(o) * 2 + h) * 2 * HB, 2 * HB)
            load(("down", i), wdn_hbm.at[pl.ds(row, 2 * HB), :], wdn_v.at[i])

    legs = {
        "1r": (0, 2, 0, None, right), "1l": (1, 2, 1, None, left),
        "2r": (2, 1, 1, None, right), "2l": (3, 3, 0, None, left),
        "3r": (4, 1, 0, 0, right), "3l": (5, 3, 1, 1, left),
    }

    def leg(tag, key, own, stage, landing):
        i, o, h, add, to = legs[key]
        val = own(o, h)
        if add is not None:
            arrived((tag, add))
            val = val + landing[add].astype(F32)
        stage[i] = val.astype(BF16)
        send((tag, i), stage.at[i], landing.at[i], "tpw", to)

    def total(tag, h, own, landing):
        val = own(0, h)
        for i in ((3, 4), (2, 5))[h]:
            arrived((tag, i))
            val = val + landing[i].astype(F32)
        return val

    def qmm(g):
        need(("qkv", g))
        part = dot(ha_v[...], wqkv_v[g], NT).astype(BF16)
        qpart[g] = part.reshape(NX, 2, RB, qw)
        send(("qs", g), qpart.at[g, :, 1 - c], qsib.at[g], "tpw", sib)

    def qkv_own(o, g):
        arrived(("qs", g))
        return qpart[g, chip(o), c].astype(F32) + qsib[g, chip(o)].astype(F32)

    def qm(key):
        leg("q", key, qkv_own, qsend, qrecv)

    def umm(i):
        need(("up", i))
        for k in range(2):
            upart[i, k] = dot(hm_v[...], wup_v[i, :, k * HB:(k + 1) * HB]).astype(BF16)
        send(("us", i), upart.at[i, 1 - c], usib.at[i], "tpw", sib)

    def up_own(r):
        def own(o, h):
            i = PIECES.index((o, h))
            arrived(("us", i))
            rows = slice(r * RG, (r + 1) * RG)
            return upart[i, c, rows].astype(F32) + usib[i, rows].astype(F32)

        return own

    def um(r, key):
        leg(("u", r), key, up_own(r), usend.at[r], urecv.at[r])

    mine = pl.ds(pl.multiple_of(c * HB, HB), HB)

    def act_send(r, name, o, h, to, to_o):
        src = act_all.at[ARRIVALS.index((o, h)), pl.ds(r * RG, RG), mine]
        dst = act_all.at[ARRIVALS.index((to_o, h)), pl.ds(r * RG, RG), mine]
        send(("a", r, name), src, dst, "tpw", to)

    def act(r, key):
        if key in ("0", "1"):
            h = int(key)
            pre = total(("u", r), h, up_own(r), urecv.at[r])
            val = 0.5 * pre * (1.0 + lax.erf(pre * (2.0 ** -0.5)))
            act_all[ARRIVALS.index((0, h)), r * RG:(r + 1) * RG, mine] = val.astype(BF16)
            if h == 0:
                act_send(r, "1r", 0, 0, right, 3)
            else:
                act_send(r, "1l", 0, 1, left, 1)
            act_send(r, ("s", 0, h), 0, h, sib, 0)
        elif key == "2r":
            act_send(r, "2r", 0, 1, right, 3)
        elif key == "2l":
            act_send(r, "2l", 0, 0, left, 1)
        elif key == "3r":
            arrived(("a", r, "1r"))
            act_send(r, "3r", 3, 0, right, 2)
            act_send(r, ("s", 3, 0), 3, 0, sib, 3)
        else:
            arrived(("a", r, "1l"))
            act_send(r, "3l", 1, 1, left, 2)
            act_send(r, ("s", 1, 1), 1, 1, sib, 1)

    def ap(r, key):
        o, h = {"2r": (3, 1), "2l": (1, 0), "3r": (2, 0), "3l": (2, 1)}[key]
        arrived(("a", r, key))
        act_send(r, ("s", o, h), o, h, sib, o)

    begun = set()

    def accumulate(part, *j):
        cols = slice(j[0] * DC, (j[0] + 1) * DC) if j else slice(0, D)
        if begun:
            acc[:, cols] += part
        else:
            acc[...] = part
            begun.add(0)

    def dmm(i, *j):
        o, h = ARRIVALS[i]
        for r in range(NG):
            arrived(("a", r, ("s", o, h)))
        need(("down", i))
        if j:
            accumulate(dot(act_all[i], wdn_v[i, :, j[0] * DC:(j[0] + 1) * DC]), *j)
        else:
            accumulate(dot(act_all[i], wdn_v[i]))

    scale = HD ** -0.5
    when = lax.broadcasted_iota(jnp.int32, (2 * QT, L), 1)

    def rotary(t):
        swapped = jnp.where(first, pltpu.roll(t, 128 - half, 1), pltpu.roll(t, half, 1))
        return (t * cos_t + swapped * sin_t).astype(BF16).astype(F32)

    def qt(g):
        qkv = total("q", g, qkv_own, qrecv).astype(BF16).astype(F32)
        for t in range(QT):
            qrot[g, t * RB:(t + 1) * RB, :] = rotary(qkv[:, t * 128:(t + 1) * 128])
        last = qkv[:, QT * 128:]
        kv = jnp.where(plane < HD, rotary(last), last)
        kvrot[g] = kv
        knew_ref[:, g * HD:(g + 1) * HD] = kv[:, :HD].astype(BF16)
        vnew_ref[:, g * HD:(g + 1) * HD] = kv[:, HD:].astype(BF16)

    def att(g):
        need("k")
        need("v")

        def row(b):
            q8 = qrot[g, pl.ds(b, QT, stride=RB), :]
            q = jnp.concatenate([q8[:, :HD], q8[:, HD:]], axis=0)
            kv = kvrot[g, pl.ds(b, 1), :]
            s = dot(q.astype(BF16), k_v[b * G + g]) * scale
            s = jnp.where(when < pos_ref[b], s, -jnp.inf)
            sn = jnp.sum(q * kv[:, :HD], axis=1, keepdims=True) * scale
            m = jnp.maximum(jnp.max(s, axis=1, keepdims=True), sn)
            e = jnp.exp(s - m)
            en = jnp.exp(sn - m)
            rz = 1.0 / (jnp.sum(e, axis=1, keepdims=True) + en)
            wn = (en * rz).astype(BF16).astype(F32)
            ctx = dot((e * rz).astype(BF16), v_v[b * G + g], NT) + wn * kv[:, HD:]
            ctxs[g, pl.ds(b, QT, stride=RB), :] = jnp.concatenate([ctx[:QT], ctx[QT:]], axis=1)

        def rows(i, _):
            for j in range(8):
                row(i * 8 + j)
            return 0

        lax.fori_loop(0, RB // 8, rows, 0)
        for t in range(QT):
            ctx_all[w, g, :, t * 128:(t + 1) * 128] = ctxs[g, t * RB:(t + 1) * RB, :].astype(BF16)
        send(("c", ("s", 0, g)), ctx_all.at[w, g], ctx_all.at[w, g], "tpw", sib)

    def ctx_send(name, who, g, to):
        send(("c", name), ctx_all.at[who, g], ctx_all.at[who, g], "tpw", to)

    def ctx(key):
        if key == "1r":
            ctx_send("1r", w, 0, right)
        elif key == "1l":
            ctx_send("1l", w, 1, left)
        elif key == "2r":
            ctx_send("2r", w, 1, right)
        elif key == "2l":
            ctx_send("2l", w, 0, left)
        elif key == "3r":
            arrived(("c", "1r"))
            ctx_send("3r", left, 0, right)
            ctx_send(("s", 3, 0), left, 0, sib)
        else:
            arrived(("c", "1l"))
            ctx_send("3l", right, 1, left)
            ctx_send(("s", 1, 1), right, 1, sib)

    def pc(key):
        who, o, g = {"2r": (left, 3, 1), "2l": (right, 1, 0), "3r": (opp, 2, 0), "3l": (opp, 2, 1)}[key]
        arrived(("c", key))
        ctx_send(("s", o, g), who, g, sib)

    def amm():
        for o in range(NX):
            for g in range(G):
                arrived(("c", ("s", o, g)))
        need("out")
        n = QT * 128
        for g in range(G):
            accumulate(dot(ctx_all[:, g].reshape(R, n), wout_v[g * n:(g + 1) * n, :]))

    def ysc(j):
        for i in (2, 1, 3):
            to = lax.rem(y + i, NY)
            rows = pl.ds(pl.multiple_of(to * RY, RY), RY)
            ysend[j, rows, :] = acc[rows, j * DC:(j + 1) * DC].astype(BF16)
            send(("y", j, i), ysend.at[j, rows], yrecv.at[j, i - 1], "tph", to)

    def yga(j):
        rows = pl.ds(pl.multiple_of(y * RY, RY), RY)
        cols = slice(j * DC, (j + 1) * DC)
        tot = acc[rows, cols]
        for i in range(1, NY):
            arrived(("y", j, i))
            tot = tot + yrecv[j, i - 1].astype(F32)
        xout_ref[rows, cols] = (x_v[rows, cols].astype(F32) + tot).astype(BF16)
        block = xout_ref.at[rows, pl.ds(j * DC, DC)]
        for i in (2, 1, 3):
            send(("z", j, i), block, block, "tph", lax.rem(y + i, NY))

    steps = {
        "qmm": qmm, "qm": qm, "umm": umm, "um": um, "a": act, "ap": ap, "dmm": dmm, "qt": qt, "att": att,
        "c": ctx, "pc": pc, "amm": amm, "ysc": ysc, "yga": yga,
    }
    last_up = max(i for i, step in enumerate(ORDER) if step[0] == "umm")
    first_sum = min(i for i, step in enumerate(ORDER) if step[0] == "yga")
    done = 0
    for i, step in enumerate(ORDER):
        if i == first_sum:
            for cp in sent:
                cp.wait_send()
            done = len(sent)
        steps[step[0]](*step[1:])
        if i == last_up:
            load_late()
    for name in messages:
        arrived(name)
    for cp in sent[done:]:
        cp.wait_send()


def finish_kernel(x_ref, k_ref, v_ref, xout_ref, knew_ref, vnew_ref, sem):
    cp = pltpu.make_async_copy(x_ref, xout_ref, sem)
    cp.start()
    hd = knew_ref.shape[2]
    for g in range(knew_ref.shape[1]):
        knew_ref[:, g, :] = k_ref[:, g * hd:(g + 1) * hd]
        vnew_ref[:, g, :] = v_ref[:, g * hd:(g + 1) * hd]
    cp.wait()


def solution(mesh):
    W = mesh.shape["tpw"]
    NY = mesh.shape["tph"]
    if W != 8:
        raise ValueError("tpw")

    def local_layer(x_in, ln_attn, ln_mlp, w_qkv, w_out, w_up, w_down, k_cache, v_cache, positions):
        R, D = x_in.shape
        _, G, S, HD = w_qkv.shape
        F = w_up.shape[1]
        L = k_cache.shape[2]
        RB = R // W
        NX = W // 2
        NG = GROUPS_OF_ROWS
        RG = R // NG
        qw = S * HD
        cw = (S - 2) * HD
        QT = cw // 128
        HB = F // W // 2
        wqkv_t = jnp.transpose(w_qkv, (1, 2, 3, 0)).reshape(G * qw, D)
        k_t = jnp.swapaxes(k_cache, 2, 3).reshape(RB * G, HD, L)
        v_t = jnp.swapaxes(v_cache, 2, 3).reshape(RB * G, HD, L)
        NC = GROUPS_OF_COLUMNS
        n_messages = W - 1 + 2 + 6 + 8 + NG * 6 + NG * 14 + 14 + NC * 6
        any_spec = pl.BlockSpec(memory_space=pl.ANY)
        vmem_spec = pl.BlockSpec(memory_space=pltpu.VMEM)
        x_out, k_new, v_new = pl.pallas_call(
            functools.partial(layer_kernel, W, NY),
            name="layer",
            out_shape=(
                pltpu.VMEM((R, D), BF16),
                pltpu.VMEM((RB, G * HD), BF16),
                pltpu.VMEM((RB, G * HD), BF16),
            ),
            in_specs=[any_spec] * 10,
            out_specs=(vmem_spec,) * 3,
            scratch_shapes=[
                pltpu.SMEM((RB,), jnp.int32),
                pltpu.VMEM((R, D), BF16),
                pltpu.VMEM((2, D), F32),
                pltpu.VMEM((2, D), F32),
                pltpu.VMEM((G, qw, D), BF16),
                pltpu.VMEM((G * cw, D), BF16),
                pltpu.VMEM((8, D, 2 * HB), BF16),
                pltpu.VMEM((8, 2 * HB, D), BF16),
                pltpu.VMEM((RB * G, HD, L), BF16),
                pltpu.VMEM((RB * G, HD, L), BF16),
                pltpu.VMEM((8, 128), F32),
                pltpu.VMEM((W - 1, 8, 128), F32),
                pltpu.VMEM((R, D), BF16),
                pltpu.VMEM((R, D), BF16),
                pltpu.VMEM((G, NX, 2, RB, qw), BF16),
                pltpu.VMEM((G, NX, RB, qw), BF16),
                pltpu.VMEM((6, RB, qw), BF16),
                pltpu.VMEM((6, RB, qw), BF16),
                pltpu.VMEM((G, QT * RB, 128), F32),
                pltpu.VMEM((G, RB, 128), F32),
                pltpu.VMEM((G, QT * RB, 128), F32),
                pltpu.VMEM((W, G, RB, cw), BF16),
                pltpu.VMEM((8, 2, R, HB), BF16),
                pltpu.VMEM((8, R, HB), BF16),
                pltpu.VMEM((NG, 6, RG, HB), BF16),
                pltpu.VMEM((NG, 6, RG, HB), BF16),
                pltpu.VMEM((8, R, 2 * HB), BF16),
                pltpu.VMEM((R, D), F32),
                pltpu.VMEM((NC, R, D // NC), BF16),
                pltpu.VMEM((NC, NY - 1, R // NY, D // NC), BF16),
                pltpu.SemaphoreType.DMA((32,)),
                pltpu.SemaphoreType.DMA((n_messages,)),
                pltpu.SemaphoreType.DMA((n_messages,)),
            ],
            compiler_params=pltpu.CompilerParams(
                collective_id=0, has_side_effects=True, vmem_limit_bytes=VMEM_LIMIT
            ),
        )(
            positions, x_in, ln_attn, ln_mlp, wqkv_t, w_out.reshape(G * cw, D), w_up, w_down, k_t, v_t,
        )
        return pl.pallas_call(
            finish_kernel,
            name="finish",
            out_shape=(
                jax.ShapeDtypeStruct((R, D), BF16),
                jax.ShapeDtypeStruct((RB, G, HD), BF16),
                jax.ShapeDtypeStruct((RB, G, HD), BF16),
            ),
            in_specs=[vmem_spec] * 3,
            out_specs=(any_spec, vmem_spec, vmem_spec),
            scratch_shapes=[pltpu.SemaphoreType.DMA],
        )(*(pltpu.with_memory_space_constraint(a, pltpu.VMEM) for a in (x_out, k_new, v_new)))

    cache_spec = P(("dp", "tpw"), "tph", None, None)
    new_spec = P(("dp", "tpw"), "tph", None)
    in_specs = (
        P("dp", "tpw"),
        P(None, "tpw"),
        P(None, "tpw"),
        P("tpw", "tph", None, None),
        P("tph", None, None, "tpw"),
        P("tpw", "tph"),
        P("tph", "tpw"),
        cache_spec,
        cache_spec,
        P(("dp", "tpw")),
    )
    out_specs = (P("dp", "tpw"), new_spec, new_spec)
    return jax.shard_map(local_layer, mesh=mesh, in_specs=in_specs, out_specs=out_specs, check_vma=False)
```

```python
import functools
import math

import jax
import jax.numpy as jnp
from jax import lax
from jax.experimental import pallas as pl
from jax.experimental.pallas import tpu as pltpu
from jax.sharding import PartitionSpec as P

LN_EPS = 1e-5
ROPE_BASE = 10000.0
MESH = pl.DeviceIdType.MESH
F32 = jnp.float32
BF16 = jnp.bfloat16
VMEM_LIMIT = 58 << 20
GROUPS_OF_ROWS = 2
GROUPS_OF_COLUMNS = 2
NN = (((1,), (0,)), ((), ()))
NT = (((1,), (1,)), ((), ()))
PIECES = ((2, 0), (2, 1), (1, 1), (3, 0), (1, 0), (3, 1), (0, 0), (0, 1))
ARRIVALS = ((0, 0), (0, 1), (3, 0), (1, 1), (3, 1), (1, 0), (2, 0), (2, 1))

ORDER = (
    ("qmm", 0), ("qmm", 1), ("umm", 1), ("qm", "1r"), ("qm", "2l"), ("umm", 0),
    ("umm", 6), ("qm", "1l"), ("qm", "2r"), ("um", 1, "1l"), ("um", 0, "1l"), ("umm", 4),
    ("um", 1, "1r"), ("umm", 7), ("um", 0, "1r"), ("umm", 3), ("umm", 2), ("qm", "3r"),
    ("umm", 5), ("um", 0, "2l"), ("qm", "3l"), ("um", 1, "2l"), ("um", 1, "2r"), ("um", 0, "2r"),
    ("um", 1, "3l"), ("um", 1, "3r"), ("um", 0, "3l"), ("um", 0, "3r"), ("qt", 0), ("att", 0),
    ("c", "2l"), ("qt", 1), ("att", 1), ("c", "1r"), ("c", "2r"), ("c", "1l"),
    ("a", 1, "0"), ("a", 1, "2l"), ("a", 1, "1"), ("a", 1, "2r"), ("a", 0, "1"), ("a", 0, "0"),
    ("a", 0, "2l"), ("a", 0, "2r"), ("pc", "2l"), ("c", "3r"), ("dmm", 1), ("c", "3l"),
    ("pc", "2r"), ("dmm", 0), ("a", 1, "3r"), ("ap", 1, "2l"), ("ap", 1, "2r"), ("a", 1, "3l"),
    ("a", 0, "3l"), ("a", 0, "3r"), ("dmm", 3), ("ap", 0, "2r"), ("ap", 0, "2l"), ("dmm", 2),
    ("pc", "3l"), ("pc", "3r"), ("dmm", 4), ("dmm", 5), ("ap", 1, "3l"), ("ap", 1, "3r"),
    ("amm",), ("ap", 0, "3l"), ("ap", 0, "3r"), ("last", 1), ("ysc", 1), ("last", 0),
    ("ysc", 0), ("yga", 1), ("yga", 0),
)


def dot(a, b, dims=NN):
    return lax.dot_general(a, b, dims, preferred_element_type=F32)


def layer_kernel(
    W, NY,
    pos_hbm, x_hbm, lna_hbm, lnm_hbm, wqkv_hbm, wout_hbm, wup_hbm, wdn_hbm, k_hbm, v_hbm,
    xout_ref, knew_ref, vnew_ref,
    pos_ref, x_v, lna_v, lnm_v, wqkv_v, wout_v, wup_v, wdn_v, k_v, v_v,
    stat_send, stat_recv, ha_v, hm_v,
    qpart, qsib, qsend, qrecv, qrot, kvrot, ctxs, ctx_all,
    upart, usib, usend, urecv, act_all, acc, ysend, yrecv,
    lsem, ssem, rsem,
):
    NX = W // 2
    R, D = x_v.shape
    NG = GROUPS_OF_ROWS
    RG = R // NG
    RY = R // NY
    NC = GROUPS_OF_COLUMNS
    DC = D // NC
    RB = R // W
    G, HD = kvrot.shape[0], k_v.shape[1]
    L = k_v.shape[2]
    QT = qrot.shape[1] // RB
    HB = wup_v.shape[2] // 2
    model_width = float(D * W)

    w = lax.axis_index("tpw")
    y = lax.axis_index("tph")
    c = lax.rem(w, 2)
    x = lax.div(w, 2)
    sib = w + 1 - 2 * c
    right = lax.rem(w + 2, W)
    left = lax.rem(w + W - 2, W)
    opp = lax.rem(w + W // 2, W)

    def chip(o):
        return lax.rem(x + o, NX)

    barrier = pltpu.get_barrier_semaphore()
    for i in range(1, W):
        pl.semaphore_signal(barrier, inc=1, device_id={"tpw": lax.rem(w + i, W)}, device_id_type=MESH)
    for i in range(1, NY):
        pl.semaphore_signal(barrier, inc=1, device_id={"tph": lax.rem(y + i, NY)}, device_id_type=MESH)

    loads = {}

    def load(name, src, dst):
        cp = pltpu.make_async_copy(src, dst, lsem.at[len(loads)])
        cp.start()
        loads[name] = cp

    load("x", x_hbm, x_v)
    load("pos", pos_hbm, pos_ref)
    load("lna", lna_hbm, lna_v)
    load("lnm", lnm_hbm, lnm_v)
    qw = wqkv_v.shape[1]
    for g in range(G):
        load(("qkv", g), wqkv_hbm.at[pl.ds(g * qw, qw), :], wqkv_v.at[g])
    for i, (o, h) in enumerate(PIECES):
        col = pl.multiple_of((chip(o) * 2 + h) * 2 * HB, 2 * HB)
        load(("up", i), wup_hbm.at[:, pl.ds(col, 2 * HB)], wup_v.at[i])
    sent = []
    messages = {}

    def send(name, src, dst, axis, to):
        i = len(sent)
        cp = pltpu.make_async_remote_copy(
            src_ref=src, dst_ref=dst, send_sem=ssem.at[i], recv_sem=rsem.at[i],
            device_id={axis: to}, device_id_type=MESH,
        )
        cp.start()
        sent.append(cp)
        messages[name] = cp

    seen = set()

    def arrived(name):
        if name not in seen:
            seen.add(name)
            messages[name].wait_recv()

    def need(name):
        if name not in seen:
            seen.add(name)
            loads[name].wait()

    loads["x"].wait()
    xf = x_v[...].astype(F32)
    s1 = jnp.sum(xf, axis=1, keepdims=True)
    s2 = jnp.sum(xf * xf, axis=1, keepdims=True)
    lane = lax.broadcasted_iota(jnp.int32, (R, 128), 1)
    stat_send[...] = jnp.where(lane == 0, s1, jnp.where(lane == 1, s2, 0.0)).T[0:8, :]
    pl.semaphore_wait(barrier, W - 1 + NY - 1)
    for i in range(1, W):
        send(("stat", i), stat_send, stat_recv.at[i - 1], "tpw", lax.rem(w + i, W))

    loads["pos"].wait()
    prow = lax.broadcasted_iota(jnp.int32, (RB, 128), 0)
    plane = lax.broadcasted_iota(jnp.int32, (RB, 128), 1)
    pos = jnp.zeros((RB, 128), jnp.int32)
    for b in range(RB):
        pos = jnp.where(prow == b, pos_ref[b], pos)
    half = HD // 2
    freq = jnp.exp(lax.rem(plane, half).astype(F32) * (-math.log(ROPE_BASE) * 2.0 / HD))
    angle = pos.astype(F32) * freq
    cos_t = jnp.cos(angle)
    first = lax.rem(plane, HD) < half
    sin_t = jnp.where(first, -jnp.sin(angle), jnp.sin(angle))

    for i in range(1, W):
        arrived(("stat", i))
    tot = stat_send[...]
    for i in range(1, W):
        tot = tot + stat_recv[i - 1]
    cols = jnp.concatenate([tot, jnp.zeros((R - 8, R), F32)], axis=0).T
    mean = cols[:, 0:1] / model_width
    var = cols[:, 1:2] / model_width - mean * mean
    rstd = lax.rsqrt(var + LN_EPS)
    loads["lna"].wait()
    loads["lnm"].wait()
    cen = (x_v[...].astype(F32) - mean) * rstd
    ha_v[...] = (cen * lna_v[0:1, :] + lna_v[1:2, :]).astype(BF16)
    hm_v[...] = (cen * lnm_v[0:1, :] + lnm_v[1:2, :]).astype(BF16)

    def load_late():
        load("k", k_hbm, k_v)
        load("v", v_hbm, v_v)
        load("out", wout_hbm, wout_v)
        for i, (o, h) in enumerate(ARRIVALS):
            row = pl.multiple_of((chip(o) * 2 + h) * 2 * HB, 2 * HB)
            load(("down", i), wdn_hbm.at[pl.ds(row, 2 * HB), :], wdn_v.at[i])

    legs = {
        "1r": (0, 2, 0, None, right), "1l": (1, 2, 1, None, left),
        "2r": (2, 1, 1, None, right), "2l": (3, 3, 0, None, left),
        "3r": (4, 1, 0, 0, right), "3l": (5, 3, 1, 1, left),
    }

    def leg(tag, key, own, stage, landing):
        i, o, h, add, to = legs[key]
        val = own(o, h)
        if add is not None:
            arrived((tag, add))
            val = val + landing[add].astype(F32)
        stage[i] = val.astype(BF16)
        send((tag, i), stage.at[i], landing.at[i], "tpw", to)

    def total(tag, h, own, landing):
        val = own(0, h)
        for i in ((3, 4), (2, 5))[h]:
            arrived((tag, i))
            val = val + landing[i].astype(F32)
        return val

    def qmm(g):
        need(("qkv", g))
        part = dot(ha_v[...], wqkv_v[g], NT).astype(BF16)
        qpart[g] = part.reshape(NX, 2, RB, qw)
        send(("qs", g), qpart.at[g, :, 1 - c], qsib.at[g], "tpw", sib)

    def qkv_own(o, g):
        arrived(("qs", g))
        return qpart[g, chip(o), c].astype(F32) + qsib[g, chip(o)].astype(F32)

    def qm(key):
        leg("q", key, qkv_own, qsend, qrecv)

    def umm(i):
        need(("up", i))
        for k in range(2):
            upart[i, k] = dot(hm_v[...], wup_v[i, :, k * HB:(k + 1) * HB]).astype(BF16)
        send(("us", i), upart.at[i, 1 - c], usib.at[i], "tpw", sib)

    def up_own(r):
        def own(o, h):
            i = PIECES.index((o, h))
            arrived(("us", i))
            rows = slice(r * RG, (r + 1) * RG)
            return upart[i, c, rows].astype(F32) + usib[i, rows].astype(F32)

        return own

    def um(r, key):
        leg(("u", r), key, up_own(r), usend.at[r], urecv.at[r])

    mine = pl.ds(pl.multiple_of(c * HB, HB), HB)

    def act_send(r, name, o, h, to, to_o):
        src = act_all.at[ARRIVALS.index((o, h)), pl.ds(r * RG, RG), mine]
        dst = act_all.at[ARRIVALS.index((to_o, h)), pl.ds(r * RG, RG), mine]
        send(("a", r, name), src, dst, "tpw", to)

    def act(r, key):
        if key in ("0", "1"):
            h = int(key)
            pre = total(("u", r), h, up_own(r), urecv.at[r])
            val = 0.5 * pre * (1.0 + lax.erf(pre * (2.0 ** -0.5)))
            act_all[ARRIVALS.index((0, h)), r * RG:(r + 1) * RG, mine] = val.astype(BF16)
            if h == 0:
                act_send(r, "1r", 0, 0, right, 3)
            else:
                act_send(r, "1l", 0, 1, left, 1)
            act_send(r, ("s", 0, h), 0, h, sib, 0)
        elif key == "2r":
            act_send(r, "2r", 0, 1, right, 3)
        elif key == "2l":
            act_send(r, "2l", 0, 0, left, 1)
        elif key == "3r":
            arrived(("a", r, "1r"))
            act_send(r, "3r", 3, 0, right, 2)
            act_send(r, ("s", 3, 0), 3, 0, sib, 3)
        else:
            arrived(("a", r, "1l"))
            act_send(r, "3l", 1, 1, left, 2)
            act_send(r, ("s", 1, 1), 1, 1, sib, 1)

    def ap(r, key):
        o, h = {"2r": (3, 1), "2l": (1, 0), "3r": (2, 0), "3l": (2, 1)}[key]
        arrived(("a", r, key))
        act_send(r, ("s", o, h), o, h, sib, o)

    begun = set()

    def accumulate(part, *j):
        cols = slice(j[0] * DC, (j[0] + 1) * DC) if j else slice(0, D)
        if begun:
            acc[:, cols] += part
        else:
            acc[...] = part
            begun.add(0)

    def ready(i):
        o, h = ARRIVALS[i]
        for r in range(NG):
            arrived(("a", r, ("s", o, h)))
        need(("down", i))

    def dmm(i):
        ready(i)
        accumulate(dot(act_all[i], wdn_v[i]))

    def last(j):
        cols = slice(j * DC, (j + 1) * DC)
        n = len(ARRIVALS)
        ready(n - 2)
        ready(n - 1)
        accumulate(dot(act_all[n - 2], wdn_v[n - 2, :, cols]) + dot(act_all[n - 1], wdn_v[n - 1, :, cols]), j)

    scale = HD ** -0.5
    when = lax.broadcasted_iota(jnp.int32, (2 * QT, L), 1)

    def rotary(t):
        swapped = jnp.where(first, pltpu.roll(t, 128 - half, 1), pltpu.roll(t, half, 1))
        return (t * cos_t + swapped * sin_t).astype(BF16).astype(F32)

    def qt(g):
        qkv = total("q", g, qkv_own, qrecv).astype(BF16).astype(F32)
        for t in range(QT):
            qrot[g, t * RB:(t + 1) * RB, :] = rotary(qkv[:, t * 128:(t + 1) * 128])
        last = qkv[:, QT * 128:]
        kv = jnp.where(plane < HD, rotary(last), last)
        kvrot[g] = kv
        knew_ref[:, g * HD:(g + 1) * HD] = kv[:, :HD].astype(BF16)
        vnew_ref[:, g * HD:(g + 1) * HD] = kv[:, HD:].astype(BF16)

    def att(g):
        need("k")
        need("v")

        def row(b):
            q8 = qrot[g, pl.ds(b, QT, stride=RB), :]
            q = jnp.concatenate([q8[:, :HD], q8[:, HD:]], axis=0)
            kv = kvrot[g, pl.ds(b, 1), :]
            s = dot(q.astype(BF16), k_v[b * G + g]) * scale
            s = jnp.where(when < pos_ref[b], s, -jnp.inf)
            sn = jnp.sum(q * kv[:, :HD], axis=1, keepdims=True) * scale
            m = jnp.maximum(jnp.max(s, axis=1, keepdims=True), sn)
            e = jnp.exp(s - m)
            en = jnp.exp(sn - m)
            rz = 1.0 / (jnp.sum(e, axis=1, keepdims=True) + en)
            wn = (en * rz).astype(BF16).astype(F32)
            ctx = dot((e * rz).astype(BF16), v_v[b * G + g], NT) + wn * kv[:, HD:]
            ctxs[g, pl.ds(b, QT, stride=RB), :] = jnp.concatenate([ctx[:QT], ctx[QT:]], axis=1)

        def rows(i, _):
            for j in range(8):
                row(i * 8 + j)
            return 0

        lax.fori_loop(0, RB // 8, rows, 0)
        for t in range(QT):
            ctx_all[w, g, :, t * 128:(t + 1) * 128] = ctxs[g, t * RB:(t + 1) * RB, :].astype(BF16)
        send(("c", ("s", 0, g)), ctx_all.at[w, g], ctx_all.at[w, g], "tpw", sib)

    def ctx_send(name, who, g, to):
        send(("c", name), ctx_all.at[who, g], ctx_all.at[who, g], "tpw", to)

    def ctx(key):
        if key == "1r":
            ctx_send("1r", w, 0, right)
        elif key == "1l":
            ctx_send("1l", w, 1, left)
        elif key == "2r":
            ctx_send("2r", w, 1, right)
        elif key == "2l":
            ctx_send("2l", w, 0, left)
        elif key == "3r":
            arrived(("c", "1r"))
            ctx_send("3r", left, 0, right)
            ctx_send(("s", 3, 0), left, 0, sib)
        else:
            arrived(("c", "1l"))
            ctx_send("3l", right, 1, left)
            ctx_send(("s", 1, 1), right, 1, sib)

    def pc(key):
        who, o, g = {"2r": (left, 3, 1), "2l": (right, 1, 0), "3r": (opp, 2, 0), "3l": (opp, 2, 1)}[key]
        arrived(("c", key))
        ctx_send(("s", o, g), who, g, sib)

    def amm():
        for o in range(NX):
            for g in range(G):
                arrived(("c", ("s", o, g)))
        need("out")
        n = QT * 128
        for g in range(G):
            accumulate(dot(ctx_all[:, g].reshape(R, n), wout_v[g * n:(g + 1) * n, :]))

    def ysc(j):
        for i in (2, 1, 3):
            to = lax.rem(y + i, NY)
            rows = pl.ds(pl.multiple_of(to * RY, RY), RY)
            ysend[j, rows, :] = acc[rows, j * DC:(j + 1) * DC].astype(BF16)
            send(("y", j, i), ysend.at[j, rows], yrecv.at[j, i - 1], "tph", to)

    def yga(j):
        rows = pl.ds(pl.multiple_of(y * RY, RY), RY)
        cols = slice(j * DC, (j + 1) * DC)
        tot = acc[rows, cols]
        for i in range(1, NY):
            arrived(("y", j, i))
            tot = tot + yrecv[j, i - 1].astype(F32)
        xout_ref[rows, cols] = (x_v[rows, cols].astype(F32) + tot).astype(BF16)
        block = xout_ref.at[rows, pl.ds(j * DC, DC)]
        for i in (2, 1, 3):
            send(("z", j, i), block, block, "tph", lax.rem(y + i, NY))

    steps = {
        "qmm": qmm, "qm": qm, "umm": umm, "um": um, "a": act, "ap": ap, "dmm": dmm, "last": last, "qt": qt, "att": att,
        "c": ctx, "pc": pc, "amm": amm, "ysc": ysc, "yga": yga,
    }
    last_up = max(i for i, step in enumerate(ORDER) if step[0] == "umm")
    first_sum = min(i for i, step in enumerate(ORDER) if step[0] == "yga")
    done = 0
    for i, step in enumerate(ORDER):
        if i == first_sum:
            for cp in sent:
                cp.wait_send()
            done = len(sent)
        steps[step[0]](*step[1:])
        if i == last_up:
            load_late()
    for name in messages:
        arrived(name)
    for cp in sent[done:]:
        cp.wait_send()


def finish_kernel(x_ref, k_ref, v_ref, xout_ref, knew_ref, vnew_ref):
    xout_ref[...] = x_ref[...]
    hd = knew_ref.shape[2]
    for g in range(knew_ref.shape[1]):
        knew_ref[:, g, :] = k_ref[:, g * hd:(g + 1) * hd]
        vnew_ref[:, g, :] = v_ref[:, g * hd:(g + 1) * hd]


def solution(mesh):
    W = mesh.shape["tpw"]
    NY = mesh.shape["tph"]
    if W != 8:
        raise ValueError("tpw")

    def local_layer(x_in, ln_attn, ln_mlp, w_qkv, w_out, w_up, w_down, k_cache, v_cache, positions):
        R, D = x_in.shape
        _, G, S, HD = w_qkv.shape
        F = w_up.shape[1]
        L = k_cache.shape[2]
        RB = R // W
        NX = W // 2
        NG = GROUPS_OF_ROWS
        RG = R // NG
        qw = S * HD
        cw = (S - 2) * HD
        QT = cw // 128
        HB = F // W // 2
        wqkv_t = jnp.transpose(w_qkv, (1, 2, 3, 0)).reshape(G * qw, D)
        k_t = jnp.swapaxes(k_cache, 2, 3).reshape(RB * G, HD, L)
        v_t = jnp.swapaxes(v_cache, 2, 3).reshape(RB * G, HD, L)
        NC = GROUPS_OF_COLUMNS
        n_messages = W - 1 + 2 + 6 + 8 + NG * 6 + NG * 14 + 14 + NC * 6
        any_spec = pl.BlockSpec(memory_space=pl.ANY)
        vmem_spec = pl.BlockSpec(memory_space=pltpu.VMEM)
        x_out, k_new, v_new = pl.pallas_call(
            functools.partial(layer_kernel, W, NY),
            name="layer",
            out_shape=(
                pltpu.VMEM((R, D), BF16),
                pltpu.VMEM((RB, G * HD), BF16),
                pltpu.VMEM((RB, G * HD), BF16),
            ),
            in_specs=[any_spec] * 10,
            out_specs=(vmem_spec,) * 3,
            scratch_shapes=[
                pltpu.SMEM((RB,), jnp.int32),
                pltpu.VMEM((R, D), BF16),
                pltpu.VMEM((2, D), F32),
                pltpu.VMEM((2, D), F32),
                pltpu.VMEM((G, qw, D), BF16),
                pltpu.VMEM((G * cw, D), BF16),
                pltpu.VMEM((8, D, 2 * HB), BF16),
                pltpu.VMEM((8, 2 * HB, D), BF16),
                pltpu.VMEM((RB * G, HD, L), BF16),
                pltpu.VMEM((RB * G, HD, L), BF16),
                pltpu.VMEM((8, 128), F32),
                pltpu.VMEM((W - 1, 8, 128), F32),
                pltpu.VMEM((R, D), BF16),
                pltpu.VMEM((R, D), BF16),
                pltpu.VMEM((G, NX, 2, RB, qw), BF16),
                pltpu.VMEM((G, NX, RB, qw), BF16),
                pltpu.VMEM((6, RB, qw), BF16),
                pltpu.VMEM((6, RB, qw), BF16),
                pltpu.VMEM((G, QT * RB, 128), F32),
                pltpu.VMEM((G, RB, 128), F32),
                pltpu.VMEM((G, QT * RB, 128), F32),
                pltpu.VMEM((W, G, RB, cw), BF16),
                pltpu.VMEM((8, 2, R, HB), BF16),
                pltpu.VMEM((8, R, HB), BF16),
                pltpu.VMEM((NG, 6, RG, HB), BF16),
                pltpu.VMEM((NG, 6, RG, HB), BF16),
                pltpu.VMEM((8, R, 2 * HB), BF16),
                pltpu.VMEM((R, D), F32),
                pltpu.VMEM((NC, R, D // NC), BF16),
                pltpu.VMEM((NC, NY - 1, R // NY, D // NC), BF16),
                pltpu.SemaphoreType.DMA((32,)),
                pltpu.SemaphoreType.DMA((n_messages,)),
                pltpu.SemaphoreType.DMA((n_messages,)),
            ],
            compiler_params=pltpu.CompilerParams(
                collective_id=0, has_side_effects=True, vmem_limit_bytes=VMEM_LIMIT
            ),
        )(
            positions, x_in, ln_attn, ln_mlp, wqkv_t, w_out.reshape(G * cw, D), w_up, w_down, k_t, v_t,
        )
        return pl.pallas_call(
            finish_kernel,
            name="finish",
            out_shape=(
                jax.ShapeDtypeStruct((R, D), BF16),
                jax.ShapeDtypeStruct((RB, G, HD), BF16),
                jax.ShapeDtypeStruct((RB, G, HD), BF16),
            ),
            in_specs=[vmem_spec] * 3,
            out_specs=(vmem_spec,) * 3,
        )(*(pltpu.with_memory_space_constraint(a, pltpu.VMEM) for a in (x_out, k_new, v_new)))

    cache_spec = P(("dp", "tpw"), "tph", None, None)
    new_spec = P(("dp", "tpw"), "tph", None)
    in_specs = (
        P("dp", "tpw"),
        P(None, "tpw"),
        P(None, "tpw"),
        P("tpw", "tph", None, None),
        P("tph", None, None, "tpw"),
        P("tpw", "tph"),
        P("tph", "tpw"),
        cache_spec,
        cache_spec,
        P(("dp", "tpw")),
    )
    out_specs = (P("dp", "tpw"), new_spec, new_spec)
    return jax.shard_map(local_layer, mesh=mesh, in_specs=in_specs, out_specs=out_specs, check_vma=False)
```

```python
import functools
import math

import jax
import jax.numpy as jnp
from jax import lax
from jax.experimental import pallas as pl
from jax.experimental.pallas import tpu as pltpu
from jax.sharding import PartitionSpec as P

LN_EPS = 1e-5
ROPE_BASE = 10000.0
MESH = pl.DeviceIdType.MESH
F32 = jnp.float32
BF16 = jnp.bfloat16
VMEM_LIMIT = 58 << 20
GROUPS_OF_ROWS = 2
GROUPS_OF_COLUMNS = 2
NN = (((1,), (0,)), ((), ()))
NT = (((1,), (1,)), ((), ()))
PIECES = ((2, 0), (2, 1), (1, 1), (3, 0), (1, 0), (3, 1), (0, 0), (0, 1))
ARRIVALS = ((0, 0), (0, 1), (3, 0), (1, 1), (3, 1), (1, 0), (2, 0), (2, 1))

ORDER = (
    ("qmm", 0), ("qmm", 1), ("umm", 1), ("qm", "1r"), ("qm", "2l"), ("umm", 0),
    ("umm", 6), ("qm", "1l"), ("qm", "2r"), ("um", 1, "1l"), ("um", 0, "1l"), ("umm", 4),
    ("um", 1, "1r"), ("umm", 7), ("um", 0, "1r"), ("umm", 3), ("umm", 2), ("qm", "3r"),
    ("umm", 5), ("um", 0, "2l"), ("qm", "3l"), ("um", 1, "2l"), ("um", 1, "2r"), ("um", 0, "2r"),
    ("um", 1, "3l"), ("um", 1, "3r"), ("um", 0, "3l"), ("um", 0, "3r"), ("qt", 0), ("att", 0),
    ("c", "2l"), ("qt", 1), ("att", 1), ("c", "1r"), ("c", "2r"), ("c", "1l"),
    ("a", 1, "0"), ("a", 1, "2l"), ("a", 1, "1"), ("a", 1, "2r"), ("a", 0, "1"), ("a", 0, "0"),
    ("a", 0, "2l"), ("a", 0, "2r"), ("pc", "2l"), ("c", "3r"), ("dmm", 1), ("c", "3l"),
    ("pc", "2r"), ("dmm", 0), ("a", 1, "3r"), ("ap", 1, "2l"), ("ap", 1, "2r"), ("a", 1, "3l"),
    ("a", 0, "3l"), ("a", 0, "3r"), ("dmm", 3), ("ap", 0, "2r"), ("ap", 0, "2l"), ("dmm", 2),
    ("pc", "3l"), ("pc", "3r"), ("dmm", 4), ("dmm", 5), ("ap", 1, "3l"), ("ap", 1, "3r"),
    ("amm",), ("ap", 0, "3l"), ("ap", 0, "3r"), ("last", 1), ("ysc", 1), ("last", 0),
    ("ysc", 0), ("yga", 1), ("yga", 0),
)


def dot(a, b, dims=NN):
    return lax.dot_general(a, b, dims, preferred_element_type=F32)


def layer_kernel(
    W, NY,
    pos_hbm, x_hbm, lna_hbm, lnm_hbm, wqkv_hbm, wout_hbm, wup_hbm, wdn_hbm, k_hbm, v_hbm,
    xout_ref, knew_ref, vnew_ref,
    pos_ref, x_v, lna_v, lnm_v, wqkv_v, wout_v, wup_v, wdn_v, k_v, v_v,
    stat_send, stat_recv, ha_v, hm_v,
    qpart, qsib, qsend, qrecv, qrot, kvrot, ctxs, ctx_all,
    upart, usib, usend, urecv, act_all, acc, ysend, yrecv,
    lsem, ssem, rsem,
):
    NX = W // 2
    R, D = x_v.shape
    NG = GROUPS_OF_ROWS
    RG = R // NG
    RY = R // NY
    NC = GROUPS_OF_COLUMNS
    DC = D // NC
    RB = R // W
    G, HD = kvrot.shape[0], k_v.shape[1]
    L = k_v.shape[2]
    QT = qrot.shape[1] // RB
    HB = wup_v.shape[2] // 2
    model_width = float(D * W)

    w = lax.axis_index("tpw")
    y = lax.axis_index("tph")
    c = lax.rem(w, 2)
    x = lax.div(w, 2)
    sib = w + 1 - 2 * c
    right = lax.rem(w + 2, W)
    left = lax.rem(w + W - 2, W)
    opp = lax.rem(w + W // 2, W)

    def chip(o):
        return lax.rem(x + o, NX)

    barrier = pltpu.get_barrier_semaphore()
    far_first = sorted(range(1, W), key=lambda i: -min(i, W - i))
    for i in far_first:
        pl.semaphore_signal(barrier, inc=1, device_id={"tpw": lax.rem(w + i, W)}, device_id_type=MESH)
    for i in range(1, NY):
        pl.semaphore_signal(barrier, inc=1, device_id={"tph": lax.rem(y + i, NY)}, device_id_type=MESH)

    loads = {}

    def load(name, src, dst):
        cp = pltpu.make_async_copy(src, dst, lsem.at[len(loads)])
        cp.start()
        loads[name] = cp

    load("x", x_hbm, x_v)
    load("pos", pos_hbm, pos_ref)
    load("lna", lna_hbm, lna_v)
    load("lnm", lnm_hbm, lnm_v)
    qw = wqkv_v.shape[1]
    for g in range(G):
        load(("qkv", g), wqkv_hbm.at[pl.ds(g * qw, qw), :], wqkv_v.at[g])
    for i, (o, h) in enumerate(PIECES):
        col = pl.multiple_of((chip(o) * 2 + h) * 2 * HB, 2 * HB)
        load(("up", i), wup_hbm.at[:, pl.ds(col, 2 * HB)], wup_v.at[i])
    sent = []
    messages = {}

    def send(name, src, dst, axis, to):
        i = len(sent)
        cp = pltpu.make_async_remote_copy(
            src_ref=src, dst_ref=dst, send_sem=ssem.at[i], recv_sem=rsem.at[i],
            device_id={axis: to}, device_id_type=MESH,
        )
        cp.start()
        sent.append(cp)
        messages[name] = cp

    seen = set()

    def arrived(name):
        if name not in seen:
            seen.add(name)
            messages[name].wait_recv()

    def need(name):
        if name not in seen:
            seen.add(name)
            loads[name].wait()

    loads["x"].wait()
    xf = x_v[...].astype(F32)
    s1 = jnp.sum(xf, axis=1, keepdims=True)
    s2 = jnp.sum(xf * xf, axis=1, keepdims=True)
    lane = lax.broadcasted_iota(jnp.int32, (R, 128), 1)
    stat_send[...] = jnp.where(lane == 0, s1, jnp.where(lane == 1, s2, 0.0)).T[0:8, :]
    pl.semaphore_wait(barrier, W - 1 + NY - 1)
    for i in far_first:
        send(("stat", i), stat_send, stat_recv.at[i - 1], "tpw", lax.rem(w + i, W))

    loads["pos"].wait()
    prow = lax.broadcasted_iota(jnp.int32, (RB, 128), 0)
    plane = lax.broadcasted_iota(jnp.int32, (RB, 128), 1)
    pos = jnp.zeros((RB, 128), jnp.int32)
    for b in range(RB):
        pos = jnp.where(prow == b, pos_ref[b], pos)
    half = HD // 2
    freq = jnp.exp(lax.rem(plane, half).astype(F32) * (-math.log(ROPE_BASE) * 2.0 / HD))
    angle = pos.astype(F32) * freq
    cos_t = jnp.cos(angle)
    first = lax.rem(plane, HD) < half
    sin_t = jnp.where(first, -jnp.sin(angle), jnp.sin(angle))

    for i in range(1, W):
        arrived(("stat", i))
    tot = stat_send[...]
    for i in range(1, W):
        tot = tot + stat_recv[i - 1]
    cols = jnp.concatenate([tot, jnp.zeros((R - 8, R), F32)], axis=0).T
    mean = cols[:, 0:1] / model_width
    var = cols[:, 1:2] / model_width - mean * mean
    rstd = lax.rsqrt(var + LN_EPS)
    loads["lna"].wait()
    loads["lnm"].wait()
    cen = (x_v[...].astype(F32) - mean) * rstd
    ha_v[...] = (cen * lna_v[0:1, :] + lna_v[1:2, :]).astype(BF16)
    hm_v[...] = (cen * lnm_v[0:1, :] + lnm_v[1:2, :]).astype(BF16)

    def load_late():
        load("k", k_hbm, k_v)
        load("v", v_hbm, v_v)
        load("out", wout_hbm, wout_v)
        for i, (o, h) in enumerate(ARRIVALS):
            row = pl.multiple_of((chip(o) * 2 + h) * 2 * HB, 2 * HB)
            load(("down", i), wdn_hbm.at[pl.ds(row, 2 * HB), :], wdn_v.at[i])

    legs = {
        "1r": (0, 2, 0, None, right), "1l": (1, 2, 1, None, left),
        "2r": (2, 1, 1, None, right), "2l": (3, 3, 0, None, left),
        "3r": (4, 1, 0, 0, right), "3l": (5, 3, 1, 1, left),
    }

    def leg(tag, key, own, stage, landing):
        i, o, h, add, to = legs[key]
        val = own(o, h)
        if add is not None:
            arrived((tag, add))
            val = val + landing[add].astype(F32)
        stage[i] = val.astype(BF16)
        send((tag, i), stage.at[i], landing.at[i], "tpw", to)

    def total(tag, h, own, landing):
        val = own(0, h)
        for i in ((3, 4), (2, 5))[h]:
            arrived((tag, i))
            val = val + landing[i].astype(F32)
        return val

    def qmm(g):
        need(("qkv", g))
        part = dot(ha_v[...], wqkv_v[g], NT).astype(BF16)
        qpart[g] = part.reshape(NX, 2, RB, qw)
        send(("qs", g), qpart.at[g, :, 1 - c], qsib.at[g], "tpw", sib)

    def qkv_own(o, g):
        arrived(("qs", g))
        return qpart[g, chip(o), c].astype(F32) + qsib[g, chip(o)].astype(F32)

    def qm(key):
        leg("q", key, qkv_own, qsend, qrecv)

    def umm(i):
        need(("up", i))
        for k in range(2):
            upart[i, k] = dot(hm_v[...], wup_v[i, :, k * HB:(k + 1) * HB]).astype(BF16)
        send(("us", i), upart.at[i, 1 - c], usib.at[i], "tpw", sib)

    def up_own(r):
        def own(o, h):
            i = PIECES.index((o, h))
            arrived(("us", i))
            rows = slice(r * RG, (r + 1) * RG)
            return upart[i, c, rows].astype(F32) + usib[i, rows].astype(F32)

        return own

    def um(r, key):
        leg(("u", r), key, up_own(r), usend.at[r], urecv.at[r])

    mine = pl.ds(pl.multiple_of(c * HB, HB), HB)

    def act_send(r, name, o, h, to, to_o):
        src = act_all.at[ARRIVALS.index((o, h)), pl.ds(r * RG, RG), mine]
        dst = act_all.at[ARRIVALS.index((to_o, h)), pl.ds(r * RG, RG), mine]
        send(("a", r, name), src, dst, "tpw", to)

    def act(r, key):
        if key in ("0", "1"):
            h = int(key)
            pre = total(("u", r), h, up_own(r), urecv.at[r])
            val = 0.5 * pre * (1.0 + lax.erf(pre * (2.0 ** -0.5)))
            act_all[ARRIVALS.index((0, h)), r * RG:(r + 1) * RG, mine] = val.astype(BF16)
            if h == 0:
                act_send(r, "1r", 0, 0, right, 3)
            else:
                act_send(r, "1l", 0, 1, left, 1)
            act_send(r, ("s", 0, h), 0, h, sib, 0)
        elif key == "2r":
            act_send(r, "2r", 0, 1, right, 3)
        elif key == "2l":
            act_send(r, "2l", 0, 0, left, 1)
        elif key == "3r":
            arrived(("a", r, "1r"))
            act_send(r, "3r", 3, 0, right, 2)
            act_send(r, ("s", 3, 0), 3, 0, sib, 3)
        else:
            arrived(("a", r, "1l"))
            act_send(r, "3l", 1, 1, left, 2)
            act_send(r, ("s", 1, 1), 1, 1, sib, 1)

    def ap(r, key):
        o, h = {"2r": (3, 1), "2l": (1, 0), "3r": (2, 0), "3l": (2, 1)}[key]
        arrived(("a", r, key))
        act_send(r, ("s", o, h), o, h, sib, o)

    begun = set()

    def accumulate(part, *j):
        cols = slice(j[0] * DC, (j[0] + 1) * DC) if j else slice(0, D)
        if begun:
            acc[:, cols] += part
        else:
            acc[...] = part
            begun.add(0)

    def ready(i):
        o, h = ARRIVALS[i]
        for r in range(NG):
            arrived(("a", r, ("s", o, h)))
        need(("down", i))

    def dmm(i):
        ready(i)
        accumulate(dot(act_all[i], wdn_v[i]))

    def last(j):
        cols = slice(j * DC, (j + 1) * DC)
        n = len(ARRIVALS)
        ready(n - 2)
        ready(n - 1)
        accumulate(dot(act_all[n - 2], wdn_v[n - 2, :, cols]) + dot(act_all[n - 1], wdn_v[n - 1, :, cols]), j)

    scale = HD ** -0.5
    when = lax.broadcasted_iota(jnp.int32, (2 * QT, L), 1)

    def rotary(t):
        swapped = jnp.where(first, pltpu.roll(t, 128 - half, 1), pltpu.roll(t, half, 1))
        return (t * cos_t + swapped * sin_t).astype(BF16).astype(F32)

    def qt(g):
        qkv = total("q", g, qkv_own, qrecv).astype(BF16).astype(F32)
        for t in range(QT):
            qrot[g, t * RB:(t + 1) * RB, :] = rotary(qkv[:, t * 128:(t + 1) * 128])
        last = qkv[:, QT * 128:]
        kv = jnp.where(plane < HD, rotary(last), last)
        kvrot[g] = kv
        knew_ref[:, g * HD:(g + 1) * HD] = kv[:, :HD].astype(BF16)
        vnew_ref[:, g * HD:(g + 1) * HD] = kv[:, HD:].astype(BF16)

    def att(g):
        need("k")
        need("v")

        def row(b):
            q8 = qrot[g, pl.ds(b, QT, stride=RB), :]
            q = jnp.concatenate([q8[:, :HD], q8[:, HD:]], axis=0)
            kv = kvrot[g, pl.ds(b, 1), :]
            s = dot(q.astype(BF16), k_v[b * G + g]) * scale
            s = jnp.where(when < pos_ref[b], s, -jnp.inf)
            sn = jnp.sum(q * kv[:, :HD], axis=1, keepdims=True) * scale
            m = jnp.maximum(jnp.max(s, axis=1, keepdims=True), sn)
            e = jnp.exp(s - m)
            en = jnp.exp(sn - m)
            rz = 1.0 / (jnp.sum(e, axis=1, keepdims=True) + en)
            wn = (en * rz).astype(BF16).astype(F32)
            ctx = dot((e * rz).astype(BF16), v_v[b * G + g], NT) + wn * kv[:, HD:]
            ctxs[g, pl.ds(b, QT, stride=RB), :] = jnp.concatenate([ctx[:QT], ctx[QT:]], axis=1)

        def rows(i, _):
            for j in range(8):
                row(i * 8 + j)
            return 0

        lax.fori_loop(0, RB // 8, rows, 0)
        for t in range(QT):
            ctx_all[w, g, :, t * 128:(t + 1) * 128] = ctxs[g, t * RB:(t + 1) * RB, :].astype(BF16)
        send(("c", ("s", 0, g)), ctx_all.at[w, g], ctx_all.at[w, g], "tpw", sib)

    def ctx_send(name, who, g, to):
        send(("c", name), ctx_all.at[who, g], ctx_all.at[who, g], "tpw", to)

    def ctx(key):
        if key == "1r":
            ctx_send("1r", w, 0, right)
        elif key == "1l":
            ctx_send("1l", w, 1, left)
        elif key == "2r":
            ctx_send("2r", w, 1, right)
        elif key == "2l":
            ctx_send("2l", w, 0, left)
        elif key == "3r":
            arrived(("c", "1r"))
            ctx_send("3r", left, 0, right)
            ctx_send(("s", 3, 0), left, 0, sib)
        else:
            arrived(("c", "1l"))
            ctx_send("3l", right, 1, left)
            ctx_send(("s", 1, 1), right, 1, sib)

    def pc(key):
        who, o, g = {"2r": (left, 3, 1), "2l": (right, 1, 0), "3r": (opp, 2, 0), "3l": (opp, 2, 1)}[key]
        arrived(("c", key))
        ctx_send(("s", o, g), who, g, sib)

    def amm():
        for o in range(NX):
            for g in range(G):
                arrived(("c", ("s", o, g)))
        need("out")
        n = QT * 128
        for g in range(G):
            accumulate(dot(ctx_all[:, g].reshape(R, n), wout_v[g * n:(g + 1) * n, :]))

    def ysc(j):
        for i in (2, 1, 3):
            to = lax.rem(y + i, NY)
            rows = pl.ds(pl.multiple_of(to * RY, RY), RY)
            ysend[j, rows, :] = acc[rows, j * DC:(j + 1) * DC].astype(BF16)
            send(("y", j, i), ysend.at[j, rows], yrecv.at[j, i - 1], "tph", to)

    def yga(j):
        rows = pl.ds(pl.multiple_of(y * RY, RY), RY)
        cols = slice(j * DC, (j + 1) * DC)
        tot = acc[rows, cols]
        for i in range(1, NY):
            arrived(("y", j, i))
            tot = tot + yrecv[j, i - 1].astype(F32)
        xout_ref[rows, cols] = (x_v[rows, cols].astype(F32) + tot).astype(BF16)
        block = xout_ref.at[rows, pl.ds(j * DC, DC)]
        for i in (2, 1, 3):
            send(("z", j, i), block, block, "tph", lax.rem(y + i, NY))

    steps = {
        "qmm": qmm, "qm": qm, "umm": umm, "um": um, "a": act, "ap": ap, "dmm": dmm, "last": last, "qt": qt, "att": att,
        "c": ctx, "pc": pc, "amm": amm, "ysc": ysc, "yga": yga,
    }
    last_up = max(i for i, step in enumerate(ORDER) if step[0] == "umm")
    first_sum = min(i for i, step in enumerate(ORDER) if step[0] == "yga")
    done = 0
    for i, step in enumerate(ORDER):
        if i == first_sum:
            for cp in sent:
                cp.wait_send()
            done = len(sent)
        steps[step[0]](*step[1:])
        if i == last_up:
            load_late()
    for name in messages:
        arrived(name)
    for cp in sent[done:]:
        cp.wait_send()


def finish_kernel(x_ref, k_ref, v_ref, xout_ref, knew_ref, vnew_ref):
    xout_ref[...] = x_ref[...]
    hd = knew_ref.shape[2]
    for g in range(knew_ref.shape[1]):
        knew_ref[:, g, :] = k_ref[:, g * hd:(g + 1) * hd]
        vnew_ref[:, g, :] = v_ref[:, g * hd:(g + 1) * hd]


def solution(mesh):
    W = mesh.shape["tpw"]
    NY = mesh.shape["tph"]
    if W != 8:
        raise ValueError("tpw")

    def local_layer(x_in, ln_attn, ln_mlp, w_qkv, w_out, w_up, w_down, k_cache, v_cache, positions):
        R, D = x_in.shape
        _, G, S, HD = w_qkv.shape
        F = w_up.shape[1]
        L = k_cache.shape[2]
        RB = R // W
        NX = W // 2
        NG = GROUPS_OF_ROWS
        RG = R // NG
        qw = S * HD
        cw = (S - 2) * HD
        QT = cw // 128
        HB = F // W // 2
        wqkv_t = jnp.transpose(w_qkv, (1, 2, 3, 0)).reshape(G * qw, D)
        k_t = jnp.swapaxes(k_cache, 2, 3).reshape(RB * G, HD, L)
        v_t = jnp.swapaxes(v_cache, 2, 3).reshape(RB * G, HD, L)
        NC = GROUPS_OF_COLUMNS
        n_messages = W - 1 + 2 + 6 + 8 + NG * 6 + NG * 14 + 14 + NC * 6
        any_spec = pl.BlockSpec(memory_space=pl.ANY)
        vmem_spec = pl.BlockSpec(memory_space=pltpu.VMEM)
        x_out, k_new, v_new = pl.pallas_call(
            functools.partial(layer_kernel, W, NY),
            name="layer",
            out_shape=(
                pltpu.VMEM((R, D), BF16),
                pltpu.VMEM((RB, G * HD), BF16),
                pltpu.VMEM((RB, G * HD), BF16),
            ),
            in_specs=[any_spec] * 10,
            out_specs=(vmem_spec,) * 3,
            scratch_shapes=[
                pltpu.SMEM((RB,), jnp.int32),
                pltpu.VMEM((R, D), BF16),
                pltpu.VMEM((2, D), F32),
                pltpu.VMEM((2, D), F32),
                pltpu.VMEM((G, qw, D), BF16),
                pltpu.VMEM((G * cw, D), BF16),
                pltpu.VMEM((8, D, 2 * HB), BF16),
                pltpu.VMEM((8, 2 * HB, D), BF16),
                pltpu.VMEM((RB * G, HD, L), BF16),
                pltpu.VMEM((RB * G, HD, L), BF16),
                pltpu.VMEM((8, 128), F32),
                pltpu.VMEM((W - 1, 8, 128), F32),
                pltpu.VMEM((R, D), BF16),
                pltpu.VMEM((R, D), BF16),
                pltpu.VMEM((G, NX, 2, RB, qw), BF16),
                pltpu.VMEM((G, NX, RB, qw), BF16),
                pltpu.VMEM((6, RB, qw), BF16),
                pltpu.VMEM((6, RB, qw), BF16),
                pltpu.VMEM((G, QT * RB, 128), F32),
                pltpu.VMEM((G, RB, 128), F32),
                pltpu.VMEM((G, QT * RB, 128), F32),
                pltpu.VMEM((W, G, RB, cw), BF16),
                pltpu.VMEM((8, 2, R, HB), BF16),
                pltpu.VMEM((8, R, HB), BF16),
                pltpu.VMEM((NG, 6, RG, HB), BF16),
                pltpu.VMEM((NG, 6, RG, HB), BF16),
                pltpu.VMEM((8, R, 2 * HB), BF16),
                pltpu.VMEM((R, D), F32),
                pltpu.VMEM((NC, R, D // NC), BF16),
                pltpu.VMEM((NC, NY - 1, R // NY, D // NC), BF16),
                pltpu.SemaphoreType.DMA((32,)),
                pltpu.SemaphoreType.DMA((n_messages,)),
                pltpu.SemaphoreType.DMA((n_messages,)),
            ],
            compiler_params=pltpu.CompilerParams(
                collective_id=0, has_side_effects=True, vmem_limit_bytes=VMEM_LIMIT
            ),
        )(
            positions, x_in, ln_attn, ln_mlp, wqkv_t, w_out.reshape(G * cw, D), w_up, w_down, k_t, v_t,
        )
        return pl.pallas_call(
            finish_kernel,
            name="finish",
            out_shape=(
                jax.ShapeDtypeStruct((R, D), BF16),
                jax.ShapeDtypeStruct((RB, G, HD), BF16),
                jax.ShapeDtypeStruct((RB, G, HD), BF16),
            ),
            in_specs=[vmem_spec] * 3,
            out_specs=(vmem_spec,) * 3,
        )(*(pltpu.with_memory_space_constraint(a, pltpu.VMEM) for a in (x_out, k_new, v_new)))

    cache_spec = P(("dp", "tpw"), "tph", None, None)
    new_spec = P(("dp", "tpw"), "tph", None)
    in_specs = (
        P("dp", "tpw"),
        P(None, "tpw"),
        P(None, "tpw"),
        P("tpw", "tph", None, None),
        P("tph", None, None, "tpw"),
        P("tpw", "tph"),
        P("tph", "tpw"),
        cache_spec,
        cache_spec,
        P(("dp", "tpw")),
    )
    out_specs = (P("dp", "tpw"), new_spec, new_spec)
    return jax.shard_map(local_layer, mesh=mesh, in_specs=in_specs, out_specs=out_specs, check_vma=False)
```
